256 devices in a mesh: stage: 4 (over x), expert: 64 (over z, y, core).
Axes of the slice: x: 4, y: 4, z: 8, core: 2. Of those that a mesh axis runs over, the one named last changes fastest.
Arguments:
- x_acts: bfloat16 [2, 4, 32768, 512], P(None, 'stage', 'expert')
- expert_ids: int32 [2, 4, 32768, 8], P(None, 'stage', 'expert')
- gate_wts: float32 [2, 4, 32768, 8], P(None, 'stage', 'expert')
- w_in: bfloat16 [4, 64, 512, 256], P('stage', 'expert')
- w_up: bfloat16 [4, 64, 512, 256], P('stage', 'expert')
- w_out: bfloat16 [4, 64, 256, 512], P('stage', 'expert')
- d_out: bfloat16 [4, 32768, 512], P('stage', 'expert')
Outputs:
- output 1: bfloat16 [4, 32768, 512], P('stage', 'expert')
- output 2: bfloat16 [4, 32768, 512], P('stage', 'expert')
- output 3: bfloat16 [4, 64, 512, 256], P('stage', 'expert')
- output 4: bfloat16 [4, 64, 512, 256], P('stage', 'expert')
- output 5: bfloat16 [4, 64, 256, 512], P('stage', 'expert')
All inputs are finite; a program needn't handle non-finite values.
Results may differ from the reference program's by a relative error of at most 0.001.
Values are sent between devices in bfloat16 or wider.
A program may use at most 768 MiB of HBM per device.

```python
import jax
import jax.numpy as jnp
from jax import lax

NUM_STAGES = 4
GROUP_SIZE = 64
TOKENS_DEV = 512
MODEL_DIM = 512
FFN_DIM = 256
NUM_EXPERTS = 64
TOP_K = 8
CAPACITY = 3 * TOP_K * TOKENS_DEV // (2 * NUM_EXPERTS)
SLOTS = NUM_EXPERTS * CAPACITY


def device_routing(dev_key):
    key_order, key_pos = jax.random.split(dev_key)
    block_expert = jax.random.permutation(key_order, NUM_EXPERTS)
    token_pos = jax.random.permutation(key_pos, TOKENS_DEV)
    spacing = TOKENS_DEV // TOP_K
    cold_len = TOKENS_DEV // (2 * NUM_EXPERTS)
    slot_pos = (token_pos[:, None] + spacing * jnp.arange(TOP_K)[None, :]) % TOKENS_DEV
    within = slot_pos % (4 * cold_len)
    block_idx = 2 * (slot_pos // (4 * cold_len)) + (within >= 3 * cold_len).astype(jnp.int32)
    return block_expert[block_idx].astype(jnp.int32)


def draw_routing(route_key):
    sub_keys = jax.random.split(route_key, 2 * NUM_STAGES * GROUP_SIZE)
    choices = jax.vmap(device_routing)(sub_keys)
    return choices.reshape(2, NUM_STAGES, GROUP_SIZE * TOKENS_DEV, TOP_K)


def setup_inputs(seed: int = 0) -> dict:
    sub_keys = jax.random.split(jax.random.key(seed), 7)
    tok_shape = (2, NUM_STAGES, GROUP_SIZE * TOKENS_DEV)
    w_shape = (NUM_STAGES, NUM_EXPERTS, MODEL_DIM, FFN_DIM)
    x_acts = jax.random.normal(sub_keys[0], tok_shape + (MODEL_DIM,), jnp.float32)
    expert_ids = draw_routing(sub_keys[1])
    gate_wts = jax.random.uniform(sub_keys[2], tok_shape + (TOP_K,), jnp.float32, 0.5, 1.5) / TOP_K
    w_in = jax.random.normal(sub_keys[3], w_shape, jnp.float32) * MODEL_DIM ** -0.5
    w_up = jax.random.normal(sub_keys[4], w_shape, jnp.float32) * MODEL_DIM ** -0.5
    w_out = jax.random.normal(sub_keys[5], (NUM_STAGES, NUM_EXPERTS, FFN_DIM, MODEL_DIM), jnp.float32) * FFN_DIM ** -0.5
    d_out = jax.random.normal(sub_keys[6], (NUM_STAGES, GROUP_SIZE * TOKENS_DEV, MODEL_DIM), jnp.float32)
    return dict(x_acts=x_acts.astype(jnp.bfloat16), expert_ids=expert_ids, gate_wts=gate_wts,
                w_in=w_in.astype(jnp.bfloat16), w_up=w_up.astype(jnp.bfloat16),
                w_out=w_out.astype(jnp.bfloat16), d_out=d_out.astype(jnp.bfloat16))


def bf16_cast(raw_value):
    return raw_value.astype(jnp.bfloat16).astype(jnp.float32)


def slot_index(choices):
    chosen = choices[:, :, None] == jnp.arange(NUM_EXPERTS)[None, None, :]
    taken = jnp.any(chosen, axis=1).astype(jnp.int32)
    slot_rank = jnp.cumsum(taken, axis=0) - 1
    return choices * CAPACITY + jnp.take_along_axis(slot_rank, choices, axis=1)


def gather_slots(slot_idx, gates):
    flat_idx = slot_idx.reshape(-1)
    owner = jnp.zeros((SLOTS,), jnp.int32).at[flat_idx].set(jnp.repeat(jnp.arange(TOKENS_DEV), TOP_K))
    slot_gate = jnp.zeros((SLOTS,), jnp.float32).at[flat_idx].set(gates.reshape(-1))
    return owner, slot_gate.reshape(NUM_EXPERTS, CAPACITY)


def stage_layer(stage_args):
    x_two, choice_two, gate_two, w_in_s, w_up_s, w_out_s, dy_stage = stage_args
    w_in_f = w_in_s.astype(jnp.float32)
    w_up_f = w_up_s.astype(jnp.float32)
    w_out_f = w_out_s.astype(jnp.float32)

    def per_device(tensor):
        return tensor.reshape((GROUP_SIZE, TOKENS_DEV) + tensor.shape[1:])

    def device_step(grad_acc, dev_block):
        x_fw, ch_fw, g_fw, x_bw, ch_bw, g_bw, dy_bw = dev_block
        idx_fw = slot_index(ch_fw)
        owner_fw, gate_fw = gather_slots(idx_fw, g_fw)
        rows_fw = x_fw.astype(jnp.float32)[owner_fw].reshape(NUM_EXPERTS, CAPACITY, MODEL_DIM)
        pre_in = jnp.einsum('ecd,edf->ecf', rows_fw, w_in_f)
        pre_up = jnp.einsum('ecd,edf->ecf', rows_fw, w_up_f)
        hidden = bf16_cast(jax.nn.silu(pre_in) * pre_up)
        expert_out = jnp.einsum('ecf,efd->ecd', hidden, w_out_f)
        contrib = bf16_cast(gate_fw[:, :, None] * expert_out).reshape(SLOTS, MODEL_DIM)
        y_dev = jnp.sum(contrib[idx_fw], axis=1).astype(jnp.bfloat16)

        idx_bw = slot_index(ch_bw)
        owner_bw, gate_bw = gather_slots(idx_bw, g_bw)
        rows_bw = x_bw.astype(jnp.float32)[owner_bw].reshape(NUM_EXPERTS, CAPACITY, MODEL_DIM)
        dy_rows = dy_bw.astype(jnp.float32)[owner_bw].reshape(NUM_EXPERTS, CAPACITY, MODEL_DIM)
        pre_in = jnp.einsum('ecd,edf->ecf', rows_bw, w_in_f)
        pre_up = jnp.einsum('ecd,edf->ecf', rows_bw, w_up_f)
        sig_in = jax.nn.sigmoid(pre_in)
        act_in = pre_in * sig_in
        hidden = bf16_cast(act_in * pre_up)
        gated_dy = bf16_cast(gate_bw[:, :, None] * dy_rows)
        d_hidden = jnp.einsum('ecd,efd->ecf', gated_dy, w_out_f)
        d_pre_in = bf16_cast(d_hidden * pre_up * sig_in * (1.0 + pre_in * (1.0 - sig_in)))
        d_pre_up = bf16_cast(d_hidden * act_in)
        dx_slot = bf16_cast(jnp.einsum('ecf,edf->ecd', d_pre_in, w_in_f) + jnp.einsum('ecf,edf->ecd', d_pre_up, w_up_f))
        dx_dev = jnp.sum(dx_slot.reshape(SLOTS, MODEL_DIM)[idx_bw], axis=1).astype(jnp.bfloat16)
        acc_in, acc_up, acc_out = grad_acc
        new_acc = (acc_in + jnp.einsum('ecd,ecf->edf', rows_bw, d_pre_in),
                   acc_up + jnp.einsum('ecd,ecf->edf', rows_bw, d_pre_up),
                   acc_out + jnp.einsum('ecf,ecd->efd', hidden, gated_dy))
        return new_acc, (y_dev, dx_dev)

    zero_acc = (jnp.zeros(w_in_s.shape, jnp.float32), jnp.zeros(w_up_s.shape, jnp.float32),
                jnp.zeros(w_out_s.shape, jnp.float32))
    blocks = (per_device(x_two[1]), per_device(choice_two[1]), per_device(gate_two[1]),
              per_device(x_two[0]), per_device(choice_two[0]), per_device(gate_two[0]),
              per_device(dy_stage))
    grads, outs = lax.scan(device_step, zero_acc, blocks)
    tok_total = GROUP_SIZE * TOKENS_DEV
    return (outs[0].reshape(tok_total, MODEL_DIM), outs[1].reshape(tok_total, MODEL_DIM),
            grads[0].astype(jnp.bfloat16), grads[1].astype(jnp.bfloat16), grads[2].astype(jnp.bfloat16))


def reference(x_acts, expert_ids, gate_wts, w_in, w_up, w_out, d_out):
    x_prev = jnp.moveaxis(jnp.roll(x_acts, 1, axis=1), 1, 0)
    ids_prev = jnp.moveaxis(jnp.roll(expert_ids, 1, axis=1), 1, 0)
    gate_prev = jnp.moveaxis(jnp.roll(gate_wts, 1, axis=1), 1, 0)
    y_out, dx_next, d_w_in, d_w_up, d_w_out = lax.map(
        stage_layer, (x_prev, ids_prev, gate_prev, w_in, w_up, w_out, d_out))
    d_x = jnp.roll(dx_next, -1, axis=0)
    return (y_out, d_x, d_w_in, d_w_up, d_w_out)
```

```python
import functools

import jax
import jax.numpy as jnp
from jax import lax
from jax.experimental import pallas as pl
from jax.experimental.pallas import tpu as pltpu
from jax.sharding import PartitionSpec as P

TG = 8
F32 = jnp.float32
BF16 = jnp.bfloat16


def routing_rows(route, group_rank, num_local):
    gates, ids = route[0:8], route[8:16]
    tokens = route.shape[1]
    taken, gate = [], []
    for k in range(num_local):
        hit = ids == (group_rank + k * TG).astype(F32)
        taken.append(jnp.sum(jnp.where(hit, 1.0, 0.0), axis=0, keepdims=True))
        gate.append(jnp.sum(jnp.where(hit, gates, 0.0), axis=0, keepdims=True))
    taken, gate = jnp.concatenate(taken, axis=0), jnp.concatenate(gate, axis=0)
    lane = lax.broadcasted_iota(jnp.int32, taken.shape, 1)
    count, shift = taken, 1
    while shift < tokens:
        count = count + jnp.where(lane >= shift, pltpu.roll(count, shift, 1), 0.0)
        shift *= 2
    return jnp.where(taken > 0.0, count - 1.0, -1.0), gate


def slot_mask(rank_row, capacity):
    slot = lax.broadcasted_iota(jnp.int32, (capacity, rank_row.shape[1]), 0).astype(F32)
    return slot == rank_row


def fill_onehot(hot_ref, rank, capacity):
    for k in range(rank.shape[0]):
        hit = slot_mask(rank[k:k + 1], capacity)
        hot_ref[k * capacity:(k + 1) * capacity, :] = jnp.where(hit, 1.0, 0.0).astype(BF16)


def gate_column(rank_row, gate_row, capacity):
    hit = slot_mask(rank_row, capacity)
    return jnp.sum(jnp.where(hit, gate_row, 0.0), axis=1, keepdims=True)


def gather_kernel(capacity, with_dy, *refs):
    if with_dy:
        route_ref, x_ref, dy_ref, xs_ref, q_ref, rg_ref, hot_ref = refs
    else:
        route_ref, x_ref, xs_ref, rg_ref, hot_ref = refs
    group_rank = lax.rem(lax.axis_index('expert'), TG)
    num_local = xs_ref.shape[0]
    rank, gate = routing_rows(route_ref[0], group_rank, num_local)
    rg_ref[0, 0:8] = rank
    rg_ref[0, 8:16] = gate
    fill_onehot(hot_ref, rank, capacity)
    rows = jnp.dot(hot_ref[...], x_ref[0], preferred_element_type=F32)
    xs_ref[...] = rows.astype(BF16).reshape(xs_ref.shape)
    if with_dy:
        rows = jnp.dot(hot_ref[...], dy_ref[0], preferred_element_type=F32)
        for k in range(num_local):
            col = gate_column(rank[k:k + 1], gate[k:k + 1], capacity)
            q_ref[k] = (col * rows[k * capacity:(k + 1) * capacity]).astype(BF16)


def gather_rows(route, x_all, dy_all, capacity):
    groups, tokens, width = x_all.shape
    num_local = 8
    tok_block = pl.BlockSpec((1, tokens, width), lambda s: (s, 0, 0))
    slot_block = pl.BlockSpec((num_local, capacity, width), lambda s: (0, s, 0))
    rg_block = pl.BlockSpec((1, 16, tokens), lambda s: (s, 0, 0))
    slot_shape = jax.ShapeDtypeStruct((num_local, groups * capacity, width), BF16)
    with_dy = dy_all is not None
    args = (route, x_all, dy_all) if with_dy else (route, x_all)
    flops = 2 * groups * num_local * capacity * tokens * width * (2 if with_dy else 1)
    return pl.pallas_call(
        functools.partial(gather_kernel, capacity, with_dy),
        grid=(groups,),
        in_specs=[rg_block] + [tok_block] * (len(args) - 1),
        out_specs=[slot_block] * (len(args) - 1) + [rg_block],
        out_shape=[slot_shape] * (len(args) - 1) + [jax.ShapeDtypeStruct((groups, 16, tokens), F32)],
        scratch_shapes=[pltpu.VMEM((num_local * capacity, tokens), BF16)],
        cost_estimate=pl.CostEstimate(flops=flops, bytes_accessed=16 << 20, transcendentals=0),
        name='gather_rows_b' if with_dy else 'gather_rows_f',
    )(*args)


def backward_kernel(x_ref, q_ref, wcat_ref, wout_ref, dwcat_ref, dwout_ref, dx_ref, dab_ref):
    x, q, wcat, wout = x_ref[0], q_ref[0], wcat_ref[0], wout_ref[0]
    hid = wout.shape[0]
    pre = jnp.dot(x, wcat, preferred_element_type=F32)
    a, b = pre[:, :hid], pre[:, hid:]
    sig = jax.nn.sigmoid(a)
    act = a * sig
    h = (act * b).astype(BF16)
    dwout_ref[0] = lax.dot_general(h, q, (((0,), (0,)), ((), ())), preferred_element_type=F32)
    u = lax.dot_general(q, wout, (((1,), (1,)), ((), ())), preferred_element_type=F32)
    dab_ref[:, :hid] = (u * b * sig * (1.0 + a * (1.0 - sig))).astype(BF16)
    dab_ref[:, hid:] = (u * act).astype(BF16)
    dab = dab_ref[...]
    dwcat_ref[0] = lax.dot_general(x, dab, (((0,), (0,)), ((), ())), preferred_element_type=F32)
    dx = lax.dot_general(dab, wcat, (((1,), (1,)), ((), ())), preferred_element_type=F32)
    dx_ref[0] = dx.astype(BF16)


def expert_backward(xs, q, wcat, wout):
    num_local, rows, width = xs.shape
    hid = wout.shape[1]
    row_block = pl.BlockSpec((1, rows, width), lambda e: (e, 0, 0))
    cat_block = pl.BlockSpec((1, width, 2 * hid), lambda e: (e, 0, 0))
    out_block = pl.BlockSpec((1, hid, width), lambda e: (e, 0, 0))
    return pl.pallas_call(
        backward_kernel,
        grid=(num_local,),
        in_specs=[row_block, row_block, cat_block, out_block],
        out_specs=[cat_block, out_block, row_block],
        out_shape=[jax.ShapeDtypeStruct(wcat.shape, F32), jax.ShapeDtypeStruct(wout.shape, F32),
                   jax.ShapeDtypeStruct(xs.shape, BF16)],
        scratch_shapes=[pltpu.VMEM((rows, 2 * hid), BF16)],
        cost_estimate=pl.CostEstimate(flops=16 * num_local * rows * width * hid, bytes_accessed=38 << 20,
                                      transcendentals=num_local * rows * hid),
        name='expert_backward',
    )(xs, q, wcat, wout)


def forward_kernel(capacity, rg_ref, x_ref, wcat_ref, wout_ref, c_ref):
    e = pl.program_id(0)
    x, wcat, wout = x_ref[0], wcat_ref[0], wout_ref[0]
    hid = wout.shape[0]
    pre = jnp.dot(x, wcat, preferred_element_type=F32)
    a, b = pre[:, :hid], pre[:, hid:]
    h = (a * jax.nn.sigmoid(a) * b).astype(BF16)
    o = jnp.dot(h, wout, preferred_element_type=F32)
    for s in range(rg_ref.shape[0]):
        col = gate_column(rg_ref[s, pl.ds(e, 1)], rg_ref[s, pl.ds(8 + e, 1)], capacity)
        c_ref[0, s * capacity:(s + 1) * capacity] = (col * o[s * capacity:(s + 1) * capacity]).astype(BF16)


def expert_forward(rg, xs, wcat, wout, capacity):
    num_local, rows, width = xs.shape
    hid = wout.shape[1]
    row_block = pl.BlockSpec((1, rows, width), lambda e: (e, 0, 0))
    return pl.pallas_call(
        functools.partial(forward_kernel, capacity),
        grid=(num_local,),
        in_specs=[pl.BlockSpec(rg.shape, lambda e: (0, 0, 0)), row_block,
                  pl.BlockSpec((1, width, 2 * hid), lambda e: (e, 0, 0)),
                  pl.BlockSpec((1, hid, width), lambda e: (e, 0, 0))],
        out_specs=row_block,
        out_shape=jax.ShapeDtypeStruct(xs.shape, BF16),
        cost_estimate=pl.CostEstimate(flops=6 * num_local * rows * width * hid, bytes_accessed=20 << 20,
                                      transcendentals=num_local * rows * hid),
        name='expert_forward',
    )(rg, xs, wcat, wout)


def scatter_kernel(capacity, rg_ref, c_ref, out_ref, hot_ref):
    fill_onehot(hot_ref, rg_ref[0, 0:8], capacity)
    rows = c_ref[...].reshape(hot_ref.shape[0], c_ref.shape[2])
    out_ref[0] = lax.dot_general(hot_ref[...], rows, (((0,), (0,)), ((), ())), preferred_element_type=F32)


def scatter_rows(rg, slots, capacity):
    num_local, _, width = slots.shape
    groups, _, tokens = rg.shape
    return pl.pallas_call(
        functools.partial(scatter_kernel, capacity),
        grid=(groups,),
        in_specs=[pl.BlockSpec((1, 16, tokens), lambda s: (s, 0, 0)),
                  pl.BlockSpec((num_local, capacity, width), lambda s: (0, s, 0))],
        out_specs=pl.BlockSpec((1, tokens, width), lambda s: (s, 0, 0)),
        out_shape=jax.ShapeDtypeStruct((groups, tokens, width), F32),
        scratch_shapes=[pltpu.VMEM((num_local * capacity, tokens), BF16)],
        cost_estimate=pl.CostEstimate(flops=2 * groups * num_local * capacity * tokens * width,
                                      bytes_accessed=16 << 20, transcendentals=0),
        name='scatter_rows',
    )(rg, slots)


def solution(mesh):
    group_size = mesh.shape['expert']
    num_stages = mesh.shape['stage']
    to_next = [(i, (i + 1) % num_stages) for i in range(num_stages)]
    to_prev = [((i + 1) % num_stages, i) for i in range(num_stages)]
    rows_of = group_size // TG
    tok_groups = [[z * TG + r for r in range(TG)] for z in range(rows_of)]
    wgt_groups = [[z * TG + r for z in range(rows_of)] for r in range(TG)]

    def device_fn(x_acts, expert_ids, gate_wts, w_in, w_up, w_out, d_out):
        tokens, width = x_acts.shape[2], x_acts.shape[3]
        hid = w_in.shape[3]
        capacity = 96

        def gather_tok(arr):
            return lax.all_gather(arr, 'expert', axis_index_groups=tok_groups, axis=0)

        def gather_wgt(arr):
            return lax.all_gather(arr, 'expert', axis_index_groups=wgt_groups, axis=0)

        def reduce_tok(arr):
            return lax.psum_scatter(arr, 'expert', axis_index_groups=tok_groups, scatter_dimension=0, tiled=False)

        def reduce_wgt(arr):
            return lax.psum_scatter(arr, 'expert', axis_index_groups=wgt_groups, scatter_dimension=0, tiled=False)

        wcat = gather_wgt(jnp.concatenate([w_in[0, 0], w_up[0, 0]], axis=1))
        wout = gather_wgt(w_out[0, 0])
        route = jnp.concatenate([gate_wts[0, 0].T, expert_ids[0, 0].T.astype(F32),
                                 gate_wts[1, 0].T, expert_ids[1, 0].T.astype(F32)], axis=0)
        x_bwd = lax.ppermute(x_acts[0, 0], 'stage', to_next)
        route = gather_tok(lax.ppermute(route, 'stage', to_next))
        x_fwd = lax.ppermute(x_acts[1, 0], 'stage', to_next)
        dy_all = gather_tok(d_out[0])
        x_all = gather_tok(x_bwd)
        xs, q, rg = gather_rows(route[:, 0:16], x_all, dy_all, capacity)
        dwcat, dwout, dxs = expert_backward(xs, q, wcat, wout)
        dwout = reduce_wgt(dwout)
        dwcat = reduce_wgt(dwcat)
        dx = reduce_tok(scatter_rows(rg, dxs, capacity)).astype(BF16)
        dx = lax.ppermute(dx, 'stage', to_prev)
        xf_all = gather_tok(x_fwd)
        xs_f, rg_f = gather_rows(route[:, 16:32], xf_all, None, capacity)
        c = expert_forward(rg_f, xs_f, wcat, wout, capacity)
        y = reduce_tok(scatter_rows(rg_f, c, capacity)).astype(BF16)
        dwcat = dwcat.astype(BF16)
        return (y[None], dx[None], dwcat[None, None, :, :hid], dwcat[None, None, :, hid:],
                dwout.astype(BF16)[None, None])

    tok_spec = P(None, 'stage', 'expert', None)
    w_spec = P('stage', 'expert', None, None)
    row_spec = P('stage', 'expert', None)
    return jax.shard_map(device_fn, mesh=mesh,
                         in_specs=(tok_spec, tok_spec, tok_spec, w_spec, w_spec, w_spec, row_spec),
                         out_specs=(row_spec, row_spec, w_spec, w_spec, w_spec), check_vma=False)
```

```python
import functools

import jax
import jax.numpy as jnp
from jax import lax
from jax.experimental import pallas as pl
from jax.experimental.pallas import tpu as pltpu
from jax.sharding import PartitionSpec as P

TG = 8
F32 = jnp.float32
BF16 = jnp.bfloat16
MESH = pl.DeviceIdType.MESH


def routing_rows(gates, ids, group_rank, num_local):
    tokens = ids.shape[1]
    taken, gate = [], []
    for k in range(num_local):
        hit = ids == group_rank + k * TG
        taken.append(jnp.sum(jnp.where(hit, 1.0, 0.0), axis=0, keepdims=True))
        gate.append(jnp.sum(jnp.where(hit, gates, 0.0), axis=0, keepdims=True))
    taken, gate = jnp.concatenate(taken, axis=0), jnp.concatenate(gate, axis=0)
    lane = lax.broadcasted_iota(jnp.int32, taken.shape, 1)
    count, shift = taken, 1
    while shift < tokens:
        count = count + jnp.where(lane >= shift, pltpu.roll(count, shift, 1), 0.0)
        shift *= 2
    return jnp.where(taken > 0.0, count - 1.0, -1.0), gate


def slot_mask(rank_row, capacity):
    slot = lax.broadcasted_iota(jnp.int32, (capacity, rank_row.shape[1]), 0).astype(F32)
    return slot == rank_row


def fill_onehot(hot_ref, rank, capacity):
    for k in range(rank.shape[0]):
        hit = slot_mask(rank[k:k + 1], capacity)
        hot_ref[k * capacity:(k + 1) * capacity, :] = jnp.where(hit, 1.0, 0.0).astype(BF16)


def gate_column(rank_row, gate_row, capacity):
    hit = slot_mask(rank_row, capacity)
    return jnp.sum(jnp.where(hit, gate_row, 0.0), axis=1, keepdims=True)


class Peers:
    def __init__(self, num_stages):
        stage, me = lax.axis_index('stage'), lax.axis_index('expert')
        self.rank = lax.rem(me, TG)
        self.base = me - self.rank
        self.stage = stage
        self.core = lax.rem(self.rank, 2)
        self.ypos = (self.rank - self.core) // 2
        self.own, self.up_slot = self.rank, self.slot(1)
        self.far_slot, self.down_slot = self.slot(2), self.slot(3)
        self.up = (stage, self.base + self.slot(1))
        self.down = (stage, self.base + self.slot(3))
        self.partner = (stage, self.base + self.slot(0, True))
        self.after = (lax.rem(stage + 1, num_stages), me)
        self.before = (lax.rem(stage + num_stages - 1, num_stages), me)

    def slot(self, offset, other_core=False):
        core = 1 - self.core if other_core else self.core
        return lax.rem(self.ypos + offset, 4) * 2 + core


def greet(devices):
    barrier = pltpu.get_barrier_semaphore()
    for device in devices:
        pl.semaphore_signal(barrier, inc=1, device_id=device, device_id_type=MESH)
    pl.semaphore_wait(barrier, len(devices))


def send(src, dst, send_sem, recv_sem, device):
    return pltpu.make_async_remote_copy(src_ref=src, dst_ref=dst, send_sem=send_sem, recv_sem=recv_sem,
                                        device_id=device, device_id_type=MESH)


class Spread:
    def __init__(self, peers, src, buf, send_sems, recv_sems):
        half = buf.shape[1] // 2
        p = peers

        def copy(i, ref, device, dst=None):
            return send(ref, ref if dst is None else dst, send_sems.at[i], recv_sems.at[i], device)

        own = buf.at[p.own]
        self.own_up = copy(0, src, p.up, own)
        self.own_down = copy(1, src, p.down, own)
        self.fwd_up = copy(2, buf.at[p.down_slot, pl.ds(0, half)], p.up)
        self.fwd_down = copy(3, buf.at[p.up_slot, pl.ds(half, half)], p.down)
        self.own_side = copy(4, src, p.partner, own)
        self.down_side = copy(5, buf.at[p.down_slot], p.partner)
        self.up_side = copy(6, buf.at[p.up_slot], p.partner)
        self.far_side = copy(7, buf.at[p.far_slot], p.partner)

    def start(self):
        self.own_up.start()
        self.own_down.start()
        self.own_side.start()

    def forward(self):
        self.own_up.wait_recv()
        self.fwd_up.start()
        self.down_side.start()
        self.own_down.wait_recv()
        self.fwd_down.start()
        self.up_side.start()

    def last(self):
        self.fwd_up.wait_recv()
        self.fwd_down.wait_recv()
        self.far_side.start()
        for copy in (self.own_side, self.down_side, self.up_side, self.far_side):
            copy.wait_recv()

    def finish(self):
        for copy in (self.own_up, self.own_down, self.fwd_up, self.fwd_down,
                     self.own_side, self.down_side, self.up_side, self.far_side):
            copy.wait_send()


def dispatch_kernel(num_stages, capacity, x_ref, ids_ref, gate_ref, dy_ref,
                    xs_ref, q_ref, xf_ref, rgb_ref, rgf_ref,
                    dy_buf, xb_buf, xf_buf, ids_buf, gate_buf, hot_ref, stage_ref,
                    send_sems, recv_sems, hop_send, hop_recv, local_sem, out_sems):
    p = Peers(num_stages)
    num_local = xs_ref.shape[0]
    keep = pltpu.make_async_copy(dy_ref, dy_buf.at[p.own], local_sem)
    keep.start()
    greet((p.up, p.down, p.partner, p.after, p.before))
    hops = []
    for i, (src, buf) in enumerate(((ids_ref, ids_buf), (gate_ref, gate_buf),
                                    (x_ref.at[0], xb_buf), (x_ref.at[1], xf_buf))):
        hops.append(send(src, buf.at[p.own], hop_send.at[i], hop_recv.at[i], p.after))
    spread = [Spread(p, src, buf, send_sems.at[i], recv_sems.at[i]) for i, (src, buf) in enumerate((
        (ids_buf.at[p.own], ids_buf), (gate_buf.at[p.own], gate_buf), (xb_buf.at[p.own], xb_buf),
        (xf_buf.at[p.own], xf_buf), (dy_ref, dy_buf)))]
    s_ids, s_gate, s_xb, s_xf, s_dy = spread
    hops[0].start()
    hops[1].start()
    hops[2].start()
    s_dy.start()
    hops[3].start()
    hops[0].wait_recv()
    s_ids.start()
    hops[1].wait_recv()
    s_gate.start()
    s_ids.forward()
    s_gate.forward()
    s_dy.forward()
    hops[2].wait_recv()
    s_xb.start()
    s_ids.last()
    s_gate.last()

    def route_step(s, carry):
        for mb, out in ((0, rgb_ref), (1, rgf_ref)):
            rank, gate = routing_rows(gate_buf[s, mb], ids_buf[s, mb], p.rank, num_local)
            out[s, 0:8] = rank
            out[s, 8:16] = gate
        fill_onehot(hot_ref.at[s], rgb_ref[s, 0:8], capacity)
        return carry

    lax.fori_loop(0, TG, route_step, 0)
    s_dy.last()
    keep.wait()

    def put(slot, s, out_ref):
        rows = pl.ds(pl.multiple_of(s * capacity, 16), capacity)
        return pltpu.make_async_copy(stage_ref.at[slot], out_ref.at[:, rows], out_sems.at[slot])

    def gather(buf, out_ref, lo, hi, gates):
        def step(s, carry):
            slot = lax.rem(s, 2)

            @pl.when(s >= lo + 2)
            def _():
                put(slot, s - 2, out_ref).wait()

            rows = jnp.dot(hot_ref[s], buf[s], preferred_element_type=F32)
            if gates is None:
                stage_ref[slot] = rows.astype(BF16).reshape(stage_ref.shape[1:])
            else:
                for k in range(num_local):
                    col = gate_column(gates[s, k:k + 1], gates[s, 8 + k:9 + k], capacity)
                    stage_ref[slot, k] = (col * rows[k * capacity:(k + 1) * capacity]).astype(BF16)
            put(slot, s, out_ref).start()
            return carry

        lax.fori_loop(lo, hi, step, 0)
        for s in (hi - 2, hi - 1):
            put(s % 2, s, out_ref).wait()

    gather(dy_buf, q_ref, 0, 4, rgb_ref)
    s_xb.forward()
    hops[3].wait_recv()
    s_xf.start()
    gather(dy_buf, q_ref, 4, 8, rgb_ref)
    s_xb.last()
    gather(xb_buf, xs_ref, 0, 8, None)
    s_xf.forward()

    def hot_step(s, carry):
        fill_onehot(hot_ref.at[s], rgf_ref[s, 0:8], capacity)
        return carry

    lax.fori_loop(0, TG, hot_step, 0)
    s_xf.last()
    gather(xf_buf, xf_ref, 0, 8, None)
    for s in spread:
        s.finish()
    for hop in hops:
        hop.wait_send()


def dispatch_rows(x_acts, ids, gates, dy, capacity, num_stages):
    tokens, width = dy.shape
    num_local = 8
    slot_shape = jax.ShapeDtypeStruct((num_local, TG * capacity, width), BF16)
    rg_shape = jax.ShapeDtypeStruct((TG, 16, tokens), F32)
    any_spec, vmem_spec = pl.BlockSpec(memory_space=pl.ANY), pl.BlockSpec(memory_space=pltpu.VMEM)
    return pl.pallas_call(
        functools.partial(dispatch_kernel, num_stages, capacity),
        in_specs=[any_spec] * 4,
        out_specs=[any_spec] * 3 + [vmem_spec] * 2,
        out_shape=[slot_shape] * 3 + [rg_shape] * 2,
        scratch_shapes=[
            pltpu.VMEM((TG, tokens, width), BF16), pltpu.VMEM((TG, tokens, width), BF16),
            pltpu.VMEM((TG, tokens, width), BF16), pltpu.VMEM((TG,) + ids.shape, jnp.int32),
            pltpu.VMEM((TG,) + gates.shape, F32), pltpu.VMEM((TG, num_local * capacity, tokens), BF16),
            pltpu.VMEM((2, num_local, capacity, width), BF16),
            pltpu.SemaphoreType.DMA((5, 8)), pltpu.SemaphoreType.DMA((5, 8)),
            pltpu.SemaphoreType.DMA((4,)), pltpu.SemaphoreType.DMA((4,)),
            pltpu.SemaphoreType.DMA, pltpu.SemaphoreType.DMA((2,))],
        compiler_params=pltpu.CompilerParams(collective_id=1, has_side_effects=True,
                                             vmem_limit_bytes=56 << 20),
        cost_estimate=pl.CostEstimate(flops=40 * 10 ** 9, bytes_accessed=40 << 20, transcendentals=0),
        name='dispatch_rows',
    )(x_acts, ids, gates, dy)


def backward_kernel(x_ref, q_ref, wall_ref, dw_ref, dx_ref, dab_ref):
    x, q = x_ref[0], q_ref[0]
    width, hid = x.shape[1], dab_ref.shape[1] // 2
    wcat, wout = wall_ref[0, :width], wall_ref[0, width:]
    pre = jnp.dot(x, wcat, preferred_element_type=F32)
    a, b = pre[:, :hid], pre[:, hid:]
    sig = jax.nn.sigmoid(a)
    act = a * sig
    h = (act * b).astype(BF16)
    dw_ref[0, width:] = lax.dot_general(h, q, (((0,), (0,)), ((), ())), preferred_element_type=F32)
    u = lax.dot_general(q, wout, (((1,), (1,)), ((), ())), preferred_element_type=F32)
    dab_ref[:, :hid] = (u * b * sig * (1.0 + a * (1.0 - sig))).astype(BF16)
    dab_ref[:, hid:] = (u * act).astype(BF16)
    dab = dab_ref[...]
    dw_ref[0, :width] = lax.dot_general(x, dab, (((0,), (0,)), ((), ())), preferred_element_type=F32)
    dx = lax.dot_general(dab, wcat, (((1,), (1,)), ((), ())), preferred_element_type=F32)
    dx_ref[0] = dx.astype(BF16)


def expert_backward(xs, q, wall, hid):
    num_local, rows, width = xs.shape
    row_block = pl.BlockSpec((1, rows, width), lambda e: (e, 0, 0))
    wgt_block = pl.BlockSpec((1,) + wall.shape[1:], lambda e: (e, 0, 0))
    return pl.pallas_call(
        backward_kernel,
        grid=(num_local,),
        in_specs=[row_block, row_block, wgt_block],
        out_specs=[wgt_block, row_block],
        out_shape=[jax.ShapeDtypeStruct(wall.shape, F32), jax.ShapeDtypeStruct(xs.shape, BF16)],
        scratch_shapes=[pltpu.VMEM((rows, 2 * hid), BF16)],
        cost_estimate=pl.CostEstimate(flops=16 * num_local * rows * width * hid, bytes_accessed=38 << 20,
                                      transcendentals=num_local * rows * hid),
        name='expert_backward',
    )(xs, q, wall)


def forward_kernel(capacity, rg_ref, x_ref, wall_ref, c_ref):
    e = pl.program_id(0)
    x = x_ref[0]
    width = x.shape[1]
    wcat, wout = wall_ref[0, :width], wall_ref[0, width:]
    hid = wout.shape[0]
    pre = jnp.dot(x, wcat, preferred_element_type=F32)
    a, b = pre[:, :hid], pre[:, hid:]
    h = (a * jax.nn.sigmoid(a) * b).astype(BF16)
    o = jnp.dot(h, wout, preferred_element_type=F32)
    for s in range(rg_ref.shape[0]):
        col = gate_column(rg_ref[s, pl.ds(e, 1)], rg_ref[s, pl.ds(8 + e, 1)], capacity)
        c_ref[0, s * capacity:(s + 1) * capacity] = (col * o[s * capacity:(s + 1) * capacity]).astype(BF16)


def expert_forward(rg, xs, wall, hid, capacity):
    num_local, rows, width = xs.shape
    row_block = pl.BlockSpec((1, rows, width), lambda e: (e, 0, 0))
    return pl.pallas_call(
        functools.partial(forward_kernel, capacity),
        grid=(num_local,),
        in_specs=[pl.BlockSpec(rg.shape, lambda e: (0, 0, 0)), row_block,
                  pl.BlockSpec((1,) + wall.shape[1:], lambda e: (e, 0, 0))],
        out_specs=row_block,
        out_shape=jax.ShapeDtypeStruct(xs.shape, BF16),
        cost_estimate=pl.CostEstimate(flops=6 * num_local * rows * width * hid, bytes_accessed=20 << 20,
                                      transcendentals=num_local * rows * hid),
        name='expert_forward',
    )(rg, xs, wall)


def combine_kernel(num_stages, capacity, rg_ref, c_ref, out_ref, hot_ref, side_out, side_in, acc, half_in,
                   up_in, down_in, send_sems, recv_sems):
    p = Peers(num_stages)
    half = acc.shape[1] // 2
    low, high = pl.ds(0, half), pl.ds(half, half)
    greet((p.up, p.down, p.partner))

    def partial_sum(slot):
        fill_onehot(hot_ref, rg_ref[slot, 0:8], capacity)
        start = pl.ds(pl.multiple_of(slot * capacity, 16), capacity)
        rows = c_ref[:, start].reshape(hot_ref.shape[0], c_ref.shape[2])
        return lax.dot_general(hot_ref[...], rows, (((0,), (0,)), ((), ())), preferred_element_type=F32)

    sides = [send(side_out.at[d], side_in.at[d], send_sems.at[d], recv_sems.at[d], p.partner) for d in range(4)]
    far_up = send(acc.at[2, low], half_in.at[0], send_sems.at[4], recv_sems.at[4], p.up)
    far_down = send(acc.at[2, high], half_in.at[1], send_sems.at[5], recv_sems.at[5], p.down)
    up_a = send(acc.at[1, high], up_in.at[high], send_sems.at[6], recv_sems.at[6], p.up)
    up_b = send(acc.at[1, low], up_in.at[low], send_sems.at[7], recv_sems.at[7], p.up)
    down_a = send(acc.at[3, low], down_in.at[low], send_sems.at[8], recv_sems.at[8], p.down)
    down_b = send(acc.at[3, high], down_in.at[high], send_sems.at[9], recv_sems.at[9], p.down)

    def both(d):
        side_out[d] = partial_sum(p.slot(d, True))
        sides[d].start()
        acc[d] = partial_sum(p.slot(d))

    def add_side(d):
        sides[d].wait_recv()
        acc[d] = acc[d] + side_in[d]

    both(2)
    add_side(2)
    far_up.start()
    far_down.start()
    both(1)
    add_side(1)
    up_a.start()
    both(3)
    add_side(3)
    down_a.start()
    both(0)
    add_side(0)
    far_up.wait_recv()
    acc[1, low] = acc[1, low] + half_in[0]
    up_b.start()
    far_down.wait_recv()
    acc[3, high] = acc[3, high] + half_in[1]
    down_b.start()
    up_a.wait_recv()
    up_b.wait_recv()
    down_a.wait_recv()
    down_b.wait_recv()
    out_ref[...] = (acc[0] + up_in[...] + down_in[...]).astype(BF16)
    for copy in sides + [far_up, far_down, up_a, up_b, down_a, down_b]:
        copy.wait_send()


def combine_rows(rg, slots, capacity, num_stages, collective_id):
    num_local, _, width = slots.shape
    tokens = rg.shape[2]
    vmem_spec = pl.BlockSpec(memory_space=pltpu.VMEM)
    return pl.pallas_call(
        functools.partial(combine_kernel, num_stages, capacity),
        in_specs=[vmem_spec, vmem_spec],
        out_specs=vmem_spec,
        out_shape=jax.ShapeDtypeStruct((tokens, width), BF16),
        scratch_shapes=[
            pltpu.VMEM((num_local * capacity, tokens), BF16),
            pltpu.VMEM((4, tokens, width), F32), pltpu.VMEM((4, tokens, width), F32),
            pltpu.VMEM((4, tokens, width), F32), pltpu.VMEM((2, tokens // 2, width), F32),
            pltpu.VMEM((tokens, width), F32), pltpu.VMEM((tokens, width), F32),
            pltpu.SemaphoreType.DMA((10,)), pltpu.SemaphoreType.DMA((10,))],
        compiler_params=pltpu.CompilerParams(collective_id=collective_id, has_side_effects=True,
                                             vmem_limit_bytes=56 << 20),
        cost_estimate=pl.CostEstimate(flops=20 * 10 ** 9, bytes_accessed=8 << 20, transcendentals=0),
        name='combine_rows_%d' % collective_id,
    )(rg, slots)


def solution(mesh):
    group_size = mesh.shape['expert']
    num_stages = mesh.shape['stage']
    to_prev = [((i + 1) % num_stages, i) for i in range(num_stages)]
    rows_of = group_size // TG
    wgt_groups = [[z * TG + r for z in range(rows_of)] for r in range(TG)]

    def device_fn(x_acts, expert_ids, gate_wts, w_in, w_up, w_out, d_out):
        tokens, width = x_acts.shape[2], x_acts.shape[3]
        hid = w_in.shape[3]
        capacity = 96

        def gather_wgt(arr):
            return lax.all_gather(arr, 'expert', axis_index_groups=wgt_groups, axis=0)

        def reduce_wgt(arr):
            return lax.psum_scatter(arr, 'expert', axis_index_groups=wgt_groups, scatter_dimension=0, tiled=False)

        wall = jnp.concatenate([jnp.concatenate([w_in[0, 0], w_up[0, 0]], axis=1), w_out[0, 0]], axis=0)
        wall = gather_wgt(wall)
        ids = jnp.swapaxes(expert_ids[:, 0], 1, 2)
        gates = jnp.swapaxes(gate_wts[:, 0], 1, 2)
        xs, q, xs_f, rg, rg_f = dispatch_rows(x_acts[:, 0], ids, gates, d_out[0], capacity, num_stages)
        dwall, dxs = expert_backward(xs, q, wall, hid)
        xs_f, dxs = lax.optimization_barrier((xs_f, dxs))
        dwall = reduce_wgt(dwall)
        dx = combine_rows(rg, dxs, capacity, num_stages, 2)
        dx = lax.ppermute(dx, 'stage', to_prev)
        c = expert_forward(rg_f, xs_f, wall, hid, capacity)
        y = combine_rows(rg_f, c, capacity, num_stages, 3)
        dwall = dwall.astype(BF16)
        return (y[None], dx[None], dwall[None, None, :width, :hid], dwall[None, None, :width, hid:],
                dwall[None, None, width:])

    tok_spec = P(None, 'stage', 'expert', None)
    w_spec = P('stage', 'expert', None, None)
    row_spec = P('stage', 'expert', None)
    return jax.shard_map(device_fn, mesh=mesh,
                         in_specs=(tok_spec, tok_spec, tok_spec, w_spec, w_spec, w_spec, row_spec),
                         out_specs=(row_spec, row_spec, w_spec, w_spec, w_spec), check_vma=False)
```

```python
import functools

import jax
import jax.numpy as jnp
from jax import lax
from jax.experimental import pallas as pl
from jax.experimental.pallas import tpu as pltpu
from jax.sharding import PartitionSpec as P

TG = 8
F32 = jnp.float32
BF16 = jnp.bfloat16
MESH = pl.DeviceIdType.MESH


def routing_rows(gates, ids, group_rank, num_local):
    tokens = ids.shape[1]
    taken, gate = [], []
    for k in range(num_local):
        hit = ids == group_rank + k * TG
        taken.append(jnp.sum(jnp.where(hit, 1.0, 0.0), axis=0, keepdims=True))
        gate.append(jnp.sum(jnp.where(hit, gates, 0.0), axis=0, keepdims=True))
    taken, gate = jnp.concatenate(taken, axis=0), jnp.concatenate(gate, axis=0)
    lane = lax.broadcasted_iota(jnp.int32, taken.shape, 1)
    count, shift = taken, 1
    while shift < tokens:
        count = count + jnp.where(lane >= shift, pltpu.roll(count, shift, 1), 0.0)
        shift *= 2
    return jnp.where(taken > 0.0, count - 1.0, -1.0), gate


def slot_mask(rank_row, capacity):
    slot = lax.broadcasted_iota(jnp.int32, (capacity, rank_row.shape[1]), 0).astype(F32)
    return slot == rank_row


def fill_onehot(hot_ref, rank, capacity):
    for k in range(rank.shape[0]):
        hit = slot_mask(rank[k:k + 1], capacity)
        hot_ref[k * capacity:(k + 1) * capacity, :] = jnp.where(hit, 1.0, 0.0).astype(BF16)


def gate_column(rank_row, gate_row, capacity):
    hit = slot_mask(rank_row, capacity)
    return jnp.sum(jnp.where(hit, gate_row, 0.0), axis=1, keepdims=True)


class Peers:
    def __init__(self, num_stages, group_size=64):
        stage, me = lax.axis_index('stage'), lax.axis_index('expert')
        self.rank = lax.rem(me, TG)
        self.base = me - self.rank
        self.zpos = self.base // TG
        self.z_size = group_size // TG
        self.z_up = (stage, self.z_slot(1) * TG + self.rank)
        self.z_down = (stage, self.z_slot(-1) * TG + self.rank)
        self.core = lax.rem(self.rank, 2)
        self.ypos = (self.rank - self.core) // 2
        self.own, self.up_slot = self.rank, self.slot(1)
        self.far_slot, self.down_slot = self.slot(2), self.slot(3)
        self.up = (stage, self.base + self.slot(1))
        self.down = (stage, self.base + self.slot(3))
        self.partner = (stage, self.base + self.slot(0, True))
        self.after = (lax.rem(stage + 1, num_stages), me)
        self.before = (lax.rem(stage + num_stages - 1, num_stages), me)

    def z_slot(self, offset):
        return lax.rem(self.zpos + offset + self.z_size, self.z_size)

    def slot(self, offset, other_core=False):
        core = 1 - self.core if other_core else self.core
        return lax.rem(self.ypos + offset, 4) * 2 + core


def greet(devices):
    barrier = pltpu.get_barrier_semaphore()
    for device in devices:
        pl.semaphore_signal(barrier, inc=1, device_id=device, device_id_type=MESH)
    pl.semaphore_wait(barrier, len(devices))


def send(src, dst, send_sem, recv_sem, device):
    return pltpu.make_async_remote_copy(src_ref=src, dst_ref=dst, send_sem=send_sem, recv_sem=recv_sem,
                                        device_id=device, device_id_type=MESH)


class Spread:
    def __init__(self, peers, src, buf, send_sems, recv_sems):
        half = buf.shape[1] // 2
        p = peers

        def copy(i, ref, device, dst=None):
            return send(ref, ref if dst is None else dst, send_sems.at[i], recv_sems.at[i], device)

        own = buf.at[p.own]
        self.own_up = copy(0, src, p.up, own)
        self.own_down = copy(1, src, p.down, own)
        self.fwd_up = copy(2, buf.at[p.down_slot, pl.ds(0, half)], p.up)
        self.fwd_down = copy(3, buf.at[p.up_slot, pl.ds(half, half)], p.down)
        self.own_side = copy(4, src, p.partner, own)
        self.down_side = copy(5, buf.at[p.down_slot], p.partner)
        self.up_side = copy(6, buf.at[p.up_slot], p.partner)
        self.far_side = copy(7, buf.at[p.far_slot], p.partner)

    def start(self):
        self.own_up.start()
        self.own_down.start()
        self.own_side.start()

    def forward(self):
        self.own_up.wait_recv()
        self.fwd_up.start()
        self.down_side.start()
        self.own_down.wait_recv()
        self.fwd_down.start()
        self.up_side.start()

    def last(self):
        self.fwd_up.wait_recv()
        self.fwd_down.wait_recv()
        self.far_side.start()
        for copy in (self.own_side, self.down_side, self.up_side, self.far_side):
            copy.wait_recv()

    def finish(self):
        for copy in (self.own_up, self.own_down, self.fwd_up, self.fwd_down,
                     self.own_side, self.down_side, self.up_side, self.far_side):
            copy.wait_send()


class WeightRing:
    def __init__(self, p, buf, send_sems, recv_sems):
        self.rows = buf.shape[1] // 4
        self.copies = []
        for way, device in ((0, p.z_up), (1, p.z_down)):
            way_copies = []
            for i in range(14):
                step, pos = divmod(i, 4)
                piece = (pos + 2 * way) % 4
                slot = p.z_slot(-step if way == 0 else step)
                ref = buf.at[slot, pl.ds(piece * self.rows, self.rows)]
                way_copies.append(send(ref, ref, send_sems.at[way, i], recv_sems.at[way, i], device))
            self.copies.append(way_copies)

    def start(self):
        for pos in range(4):
            for way in range(2):
                self.copies[way][pos].start()

    def event(self, i):
        for way in range(2):
            self.copies[way][i].wait_recv()
            if i + 4 < 14:
                self.copies[way][i + 4].start()

    def finish(self):
        for way in range(2):
            for copy in self.copies[way]:
                copy.wait_send()


def expert_step(x, q, wcat, wout, dw_ref, dx_ref, dab_ref):
    width, hid = wcat.shape[0], wout.shape[0]
    pre = jnp.dot(x, wcat, preferred_element_type=F32)
    a, b = pre[:, :hid], pre[:, hid:]
    sig = jax.nn.sigmoid(a)
    act = a * sig
    h = (act * b).astype(BF16)
    dw_ref[width:] = lax.dot_general(h, q, (((0,), (0,)), ((), ())), preferred_element_type=F32)
    u = lax.dot_general(q, wout, (((1,), (1,)), ((), ())), preferred_element_type=F32)
    dab_ref[:, :hid] = (u * b * sig * (1.0 + a * (1.0 - sig))).astype(BF16)
    dab_ref[:, hid:] = (u * act).astype(BF16)
    dab = dab_ref[...]
    dw_ref[:width] = lax.dot_general(x, dab, (((0,), (0,)), ((), ())), preferred_element_type=F32)
    dx = lax.dot_general(dab, wcat, (((1,), (1,)), ((), ())), preferred_element_type=F32)
    dx_ref[...] = dx.astype(BF16)


def dispatch_kernel(num_stages, capacity, x_ref, ids_ref, gate_ref, dy_ref, wi_ref, wu_ref, wo_ref,
                    dw_ref, dxs_ref, xf_ref, wall_ref, rgb_ref, rgf_ref,
                    dy_buf, xb_buf, xf_buf, ids_buf, gate_buf, hot_ref, xs_buf, q_buf, wall_buf, dw_buf, dab_ref,
                    send_sems, recv_sems, hop_send, hop_recv, z_send, z_recv, local_sems, dw_sems, dx_sems):
    p = Peers(num_stages)
    num_local = xs_buf.shape[0]
    width, hid = wi_ref.shape
    block = wall_buf.at[p.z_slot(0)]
    keep = [pltpu.make_async_copy(wi_ref, block.at[pl.ds(0, width), pl.ds(0, hid)], local_sems.at[0]),
            pltpu.make_async_copy(wu_ref, block.at[pl.ds(0, width), pl.ds(hid, hid)], local_sems.at[1]),
            pltpu.make_async_copy(wo_ref, block.at[pl.ds(width, hid)], local_sems.at[2])]
    keep_dy = pltpu.make_async_copy(dy_ref, dy_buf.at[p.own], local_sems.at[3])
    for copy in keep:
        copy.start()
    keep_dy.start()
    greet((p.up, p.down, p.partner, p.after, p.before, p.z_up, p.z_down))
    hops = []
    for i, (src, buf) in enumerate(((ids_ref, ids_buf), (gate_ref, gate_buf),
                                    (x_ref.at[0], xb_buf), (x_ref.at[1], xf_buf))):
        hops.append(send(src, buf.at[p.own], hop_send.at[i], hop_recv.at[i], p.after))
    spread = [Spread(p, src, buf, send_sems.at[i], recv_sems.at[i]) for i, (src, buf) in enumerate((
        (ids_buf.at[p.own], ids_buf), (gate_buf.at[p.own], gate_buf), (xb_buf.at[p.own], xb_buf),
        (xf_buf.at[p.own], xf_buf), (dy_ref, dy_buf)))]
    s_ids, s_gate, s_xb, s_xf, s_dy = spread
    ring = WeightRing(p, wall_buf, z_send, z_recv)
    hops[0].start()
    hops[1].start()
    hops[2].start()
    s_dy.start()
    for copy in keep:
        copy.wait()
    ring.start()
    hops[3].start()
    hops[0].wait_recv()
    s_ids.start()
    hops[1].wait_recv()
    s_gate.start()
    ring.event(0)
    ring.event(1)
    s_ids.forward()
    s_gate.forward()
    s_dy.forward()
    hops[2].wait_recv()
    s_xb.start()
    ring.event(2)
    s_ids.last()
    s_gate.last()

    def route_step(s, carry):
        for mb, out in ((0, rgb_ref), (1, rgf_ref)):
            rank, gate = routing_rows(gate_buf[s, mb], ids_buf[s, mb], p.rank, num_local)
            out[s, 0:8] = rank
            out[s, 8:16] = gate
        fill_onehot(hot_ref.at[s], rgb_ref[s, 0:8], capacity)
        return carry

    def rows_of(s):
        return pl.ds(pl.multiple_of(s * capacity, 16), capacity)

    def dy_step(s, carry):
        rows = jnp.dot(hot_ref[s], dy_buf[s], preferred_element_type=F32)
        for k in range(num_local):
            col = gate_column(rgb_ref[s, k:k + 1], rgb_ref[s, 8 + k:9 + k], capacity)
            q_buf[k, rows_of(s)] = (col * rows[k * capacity:(k + 1) * capacity]).astype(BF16)
        return carry

    def x_step(s, carry):
        rows = jnp.dot(hot_ref[s], xb_buf[s], preferred_element_type=F32).astype(BF16)
        for k in range(num_local):
            xs_buf[k, rows_of(s)] = rows[k * capacity:(k + 1) * capacity]
        return carry

    half = TG // 2
    lax.fori_loop(0, half, route_step, 0)
    ring.event(3)
    lax.fori_loop(half, TG, route_step, 0)
    s_dy.last()
    keep_dy.wait()
    ring.event(4)
    lax.fori_loop(0, half, dy_step, 0)
    ring.event(5)
    lax.fori_loop(half, TG, dy_step, 0)
    ring.event(6)
    s_xb.forward()
    hops[3].wait_recv()
    s_xf.start()
    ring.event(7)
    s_xb.last()
    ring.event(8)
    lax.fori_loop(0, half, x_step, 0)
    ring.event(9)
    lax.fori_loop(half, TG, x_step, 0)
    ring.event(10)

    def expert_of(i):
        return p.z_slot((1 - 2 * lax.rem(i, 2)) * ((i + 1) // 2))

    def put_dw(i):
        slot = lax.rem(i, 2)
        return pltpu.make_async_copy(dw_buf.at[slot], dw_ref.at[expert_of(i)], dw_sems.at[slot])

    def put_dx(i):
        e = expert_of(i)
        return pltpu.make_async_copy(q_buf.at[e], dxs_ref.at[e], dx_sems.at[i])

    put_xf = pltpu.make_async_copy(xf_buf, xf_ref, local_sems.at[0])
    put_wall = pltpu.make_async_copy(wall_buf, wall_ref, local_sems.at[1])

    def backward_step(i, carry):
        @pl.when(i == 2)
        def _():
            ring.event(11)

        @pl.when(i == 3)
        def _():
            s_xf.forward()

        @pl.when(i == 4)
        def _():
            ring.event(12)

        @pl.when(i == 6)
        def _():
            s_xf.last()
            put_xf.start()

        @pl.when(i == 7)
        def _():
            ring.event(13)
            put_wall.start()

        @pl.when(i >= 2)
        def _():
            put_dw(i - 2).wait()

        e = expert_of(i)
        expert_step(xs_buf[e], q_buf[e], wall_buf[e, :width], wall_buf[e, width:], dw_buf.at[lax.rem(i, 2)],
                    q_buf.at[e], dab_ref)
        put_dw(i).start()
        put_dx(i).start()
        return carry

    lax.fori_loop(0, num_local, backward_step, 0)
    put_xf.wait()
    put_wall.wait()
    for i in range(num_local):
        put_dx(jnp.int32(i)).wait()
    put_dw(jnp.int32(num_local - 2)).wait()
    put_dw(jnp.int32(num_local - 1)).wait()
    for s in spread:
        s.finish()
    for hop in hops:
        hop.wait_send()
    ring.finish()


def dispatch_rows(x_acts, ids, gates, dy, w_in, w_up, w_out, capacity, num_stages):
    tokens, width = dy.shape
    hid = w_in.shape[1]
    num_local = 8
    slot_shape = jax.ShapeDtypeStruct((num_local, TG * capacity, width), BF16)
    rg_shape = jax.ShapeDtypeStruct((TG, 16, tokens), F32)
    wall_size = (num_local, width + hid, width)
    any_spec, vmem_spec = pl.BlockSpec(memory_space=pl.ANY), pl.BlockSpec(memory_space=pltpu.VMEM)
    tok_buf = pltpu.VMEM((TG, tokens, width), BF16)
    slot_buf = pltpu.VMEM((num_local, TG * capacity, width), BF16)
    return pl.pallas_call(
        functools.partial(dispatch_kernel, num_stages, capacity),
        in_specs=[any_spec] * 7,
        out_specs=[any_spec] * 4 + [vmem_spec] * 2,
        out_shape=[jax.ShapeDtypeStruct(wall_size, F32), slot_shape,
                   jax.ShapeDtypeStruct((TG, tokens, width), BF16), jax.ShapeDtypeStruct(wall_size, BF16),
                   rg_shape, rg_shape],
        scratch_shapes=[
            tok_buf, tok_buf, tok_buf, pltpu.VMEM((TG,) + ids.shape, jnp.int32),
            pltpu.VMEM((TG,) + gates.shape, F32), pltpu.VMEM((TG, num_local * capacity, tokens), BF16),
            slot_buf, slot_buf, pltpu.VMEM(wall_size, BF16), pltpu.VMEM((2,) + wall_size[1:], F32),
            pltpu.VMEM((TG * capacity, 2 * hid), BF16),
            pltpu.SemaphoreType.DMA((5, 8)), pltpu.SemaphoreType.DMA((5, 8)),
            pltpu.SemaphoreType.DMA((4,)), pltpu.SemaphoreType.DMA((4,)),
            pltpu.SemaphoreType.DMA((2, 14)), pltpu.SemaphoreType.DMA((2, 14)),
            pltpu.SemaphoreType.DMA((4,)), pltpu.SemaphoreType.DMA((2,)), pltpu.SemaphoreType.DMA((num_local,))],
        compiler_params=pltpu.CompilerParams(collective_id=1, has_side_effects=True,
                                             vmem_limit_bytes=63 << 20),
        cost_estimate=pl.CostEstimate(flops=40 * 10 ** 9, bytes_accessed=40 << 20, transcendentals=0),
        name='dispatch_rows',
    )(x_acts, ids, gates, dy, w_in, w_up, w_out)


def gather_kernel(capacity, rg_ref, x_ref, xs_ref, hot_ref):
    fill_onehot(hot_ref, rg_ref[0, 0:8], capacity)
    rows = jnp.dot(hot_ref[...], x_ref[0], preferred_element_type=F32)
    xs_ref[...] = rows.astype(BF16).reshape(xs_ref.shape)


def gather_rows(rg, x_all, capacity):
    groups, tokens, width = x_all.shape
    num_local = 8
    return pl.pallas_call(
        functools.partial(gather_kernel, capacity),
        grid=(groups,),
        in_specs=[pl.BlockSpec((1, 16, tokens), lambda s: (s, 0, 0)),
                  pl.BlockSpec((1, tokens, width), lambda s: (s, 0, 0))],
        out_specs=pl.BlockSpec((num_local, capacity, width), lambda s: (0, s, 0)),
        out_shape=jax.ShapeDtypeStruct((num_local, groups * capacity, width), BF16),
        scratch_shapes=[pltpu.VMEM((num_local * capacity, tokens), BF16)],
        cost_estimate=pl.CostEstimate(flops=2 * groups * num_local * capacity * tokens * width,
                                      bytes_accessed=10 << 20, transcendentals=0),
        name='gather_rows',
    )(rg, x_all)


def forward_kernel(capacity, rg_ref, x_ref, wall_ref, c_ref):
    e = pl.program_id(0)
    x = x_ref[0]
    width = x.shape[1]
    wcat, wout = wall_ref[0, :width], wall_ref[0, width:]
    hid = wout.shape[0]
    pre = jnp.dot(x, wcat, preferred_element_type=F32)
    a, b = pre[:, :hid], pre[:, hid:]
    h = (a * jax.nn.sigmoid(a) * b).astype(BF16)
    o = jnp.dot(h, wout, preferred_element_type=F32)
    for s in range(rg_ref.shape[0]):
        col = gate_column(rg_ref[s, pl.ds(e, 1)], rg_ref[s, pl.ds(8 + e, 1)], capacity)
        c_ref[0, s * capacity:(s + 1) * capacity] = (col * o[s * capacity:(s + 1) * capacity]).astype(BF16)


def expert_forward(rg, xs, wall, hid, capacity):
    num_local, rows, width = xs.shape
    row_block = pl.BlockSpec((1, rows, width), lambda e: (e, 0, 0))
    return pl.pallas_call(
        functools.partial(forward_kernel, capacity),
        grid=(num_local,),
        in_specs=[pl.BlockSpec(rg.shape, lambda e: (0, 0, 0)), row_block,
                  pl.BlockSpec((1,) + wall.shape[1:], lambda e: (e, 0, 0))],
        out_specs=row_block,
        out_shape=jax.ShapeDtypeStruct(xs.shape, BF16),
        cost_estimate=pl.CostEstimate(flops=6 * num_local * rows * width * hid, bytes_accessed=20 << 20,
                                      transcendentals=num_local * rows * hid),
        name='expert_forward',
    )(rg, xs, wall)


def combine_kernel(num_stages, capacity, rg_ref, c_ref, out_ref, hot_ref, side_out, side_in, acc, half_in,
                   up_in, down_in, send_sems, recv_sems):
    p = Peers(num_stages)
    half = acc.shape[1] // 2
    low, high = pl.ds(0, half), pl.ds(half, half)
    greet((p.up, p.down, p.partner))

    def partial_sum(slot):
        fill_onehot(hot_ref, rg_ref[slot, 0:8], capacity)
        start = pl.ds(pl.multiple_of(slot * capacity, 16), capacity)
        rows = c_ref[:, start].reshape(hot_ref.shape[0], c_ref.shape[2])
        return lax.dot_general(hot_ref[...], rows, (((0,), (0,)), ((), ())), preferred_element_type=F32)

    sides = [send(side_out.at[d], side_in.at[d], send_sems.at[d], recv_sems.at[d], p.partner) for d in range(4)]
    far_up = send(acc.at[2, low], half_in.at[0], send_sems.at[4], recv_sems.at[4], p.up)
    far_down = send(acc.at[2, high], half_in.at[1], send_sems.at[5], recv_sems.at[5], p.down)
    up_a = send(acc.at[1, high], up_in.at[high], send_sems.at[6], recv_sems.at[6], p.up)
    up_b = send(acc.at[1, low], up_in.at[low], send_sems.at[7], recv_sems.at[7], p.up)
    down_a = send(acc.at[3, low], down_in.at[low], send_sems.at[8], recv_sems.at[8], p.down)
    down_b = send(acc.at[3, high], down_in.at[high], send_sems.at[9], recv_sems.at[9], p.down)

    def both(d):
        side_out[d] = partial_sum(p.slot(d, True))
        sides[d].start()
        acc[d] = partial_sum(p.slot(d))

    def add_side(d):
        sides[d].wait_recv()
        acc[d] = acc[d] + side_in[d]

    both(2)
    add_side(2)
    far_up.start()
    far_down.start()
    both(1)
    add_side(1)
    up_a.start()
    both(3)
    add_side(3)
    down_a.start()
    both(0)
    add_side(0)
    far_up.wait_recv()
    acc[1, low] = acc[1, low] + half_in[0]
    up_b.start()
    far_down.wait_recv()
    acc[3, high] = acc[3, high] + half_in[1]
    down_b.start()
    up_a.wait_recv()
    up_b.wait_recv()
    down_a.wait_recv()
    down_b.wait_recv()
    out_ref[...] = (acc[0] + up_in[...] + down_in[...]).astype(BF16)
    for copy in sides + [far_up, far_down, up_a, up_b, down_a, down_b]:
        copy.wait_send()


def combine_rows(rg, slots, capacity, num_stages, collective_id):
    num_local, _, width = slots.shape
    tokens = rg.shape[2]
    vmem_spec = pl.BlockSpec(memory_space=pltpu.VMEM)
    return pl.pallas_call(
        functools.partial(combine_kernel, num_stages, capacity),
        in_specs=[vmem_spec, vmem_spec],
        out_specs=vmem_spec,
        out_shape=jax.ShapeDtypeStruct((tokens, width), BF16),
        scratch_shapes=[
            pltpu.VMEM((num_local * capacity, tokens), BF16),
            pltpu.VMEM((4, tokens, width), F32), pltpu.VMEM((4, tokens, width), F32),
            pltpu.VMEM((4, tokens, width), F32), pltpu.VMEM((2, tokens // 2, width), F32),
            pltpu.VMEM((tokens, width), F32), pltpu.VMEM((tokens, width), F32),
            pltpu.SemaphoreType.DMA((10,)), pltpu.SemaphoreType.DMA((10,))],
        compiler_params=pltpu.CompilerParams(collective_id=collective_id, has_side_effects=True,
                                             vmem_limit_bytes=56 << 20),
        cost_estimate=pl.CostEstimate(flops=20 * 10 ** 9, bytes_accessed=8 << 20, transcendentals=0),
        name='combine_rows_%d' % collective_id,
    )(rg, slots)


def solution(mesh):
    group_size = mesh.shape['expert']
    num_stages = mesh.shape['stage']
    to_prev = [((i + 1) % num_stages, i) for i in range(num_stages)]
    rows_of = group_size // TG
    wgt_groups = [[z * TG + r for z in range(rows_of)] for r in range(TG)]

    def device_fn(x_acts, expert_ids, gate_wts, w_in, w_up, w_out, d_out):
        tokens, width = x_acts.shape[2], x_acts.shape[3]
        hid = w_in.shape[3]
        capacity = 96

        def reduce_wgt(arr):
            return lax.psum_scatter(arr, 'expert', axis_index_groups=wgt_groups, scatter_dimension=0, tiled=False)

        ids = jnp.swapaxes(expert_ids[:, 0], 1, 2)
        gates = jnp.swapaxes(gate_wts[:, 0], 1, 2)
        dwall, dxs, xf_all, wall, rg, rg_f = dispatch_rows(
            x_acts[:, 0], ids, gates, d_out[0], w_in[0, 0], w_up[0, 0], w_out[0, 0], capacity, num_stages)
        dwall = reduce_wgt(dwall)
        dx = combine_rows(rg, dxs, capacity, num_stages, 2)
        xf_all, dx = lax.optimization_barrier((xf_all, dx))
        dx = lax.ppermute(dx, 'stage', to_prev)
        xs_f = gather_rows(rg_f, xf_all, capacity)
        c = expert_forward(rg_f, xs_f, wall, hid, capacity)
        y = combine_rows(rg_f, c, capacity, num_stages, 3)
        dwall = dwall.astype(BF16)
        return (y[None], dx[None], dwall[None, None, :width, :hid], dwall[None, None, :width, hid:],
                dwall[None, None, width:])

    tok_spec = P(None, 'stage', 'expert', None)
    w_spec = P('stage', 'expert', None, None)
    row_spec = P('stage', 'expert', None)
    return jax.shard_map(device_fn, mesh=mesh,
                         in_specs=(tok_spec, tok_spec, tok_spec, w_spec, w_spec, w_spec, row_spec),
                         out_specs=(row_spec, row_spec, w_spec, w_spec, w_spec), check_vma=False)
```

```python
import functools

import jax
import jax.numpy as jnp
from jax import lax
from jax.experimental import pallas as pl
from jax.experimental.pallas import tpu as pltpu
from jax.sharding import PartitionSpec as P

TG = 8
F32 = jnp.float32
BF16 = jnp.bfloat16
MESH = pl.DeviceIdType.MESH


def routing_rows(gates, ids, group_rank, num_local):
    tokens = ids.shape[1]
    taken, gate = [], []
    for k in range(num_local):
        hit = ids == group_rank + k * TG
        taken.append(jnp.sum(jnp.where(hit, 1.0, 0.0), axis=0, keepdims=True))
        gate.append(jnp.sum(jnp.where(hit, gates, 0.0), axis=0, keepdims=True))
    taken, gate = jnp.concatenate(taken, axis=0), jnp.concatenate(gate, axis=0)
    lane = lax.broadcasted_iota(jnp.int32, taken.shape, 1)
    count, shift = taken, 1
    while shift < tokens:
        count = count + jnp.where(lane >= shift, pltpu.roll(count, shift, 1), 0.0)
        shift *= 2
    return jnp.where(taken > 0.0, count - 1.0, -1.0), gate


def slot_mask(rank_row, capacity):
    slot = lax.broadcasted_iota(jnp.int32, (capacity, rank_row.shape[1]), 0).astype(F32)
    return slot == rank_row


def fill_onehot(hot_ref, rank, capacity):
    for k in range(rank.shape[0]):
        hit = slot_mask(rank[k:k + 1], capacity)
        hot_ref[k * capacity:(k + 1) * capacity, :] = jnp.where(hit, 1.0, 0.0).astype(BF16)


def gate_column(rank_row, gate_row, capacity):
    hit = slot_mask(rank_row, capacity)
    return jnp.sum(jnp.where(hit, gate_row, 0.0), axis=1, keepdims=True)


class Peers:
    def __init__(self, num_stages, group_size=64):
        stage, me = lax.axis_index('stage'), lax.axis_index('expert')
        self.rank = lax.rem(me, TG)
        self.base = me - self.rank
        self.zpos = self.base // TG
        self.z_size = group_size // TG
        self.z_up = (stage, self.z_slot(1) * TG + self.rank)
        self.z_down = (stage, self.z_slot(-1) * TG + self.rank)
        self.core = lax.rem(self.rank, 2)
        self.ypos = (self.rank - self.core) // 2
        self.own, self.up_slot = self.rank, self.slot(1)
        self.far_slot, self.down_slot = self.slot(2), self.slot(3)
        self.up = (stage, self.base + self.slot(1))
        self.down = (stage, self.base + self.slot(3))
        self.partner = (stage, self.base + self.slot(0, True))
        self.after = (lax.rem(stage + 1, num_stages), me)
        self.before = (lax.rem(stage + num_stages - 1, num_stages), me)

    def z_slot(self, offset):
        return lax.rem(self.zpos + offset + self.z_size, self.z_size)

    def slot(self, offset, other_core=False):
        core = 1 - self.core if other_core else self.core
        return lax.rem(self.ypos + offset, 4) * 2 + core


def greet(devices):
    barrier = pltpu.get_barrier_semaphore()
    for device in devices:
        pl.semaphore_signal(barrier, inc=1, device_id=device, device_id_type=MESH)
    pl.semaphore_wait(barrier, len(devices))


def send(src, dst, send_sem, recv_sem, device):
    return pltpu.make_async_remote_copy(src_ref=src, dst_ref=dst, send_sem=send_sem, recv_sem=recv_sem,
                                        device_id=device, device_id_type=MESH)


class Spread:
    def __init__(self, peers, src, buf, send_sems, recv_sems):
        half = buf.shape[1] // 2
        p = peers

        def copy(i, ref, device, dst=None):
            return send(ref, ref if dst is None else dst, send_sems.at[i], recv_sems.at[i], device)

        own = buf.at[p.own]
        self.own_up = copy(0, src, p.up, own)
        self.own_down = copy(1, src, p.down, own)
        self.fwd_up = copy(2, buf.at[p.down_slot, pl.ds(0, half)], p.up)
        self.fwd_down = copy(3, buf.at[p.up_slot, pl.ds(half, half)], p.down)
        self.own_side = copy(4, src, p.partner, own)
        self.down_side = copy(5, buf.at[p.down_slot], p.partner)
        self.up_side = copy(6, buf.at[p.up_slot], p.partner)
        self.far_side = copy(7, buf.at[p.far_slot], p.partner)

    def start(self):
        self.own_up.start()
        self.own_down.start()
        self.own_side.start()

    def forward(self):
        self.own_up.wait_recv()
        self.fwd_up.start()
        self.down_side.start()
        self.own_down.wait_recv()
        self.fwd_down.start()
        self.up_side.start()

    def last(self):
        self.fwd_up.wait_recv()
        self.fwd_down.wait_recv()
        self.far_side.start()
        for copy in (self.own_side, self.down_side, self.up_side, self.far_side):
            copy.wait_recv()

    def finish(self):
        for copy in (self.own_up, self.own_down, self.fwd_up, self.fwd_down,
                     self.own_side, self.down_side, self.up_side, self.far_side):
            copy.wait_send()


class WeightRing:
    def __init__(self, p, buf, send_sems, recv_sems):
        self.rows = buf.shape[1] // 4
        self.copies = []
        for way, device in ((0, p.z_up), (1, p.z_down)):
            way_copies = []
            for i in range(14):
                step, pos = divmod(i, 4)
                piece = (pos + 2 * way) % 4
                slot = p.z_slot(-step if way == 0 else step)
                ref = buf.at[slot, pl.ds(piece * self.rows, self.rows)]
                way_copies.append(send(ref, ref, send_sems.at[way, i], recv_sems.at[way, i], device))
            self.copies.append(way_copies)

    def start(self):
        for pos in range(4):
            for way in range(2):
                self.copies[way][pos].start()

    def event(self, i):
        for way in range(2):
            self.copies[way][i].wait_recv()
            if i + 4 < 14:
                self.copies[way][i + 4].start()

    def finish(self):
        for way in range(2):
            for copy in self.copies[way]:
                copy.wait_send()


def expert_step(x, q, wcat, wout, dw_ref, dx_ref, dab_ref):
    width, hid = wcat.shape[0], wout.shape[0]
    pre = jnp.dot(x, wcat, preferred_element_type=F32)
    a, b = pre[:, :hid], pre[:, hid:]
    sig = jax.nn.sigmoid(a)
    act = a * sig
    h = (act * b).astype(BF16)
    dw_ref[width:] = lax.dot_general(h, q, (((0,), (0,)), ((), ())), preferred_element_type=F32)
    u = lax.dot_general(q, wout, (((1,), (1,)), ((), ())), preferred_element_type=F32)
    dab_ref[:, :hid] = (u * b * sig * (1.0 + a * (1.0 - sig))).astype(BF16)
    dab_ref[:, hid:] = (u * act).astype(BF16)
    dab = dab_ref[...]
    dw_ref[:width] = lax.dot_general(x, dab, (((0,), (0,)), ((), ())), preferred_element_type=F32)
    dx = lax.dot_general(dab, wcat, (((1,), (1,)), ((), ())), preferred_element_type=F32)
    dx_ref[...] = dx.astype(BF16)


def dispatch_kernel(num_stages, capacity, x_ref, ids_ref, gate_ref, dy_ref, wi_ref, wu_ref, wo_ref,
                    dw_ref, dxs_ref, xf_ref, wall_ref, rgb_ref, rgf_ref,
                    dy_buf, xb_buf, xf_buf, ids_buf, gate_buf, hot_ref, xs_buf, q_buf, wall_buf, dw_buf, dab_ref,
                    send_sems, recv_sems, hop_send, hop_recv, z_send, z_recv, local_sems, dw_sems, dx_sems):
    p = Peers(num_stages)
    num_local = xs_buf.shape[0]
    width, hid = wi_ref.shape
    block = wall_buf.at[p.z_slot(0)]
    keep = [pltpu.make_async_copy(wi_ref, block.at[pl.ds(0, width), pl.ds(0, hid)], local_sems.at[0]),
            pltpu.make_async_copy(wu_ref, block.at[pl.ds(0, width), pl.ds(hid, hid)], local_sems.at[1]),
            pltpu.make_async_copy(wo_ref, block.at[pl.ds(width, hid)], local_sems.at[2])]
    keep_dy = pltpu.make_async_copy(dy_ref, dy_buf.at[p.own], local_sems.at[3])
    for copy in keep:
        copy.start()
    keep_dy.start()
    greet((p.up, p.down, p.partner, p.after, p.before, p.z_up, p.z_down))
    hops = []
    for i, (src, buf) in enumerate(((ids_ref, ids_buf), (gate_ref, gate_buf),
                                    (x_ref.at[0], xb_buf), (x_ref.at[1], xf_buf))):
        hops.append(send(src, buf.at[p.own], hop_send.at[i], hop_recv.at[i], p.after))
    spread = [Spread(p, src, buf, send_sems.at[i], recv_sems.at[i]) for i, (src, buf) in enumerate((
        (ids_buf.at[p.own], ids_buf), (gate_buf.at[p.own], gate_buf), (xb_buf.at[p.own], xb_buf),
        (xf_buf.at[p.own], xf_buf), (dy_ref, dy_buf)))]
    s_ids, s_gate, s_xb, s_xf, s_dy = spread
    ring = WeightRing(p, wall_buf, z_send, z_recv)
    hops[0].start()
    hops[1].start()
    hops[2].start()
    s_dy.start()
    for copy in keep:
        copy.wait()
    ring.start()
    hops[3].start()
    hops[0].wait_recv()
    s_ids.start()
    hops[1].wait_recv()
    s_gate.start()
    ring.event(0)
    ring.event(1)
    s_ids.forward()
    s_gate.forward()
    s_dy.forward()
    hops[2].wait_recv()
    s_xb.start()
    ring.event(2)
    s_ids.last()
    s_gate.last()

    def route_step(s, carry):
        for mb, out in ((0, rgb_ref), (1, rgf_ref)):
            rank, gate = routing_rows(gate_buf[s, mb], ids_buf[s, mb], p.rank, num_local)
            out[s, 0:8] = rank
            out[s, 8:16] = gate
        fill_onehot(hot_ref.at[s], rgb_ref[s, 0:8], capacity)
        return carry

    def rows_of(s):
        return pl.ds(pl.multiple_of(s * capacity, 16), capacity)

    def dy_step(s, carry):
        rows = jnp.dot(hot_ref[s], dy_buf[s], preferred_element_type=F32)
        for k in range(num_local):
            col = gate_column(rgb_ref[s, k:k + 1], rgb_ref[s, 8 + k:9 + k], capacity)
            q_buf[k, rows_of(s)] = (col * rows[k * capacity:(k + 1) * capacity]).astype(BF16)
        return carry

    def x_step(s, carry):
        rows = jnp.dot(hot_ref[s], xb_buf[s], preferred_element_type=F32).astype(BF16)
        for k in range(num_local):
            xs_buf[k, rows_of(s)] = rows[k * capacity:(k + 1) * capacity]
        return carry

    half = TG // 2
    lax.fori_loop(0, half, route_step, 0)
    ring.event(3)
    lax.fori_loop(half, TG, route_step, 0)
    s_dy.last()
    keep_dy.wait()
    ring.event(4)
    lax.fori_loop(0, half, dy_step, 0)
    ring.event(5)
    lax.fori_loop(half, TG, dy_step, 0)
    ring.event(6)
    s_xb.forward()
    hops[3].wait_recv()
    s_xf.start()
    ring.event(7)
    s_xb.last()
    ring.event(8)
    lax.fori_loop(0, half, x_step, 0)
    ring.event(9)
    lax.fori_loop(half, TG, x_step, 0)
    ring.event(10)

    def expert_of(i):
        return p.z_slot((1 - 2 * lax.rem(i, 2)) * ((i + 1) // 2))

    def put_dw(i):
        slot = lax.rem(i, 2)
        return pltpu.make_async_copy(dw_buf.at[slot], dw_ref.at[expert_of(i)], dw_sems.at[slot])

    def put_dx(i):
        e = expert_of(i)
        return pltpu.make_async_copy(q_buf.at[e], dxs_ref.at[e], dx_sems.at[i])

    put_xf = pltpu.make_async_copy(xf_buf, xf_ref, local_sems.at[0])
    put_wall = pltpu.make_async_copy(wall_buf, wall_ref, local_sems.at[1])

    def backward_step(i, carry):
        @pl.when(i == 2)
        def _():
            ring.event(11)

        @pl.when(i == 3)
        def _():
            s_xf.forward()

        @pl.when(i == 4)
        def _():
            ring.event(12)

        @pl.when(i == 6)
        def _():
            s_xf.last()
            put_xf.start()

        @pl.when(i == 7)
        def _():
            ring.event(13)
            put_wall.start()

        @pl.when(i >= 2)
        def _():
            put_dw(i - 2).wait()

        e = expert_of(i)
        expert_step(xs_buf[e], q_buf[e], wall_buf[e, :width], wall_buf[e, width:], dw_buf.at[lax.rem(i, 2)],
                    q_buf.at[e], dab_ref)
        put_dw(i).start()
        put_dx(i).start()
        return carry

    lax.fori_loop(0, num_local, backward_step, 0)
    put_xf.wait()
    put_wall.wait()
    for i in range(num_local):
        put_dx(jnp.int32(i)).wait()
    put_dw(jnp.int32(num_local - 2)).wait()
    put_dw(jnp.int32(num_local - 1)).wait()
    for s in spread:
        s.finish()
    for hop in hops:
        hop.wait_send()
    ring.finish()


def dispatch_rows(x_acts, ids, gates, dy, w_in, w_up, w_out, capacity, num_stages):
    tokens, width = dy.shape
    hid = w_in.shape[1]
    num_local = 8
    slot_shape = jax.ShapeDtypeStruct((num_local, TG * capacity, width), BF16)
    rg_shape = jax.ShapeDtypeStruct((TG, 16, tokens), F32)
    wall_size = (num_local, width + hid, width)
    any_spec, vmem_spec = pl.BlockSpec(memory_space=pl.ANY), pl.BlockSpec(memory_space=pltpu.VMEM)
    tok_buf = pltpu.VMEM((TG, tokens, width), BF16)
    slot_buf = pltpu.VMEM((num_local, TG * capacity, width), BF16)
    return pl.pallas_call(
        functools.partial(dispatch_kernel, num_stages, capacity),
        in_specs=[any_spec] * 7,
        out_specs=[any_spec] * 4 + [vmem_spec] * 2,
        out_shape=[jax.ShapeDtypeStruct(wall_size, F32), slot_shape,
                   jax.ShapeDtypeStruct((TG, tokens, width), BF16), jax.ShapeDtypeStruct(wall_size, BF16),
                   rg_shape, rg_shape],
        scratch_shapes=[
            tok_buf, tok_buf, tok_buf, pltpu.VMEM((TG,) + ids.shape, jnp.int32),
            pltpu.VMEM((TG,) + gates.shape, F32), pltpu.VMEM((TG, num_local * capacity, tokens), BF16),
            slot_buf, slot_buf, pltpu.VMEM(wall_size, BF16), pltpu.VMEM((2,) + wall_size[1:], F32),
            pltpu.VMEM((TG * capacity, 2 * hid), BF16),
            pltpu.SemaphoreType.DMA((5, 8)), pltpu.SemaphoreType.DMA((5, 8)),
            pltpu.SemaphoreType.DMA((4,)), pltpu.SemaphoreType.DMA((4,)),
            pltpu.SemaphoreType.DMA((2, 14)), pltpu.SemaphoreType.DMA((2, 14)),
            pltpu.SemaphoreType.DMA((4,)), pltpu.SemaphoreType.DMA((2,)), pltpu.SemaphoreType.DMA((num_local,))],
        compiler_params=pltpu.CompilerParams(collective_id=1, has_side_effects=True,
                                             vmem_limit_bytes=63 << 20),
        cost_estimate=pl.CostEstimate(flops=40 * 10 ** 9, bytes_accessed=40 << 20, transcendentals=0),
        name='dispatch_rows',
    )(x_acts, ids, gates, dy, w_in, w_up, w_out)


class GradRing:
    def __init__(self, p, part, inbox, send_sems, recv_sems):
        self.part, self.inbox = part, inbox
        self.rows = part.shape[1] // 4
        self.copies, self.target = [], []
        self.home = p.z_slot(0)
        for way, device in ((0, p.z_up), (1, p.z_down)):
            way_copies, way_target = [], []
            for i in range(14):
                step, pos = divmod(i + 2, 4)
                piece = (pos + 2 - 2 * way) % 4
                slot = p.z_slot(4 - step if way == 0 else step - 4)
                src = part.at[slot, pl.ds(piece * self.rows, self.rows)]
                dst = inbox.at[way, pl.ds(i * self.rows, self.rows)]
                way_copies.append(send(src, dst, send_sems.at[way, i], recv_sems.at[way, i], device))
                way_target.append((slot, piece))
            self.copies.append(way_copies)
            self.target.append(way_target)

    def start(self, lo, hi):
        for i in range(lo, hi):
            for way in range(2):
                self.copies[way][i].start()

    def event(self, i):
        for way in range(2):
            self.copies[way][i].wait_recv()
            if i + 4 < 14:
                slot, piece = self.target[way][i + 4]
            else:
                slot, piece = self.home, (i - 10 + 2 - 2 * way) % 4
            rows = pl.ds(piece * self.rows, self.rows)
            self.part[slot, rows] = self.part[slot, rows] + self.inbox[way, pl.ds(i * self.rows, self.rows)]
            if i + 4 < 14:
                self.copies[way][i + 4].start()

    def finish(self):
        for way in range(2):
            for copy in self.copies[way]:
                copy.wait_send()


class Combine:
    def __init__(self, p, partial_sum, side_out, side_in, acc, half_in, up_in, down_in, send_sems, recv_sems):
        half = acc.shape[1] // 2
        self.low, self.high = pl.ds(0, half), pl.ds(half, half)
        low, high = self.low, self.high
        self.p, self.partial_sum = p, partial_sum
        self.side_out, self.side_in, self.acc, self.half_in = side_out, side_in, acc, half_in
        self.up_in, self.down_in = up_in, down_in

        def copy(i, src, dst, device):
            return send(src, dst, send_sems.at[i], recv_sems.at[i], device)

        self.sides = [copy(d, side_out.at[d], side_in.at[d], p.partner) for d in range(4)]
        self.far_up = copy(4, acc.at[2, low], half_in.at[0], p.up)
        self.far_down = copy(5, acc.at[2, high], half_in.at[1], p.down)
        self.up_a = copy(6, acc.at[1, high], up_in.at[high], p.up)
        self.up_b = copy(7, acc.at[1, low], up_in.at[low], p.up)
        self.down_a = copy(8, acc.at[3, low], down_in.at[low], p.down)
        self.down_b = copy(9, acc.at[3, high], down_in.at[high], p.down)

    def both(self, d):
        self.side_out[d] = self.partial_sum(self.p.slot(d, True))
        self.sides[d].start()
        self.acc[d] = self.partial_sum(self.p.slot(d))

    def add_side(self, d):
        self.sides[d].wait_recv()
        self.acc[d] = self.acc[d] + self.side_in[d]

    def start_far(self):
        self.far_up.start()
        self.far_down.start()

    def add_far(self):
        low, high, acc = self.low, self.high, self.acc
        self.far_up.wait_recv()
        acc[1, low] = acc[1, low] + self.half_in[0]
        self.up_b.start()
        self.far_down.wait_recv()
        acc[3, high] = acc[3, high] + self.half_in[1]
        self.down_b.start()

    def total(self):
        for copy in (self.up_a, self.up_b, self.down_a, self.down_b):
            copy.wait_recv()
        return (self.acc[0] + self.up_in[...] + self.down_in[...]).astype(BF16)

    def finish(self):
        for copy in self.sides + [self.far_up, self.far_down, self.up_a, self.up_b, self.down_a, self.down_b]:
            copy.wait_send()


def finish_kernel(num_stages, capacity, dw_ref, dxs_ref, xf_ref, wall_ref, rgb_ref, rgf_ref, out_ref,
                  part, inbox, slots, hot_ref, xf_buf, w_buf, side_out, side_in, acc, half_in, up_in, down_in,
                  stage_dx, stage_y, stage_dw, z_send, z_recv, dx_send, dx_recv, y_send, y_recv, hop_send, hop_recv,
                  load_sems, slot_sem, xf_sems, w_sems, out_sems, credit):
    p = Peers(num_stages)
    num_local = slots.shape[0]
    tokens, width = stage_y.shape
    order = (4, 3, -3, 2, -2, 1, -1, 0)
    loads = []
    for i, off in enumerate(order):
        slot = p.z_slot(off)
        loads.append(pltpu.make_async_copy(dw_ref.at[slot], part.at[slot], load_sems.at[i]))
    load_slots = pltpu.make_async_copy(dxs_ref, slots, slot_sem)
    for load in loads[:3]:
        load.start()
    load_slots.start()
    for load in loads[3:]:
        load.start()
    greet((p.up, p.down, p.partner, p.after, p.before, p.z_up, p.z_down))
    ring = GradRing(p, part, inbox, z_send, z_recv)
    loads[0].wait()
    ring.start(0, 2)
    loads[1].wait()
    loads[2].wait()
    ring.start(2, 4)
    load_slots.wait()

    def rows_of(s):
        return pl.ds(pl.multiple_of(s * capacity, 16), capacity)

    def partial_sum(rg_ref):
        def compute(s):
            fill_onehot(hot_ref, rg_ref[s, 0:8], capacity)
            rows = slots[:, rows_of(s)].reshape(hot_ref.shape[0], width)
            return lax.dot_general(hot_ref[...], rows, (((0,), (0,)), ((), ())), preferred_element_type=F32)
        return compute

    shared = (side_out, side_in, acc, half_in, up_in, down_in)
    dx_sum = Combine(p, partial_sum(rgb_ref), *shared, dx_send, dx_recv)
    y_sum = Combine(p, partial_sum(rgf_ref), *shared, y_send, y_recv)

    def load_xf(s):
        slot = lax.rem(s, 2)
        return pltpu.make_async_copy(xf_ref.at[s], xf_buf.at[slot], xf_sems.at[slot])

    def load_w(e):
        slot = lax.rem(e, 2)
        return pltpu.make_async_copy(wall_ref.at[e], w_buf.at[slot], w_sems.at[slot])

    def gather_step(s, carry):
        @pl.when(s < TG - 1)
        def _():
            load_xf(s + 1).start()

        load_xf(s).wait()
        fill_onehot(hot_ref, rgf_ref[s, 0:8], capacity)
        rows = jnp.dot(hot_ref[...], xf_buf[lax.rem(s, 2)], preferred_element_type=F32).astype(BF16)
        for k in range(num_local):
            slots[k, rows_of(s)] = rows[k * capacity:(k + 1) * capacity]
        return carry

    def forward_step(e, carry):
        @pl.when(e < num_local - 1)
        def _():
            load_w(e + 1).start()

        load_w(e).wait()
        slot = lax.rem(e, 2)
        wcat, wout = w_buf[slot, :width], w_buf[slot, width:]
        hid = wout.shape[0]
        pre = jnp.dot(slots[e], wcat, preferred_element_type=F32)
        a, b = pre[:, :hid], pre[:, hid:]
        h = (a * jax.nn.sigmoid(a) * b).astype(BF16)
        o = jnp.dot(h, wout, preferred_element_type=F32)
        for s in range(TG):
            col = gate_column(rgf_ref[s, pl.ds(e, 1)], rgf_ref[s, pl.ds(8 + e, 1)], capacity)
            slots[e, s * capacity:(s + 1) * capacity] = (col * o[s * capacity:(s + 1) * capacity]).astype(BF16)
        return carry

    load_xf(jnp.int32(0)).start()
    load_w(jnp.int32(0)).start()
    dx_sum.both(2)
    dx_sum.add_side(2)
    dx_sum.start_far()
    dx_sum.both(1)
    dx_sum.add_side(1)
    dx_sum.up_a.start()
    dx_sum.both(3)
    dx_sum.add_side(3)
    dx_sum.down_a.start()
    dx_sum.both(0)
    dx_sum.add_side(0)
    pl.semaphore_signal(credit.at[2], inc=1, device_id=p.partner, device_id_type=MESH)
    for load in loads[3:]:
        load.wait()
    ring.event(0)
    lax.fori_loop(0, 3, gather_step, 0)
    dx_sum.add_far()
    ring.event(1)
    lax.fori_loop(3, TG, gather_step, 0)
    ring.event(2)
    lax.fori_loop(0, 5, forward_step, 0)
    ring.event(3)
    lax.fori_loop(5, num_local, forward_step, 0)
    stage_dx[...] = dx_sum.total()
    hop = send(stage_dx, out_ref.at[pl.ds(tokens, tokens)], hop_send, hop_recv, p.before)
    hop.start()
    pl.semaphore_signal(credit.at[1], inc=1, device_id=p.up, device_id_type=MESH)
    pl.semaphore_signal(credit.at[0], inc=1, device_id=p.down, device_id_type=MESH)
    dx_sum.finish()
    pl.semaphore_wait(credit.at[2], 1)
    y_sum.both(2)
    y_sum.add_side(2)
    pl.semaphore_wait(credit.at[0], 1)
    pl.semaphore_wait(credit.at[1], 1)
    y_sum.start_far()
    ring.event(4)
    y_sum.both(1)
    y_sum.add_side(1)
    y_sum.up_a.start()
    y_sum.both(3)
    y_sum.add_side(3)
    y_sum.down_a.start()
    y_sum.both(0)
    y_sum.add_side(0)
    ring.event(5)
    y_sum.add_far()
    ring.event(6)
    ring.event(7)
    ring.event(8)
    stage_y[...] = y_sum.total()
    put_y = pltpu.make_async_copy(stage_y, out_ref.at[pl.ds(0, tokens)], out_sems.at[0])
    put_y.start()
    for i in range(9, 14):
        ring.event(i)
    stage_dw[...] = part[ring.home].astype(BF16)
    put_dw = pltpu.make_async_copy(stage_dw, out_ref.at[pl.ds(2 * tokens, part.shape[1])], out_sems.at[1])
    put_dw.start()
    put_y.wait()
    hop.wait()
    y_sum.finish()
    ring.finish()
    put_dw.wait()


def finish_rows(dw, dxs, xf_all, wall, rg_b, rg_f, capacity, num_stages):
    num_local, _, width = dxs.shape
    tokens = rg_b.shape[2]
    any_spec, vmem_spec = pl.BlockSpec(memory_space=pl.ANY), pl.BlockSpec(memory_space=pltpu.VMEM)
    dma, quad = pltpu.SemaphoreType.DMA, pltpu.VMEM((4, tokens, width), F32)
    one = pltpu.VMEM((tokens, width), F32)
    return pl.pallas_call(
        functools.partial(finish_kernel, num_stages, capacity),
        in_specs=[any_spec] * 4 + [vmem_spec] * 2,
        out_specs=any_spec,
        out_shape=jax.ShapeDtypeStruct((2 * tokens + dw.shape[1], width), BF16),
        scratch_shapes=[
            pltpu.VMEM(dw.shape, F32), pltpu.VMEM((2, 14 * (dw.shape[1] // 4), width), F32),
            pltpu.VMEM(dxs.shape, BF16), pltpu.VMEM((num_local * capacity, tokens), BF16),
            pltpu.VMEM((2, tokens, width), BF16), pltpu.VMEM((2,) + wall.shape[1:], BF16),
            quad, quad, quad, pltpu.VMEM((2, tokens // 2, width), F32), one, one,
            pltpu.VMEM((tokens, width), BF16), pltpu.VMEM((tokens, width), BF16),
            pltpu.VMEM(dw.shape[1:], BF16),
            dma((2, 14)), dma((2, 14)), dma((10,)), dma((10,)), dma((10,)), dma((10,)), dma, dma,
            dma((8,)), dma, dma((2,)), dma((2,)), dma((2,)), pltpu.SemaphoreType.REGULAR((3,))],
        compiler_params=pltpu.CompilerParams(collective_id=2, has_side_effects=True,
                                             vmem_limit_bytes=63 << 20),
        cost_estimate=pl.CostEstimate(flops=60 * 10 ** 9, bytes_accessed=40 << 20, transcendentals=0),
        name='finish_rows',
    )(dw, dxs, xf_all, wall, rg_b, rg_f)


def solution(mesh):
    num_stages = mesh.shape['stage']

    def device_fn(x_acts, expert_ids, gate_wts, w_in, w_up, w_out, d_out):
        tokens, width = x_acts.shape[2], x_acts.shape[3]
        hid = w_in.shape[3]
        capacity = 96

        ids = jnp.swapaxes(expert_ids[:, 0], 1, 2)
        gates = jnp.swapaxes(gate_wts[:, 0], 1, 2)
        dwall, dxs, xf_all, wall, rg, rg_f = dispatch_rows(
            x_acts[:, 0], ids, gates, d_out[0], w_in[0, 0], w_up[0, 0], w_out[0, 0], capacity, num_stages)
        out = finish_rows(dwall, dxs, xf_all, wall, rg, rg_f, capacity, num_stages)
        y, dx, dw = out[:tokens], out[tokens:2 * tokens], out[2 * tokens:]
        return (y[None], dx[None], dw[None, None, :width, :hid], dw[None, None, :width, hid:],
                dw[None, None, width:])

    tok_spec = P(None, 'stage', 'expert', None)
    w_spec = P('stage', 'expert', None, None)
    row_spec = P('stage', 'expert', None)
    return jax.shard_map(device_fn, mesh=mesh,
                         in_specs=(tok_spec, tok_spec, tok_spec, w_spec, w_spec, w_spec, row_spec),
                         out_specs=(row_spec, row_spec, w_spec, w_spec, w_spec), check_vma=False)
```

```python
import functools

import jax
import jax.numpy as jnp
from jax import lax
from jax.experimental import pallas as pl
from jax.experimental.pallas import tpu as pltpu
from jax.sharding import PartitionSpec as P

TG = 8
F32 = jnp.float32
BF16 = jnp.bfloat16
MESH = pl.DeviceIdType.MESH
EARLY = 5


def routing_rows(gates, ids, group_rank, num_local):
    tokens = ids.shape[1]
    taken, gate = [], []
    for k in range(num_local):
        hit = ids == group_rank + k * TG
        taken.append(jnp.sum(jnp.where(hit, 1.0, 0.0), axis=0, keepdims=True))
        gate.append(jnp.sum(jnp.where(hit, gates, 0.0), axis=0, keepdims=True))
    taken, gate = jnp.concatenate(taken, axis=0), jnp.concatenate(gate, axis=0)
    lane = lax.broadcasted_iota(jnp.int32, taken.shape, 1)
    count, shift = taken, 1
    while shift < tokens:
        count = count + jnp.where(lane >= shift, pltpu.roll(count, shift, 1), 0.0)
        shift *= 2
    return jnp.where(taken > 0.0, count - 1.0, -1.0), gate


def slot_mask(rank_row, capacity):
    slot = lax.broadcasted_iota(jnp.int32, (capacity, rank_row.shape[1]), 0).astype(F32)
    return slot == rank_row


def fill_onehot(hot_ref, rank, capacity):
    for k in range(rank.shape[0]):
        hit = slot_mask(rank[k:k + 1], capacity)
        hot_ref[k * capacity:(k + 1) * capacity, :] = jnp.where(hit, 1.0, 0.0).astype(BF16)


def gate_column(rank_row, gate_row, capacity):
    hit = slot_mask(rank_row, capacity)
    return jnp.sum(jnp.where(hit, gate_row, 0.0), axis=1, keepdims=True)


class Peers:
    def __init__(self, num_stages, group_size=64):
        stage, me = lax.axis_index('stage'), lax.axis_index('expert')
        self.rank = lax.rem(me, TG)
        self.base = me - self.rank
        self.zpos = self.base // TG
        self.z_size = group_size // TG
        self.z_up = (stage, self.z_slot(1) * TG + self.rank)
        self.z_down = (stage, self.z_slot(-1) * TG + self.rank)
        self.core = lax.rem(self.rank, 2)
        self.ypos = (self.rank - self.core) // 2
        self.own, self.up_slot = self.rank, self.slot(1)
        self.far_slot, self.down_slot = self.slot(2), self.slot(3)
        self.up = (stage, self.base + self.slot(1))
        self.down = (stage, self.base + self.slot(3))
        self.partner = (stage, self.base + self.slot(0, True))
        self.after = (lax.rem(stage + 1, num_stages), me)
        self.before = (lax.rem(stage + num_stages - 1, num_stages), me)

    def z_slot(self, offset):
        return lax.rem(self.zpos + offset + self.z_size, self.z_size)

    def expert(self, i):
        return self.z_slot((1 - 2 * lax.rem(i, 2)) * ((i + 1) // 2))

    def arrival(self, j):
        h = j // 2
        offset = h + h // 2 - 2 * (h // 3)
        return lax.rem(self.ypos + offset, 4) * 2 + lax.rem(self.core + lax.rem(j, 2), 2)

    def slot(self, offset, other_core=False):
        core = 1 - self.core if other_core else self.core
        return lax.rem(self.ypos + offset, 4) * 2 + core


def greet(devices):
    barrier = pltpu.get_barrier_semaphore()
    for device in devices:
        pl.semaphore_signal(barrier, inc=1, device_id=device, device_id_type=MESH)
    pl.semaphore_wait(barrier, len(devices))


def send(src, dst, send_sem, recv_sem, device):
    return pltpu.make_async_remote_copy(src_ref=src, dst_ref=dst, send_sem=send_sem, recv_sem=recv_sem,
                                        device_id=device, device_id_type=MESH)


class Spread:
    def __init__(self, peers, src, buf, send_sems, recv_sems):
        half = buf.shape[1] // 2
        p = peers

        def copy(i, ref, device, dst=None):
            return send(ref, ref if dst is None else dst, send_sems.at[i], recv_sems.at[i], device)

        own = buf.at[p.own]
        self.own_up = copy(0, src, p.up, own)
        self.own_down = copy(1, src, p.down, own)
        self.fwd_up = copy(2, buf.at[p.down_slot, pl.ds(0, half)], p.up)
        self.fwd_down = copy(3, buf.at[p.up_slot, pl.ds(half, half)], p.down)
        self.own_side = copy(4, src, p.partner, own)
        self.down_side = copy(5, buf.at[p.down_slot], p.partner)
        self.up_side = copy(6, buf.at[p.up_slot], p.partner)
        self.far_side = copy(7, buf.at[p.far_slot], p.partner)

    def start(self):
        self.own_up.start()
        self.own_down.start()
        self.own_side.start()

    def forward(self):
        self.own_up.wait_recv()
        self.fwd_up.start()
        self.down_side.start()
        self.own_down.wait_recv()
        self.fwd_down.start()
        self.up_side.start()

    def near(self):
        for copy in (self.own_side, self.down_side, self.up_side):
            copy.wait_recv()

    def last(self):
        self.fwd_up.wait_recv()
        self.fwd_down.wait_recv()
        self.far_side.start()
        self.far_side.wait_recv()

    def finish(self):
        for copy in (self.own_up, self.own_down, self.fwd_up, self.fwd_down,
                     self.own_side, self.down_side, self.up_side, self.far_side):
            copy.wait_send()


class WeightRing:
    def __init__(self, p, buf, send_sems, recv_sems):
        self.rows = buf.shape[1] // 4
        self.copies = []
        for way, device in ((0, p.z_up), (1, p.z_down)):
            way_copies = []
            for i in range(14):
                step, pos = divmod(i, 4)
                piece = (pos + 2 * way) % 4
                slot = p.z_slot(-step if way == 0 else step)
                ref = buf.at[slot, pl.ds(piece * self.rows, self.rows)]
                way_copies.append(send(ref, ref, send_sems.at[way, i], recv_sems.at[way, i], device))
            self.copies.append(way_copies)

    def start(self):
        for pos in range(4):
            for way in range(2):
                self.copies[way][pos].start()

    def event(self, i):
        for way in range(2):
            self.copies[way][i].wait_recv()
            if i + 4 < 14:
                self.copies[way][i + 4].start()

    def finish(self):
        for way in range(2):
            for copy in self.copies[way]:
                copy.wait_send()


def expert_step(x, q, wcat, wout, dw_ref, dx_ref, dab_ref):
    width, hid = wcat.shape[0], wout.shape[0]
    pre = jnp.dot(x, wcat, preferred_element_type=F32)
    a, b = pre[:, :hid], pre[:, hid:]
    sig = jax.nn.sigmoid(a)
    act = a * sig
    h = (act * b).astype(BF16)
    dw_ref[width:] = lax.dot_general(h, q, (((0,), (0,)), ((), ())), preferred_element_type=F32)
    u = lax.dot_general(q, wout, (((1,), (1,)), ((), ())), preferred_element_type=F32)
    dab_ref[:, :hid] = (u * b * sig * (1.0 + a * (1.0 - sig))).astype(BF16)
    dab_ref[:, hid:] = (u * act).astype(BF16)
    dab = dab_ref[...]
    dw_ref[:width] = lax.dot_general(x, dab, (((0,), (0,)), ((), ())), preferred_element_type=F32)
    dx = lax.dot_general(dab, wcat, (((1,), (1,)), ((), ())), preferred_element_type=F32)
    dx_ref[...] = dx.astype(BF16)


def dispatch_kernel(num_stages, capacity, x_ref, ids_ref, gate_ref, dy_ref, wi_ref, wu_ref, wo_ref,
                    dw_ref, dxs_ref, xs_ref, xf_ref, wall_ref, rgb_ref, rgf_ref,
                    dy_buf, xb_buf, xf_buf, ids_buf, gate_buf, hot_ref, xs_buf, q_buf, wall_buf, dw_buf, dab_ref,
                    send_sems, recv_sems, hop_send, hop_recv, z_send, z_recv, local_sems, dw_sems, dx_sems,
                    xs_sems, wall_sems):
    p = Peers(num_stages)
    num_local = xs_buf.shape[0]
    width, hid = wi_ref.shape
    block = wall_buf.at[p.z_slot(0)]
    keep = [pltpu.make_async_copy(wi_ref, block.at[pl.ds(0, width), pl.ds(0, hid)], local_sems.at[0]),
            pltpu.make_async_copy(wu_ref, block.at[pl.ds(0, width), pl.ds(hid, hid)], local_sems.at[1]),
            pltpu.make_async_copy(wo_ref, block.at[pl.ds(width, hid)], local_sems.at[2])]
    keep_dy = pltpu.make_async_copy(dy_ref, dy_buf.at[p.own], local_sems.at[3])
    for copy in keep:
        copy.start()
    keep_dy.start()
    greet((p.up, p.down, p.partner, p.after, p.before, p.z_up, p.z_down))
    hops = []
    for i, (src, buf) in enumerate(((ids_ref, ids_buf), (gate_ref, gate_buf),
                                    (x_ref.at[0], xb_buf), (x_ref.at[1], xf_buf))):
        hops.append(send(src, buf.at[p.own], hop_send.at[i], hop_recv.at[i], p.after))
    spread = [Spread(p, src, buf, send_sems.at[i], recv_sems.at[i]) for i, (src, buf) in enumerate((
        (ids_buf.at[p.own], ids_buf), (gate_buf.at[p.own], gate_buf), (xb_buf.at[p.own], xb_buf),
        (xf_buf.at[p.own], xf_buf), (dy_ref, dy_buf)))]
    s_ids, s_gate, s_xb, s_xf, s_dy = spread
    ring = WeightRing(p, wall_buf, z_send, z_recv)
    hops[0].start()
    hops[1].start()
    hops[2].start()
    s_dy.start()
    for copy in keep:
        copy.wait()
    ring.start()

    def put_wall(i):
        e = p.expert(jnp.int32(i))
        return pltpu.make_async_copy(wall_buf.at[e], wall_ref.at[e], wall_sems.at[i])

    put_wall(0).start()
    hops[3].start()
    hops[0].wait_recv()
    s_ids.start()
    hops[1].wait_recv()
    s_gate.start()
    ring.event(0)
    ring.event(1)
    s_ids.forward()
    s_gate.forward()
    s_dy.forward()
    hops[2].wait_recv()
    s_xb.start()
    ring.event(2)
    s_ids.near()
    s_gate.near()
    s_ids.last()
    s_gate.last()

    def route_step(s, carry):
        for mb, out in ((0, rgb_ref), (1, rgf_ref)):
            rank, gate = routing_rows(gate_buf[s, mb], ids_buf[s, mb], p.rank, num_local)
            out[s, 0:8] = rank
            out[s, 8:16] = gate
        fill_onehot(hot_ref.at[s], rgb_ref[s, 0:8], capacity)
        return carry

    def rows_of(s):
        return pl.ds(pl.multiple_of(s * capacity, 16), capacity)

    def dy_step(s, carry):
        rows = jnp.dot(hot_ref[s], dy_buf[s], preferred_element_type=F32)
        for k in range(num_local):
            col = gate_column(rgb_ref[s, k:k + 1], rgb_ref[s, 8 + k:9 + k], capacity)
            q_buf[k, rows_of(s)] = (col * rows[k * capacity:(k + 1) * capacity]).astype(BF16)
        return carry

    def x_step(j, carry):
        s = p.arrival(j)
        rows = jnp.dot(hot_ref[s], xb_buf[s], preferred_element_type=F32).astype(BF16)
        for k in range(num_local):
            xs_buf[k, rows_of(s)] = rows[k * capacity:(k + 1) * capacity]
        return carry

    half = TG // 2
    lax.fori_loop(0, half, route_step, 0)
    ring.event(3)
    put_wall(1).start()
    put_wall(2).start()
    lax.fori_loop(half, TG, route_step, 0)
    s_dy.near()
    s_dy.last()
    keep_dy.wait()
    ring.event(4)
    lax.fori_loop(0, half, dy_step, 0)
    ring.event(5)
    s_xb.forward()
    hops[3].wait_recv()
    s_xf.start()
    ring.event(6)
    lax.fori_loop(half, TG, dy_step, 0)
    ring.event(7)
    put_wall(3).start()
    put_wall(4).start()
    s_xb.near()
    lax.fori_loop(0, 6, x_step, 0)
    ring.event(8)
    s_xb.last()
    lax.fori_loop(6, TG, x_step, 0)
    ring.event(9)
    expert_of = p.expert

    def put_dw(i):
        slot = lax.rem(i, 2)
        return pltpu.make_async_copy(dw_buf.at[slot], dw_ref.at[expert_of(i)], dw_sems.at[slot])

    def put_dx(i):
        e = expert_of(i)
        return pltpu.make_async_copy(q_buf.at[e], dxs_ref.at[e], dx_sems.at[i])

    def put_xs(i):
        return pltpu.make_async_copy(xs_buf.at[expert_of(jnp.int32(i))], xs_ref.at[7 - i], xs_sems.at[7 - i])

    put_xf = pltpu.make_async_copy(xf_buf, xf_ref, local_sems.at[0])
    for i in range(EARLY, num_local):
        put_xs(i).start()
        put_dx(jnp.int32(i)).start()

    def backward_step(i, carry):
        @pl.when(i == 1)
        def _():
            ring.event(10)

        @pl.when(i == 2)
        def _():
            s_xf.forward()
            ring.event(11)
            put_wall(5).start()
            put_wall(6).start()

        @pl.when(i == 4)
        def _():
            ring.event(12)

        @pl.when(i >= 2)
        def _():
            put_dw(i - 2).wait()

        e = expert_of(i)
        expert_step(xs_buf[e], q_buf[e], wall_buf[e, :width], wall_buf[e, width:], dw_buf.at[lax.rem(i, 2)],
                    q_buf.at[e], dab_ref)
        put_dw(i).start()
        put_dx(i).start()
        return carry

    lax.fori_loop(0, EARLY, backward_step, 0)
    s_xf.near()
    s_xf.last()
    put_xf.start()
    ring.event(13)
    put_wall(7).start()
    for i in range(EARLY, num_local):
        put_xs(i).wait()
    for i in range(num_local):
        put_dx(jnp.int32(i)).wait()
    put_dw(jnp.int32(EARLY - 2)).wait()
    put_dw(jnp.int32(EARLY - 1)).wait()
    for s in spread:
        s.finish()
    for hop in hops:
        hop.wait_send()
    ring.finish()
    put_xf.wait()
    for i in range(num_local):
        put_wall(i).wait()


def dispatch_rows(x_acts, ids, gates, dy, w_in, w_up, w_out, capacity, num_stages):
    tokens, width = dy.shape
    hid = w_in.shape[1]
    num_local = 8
    slot_shape = jax.ShapeDtypeStruct((num_local, TG * capacity, width), BF16)
    rg_shape = jax.ShapeDtypeStruct((TG, 16, tokens), F32)
    wall_size = (num_local, width + hid, width)
    any_spec, vmem_spec = pl.BlockSpec(memory_space=pl.ANY), pl.BlockSpec(memory_space=pltpu.VMEM)
    tok_buf = pltpu.VMEM((TG, tokens, width), BF16)
    slot_buf = pltpu.VMEM((num_local, TG * capacity, width), BF16)
    return pl.pallas_call(
        functools.partial(dispatch_kernel, num_stages, capacity),
        in_specs=[any_spec] * 7,
        out_specs=[any_spec] * 5 + [vmem_spec] * 2,
        out_shape=[jax.ShapeDtypeStruct(wall_size, F32), slot_shape,
                   jax.ShapeDtypeStruct((num_local - EARLY,) + slot_shape.shape[1:], BF16),
                   jax.ShapeDtypeStruct((TG, tokens, width), BF16), jax.ShapeDtypeStruct(wall_size, BF16),
                   rg_shape, rg_shape],
        scratch_shapes=[
            tok_buf, tok_buf, tok_buf, pltpu.VMEM((TG,) + ids.shape, jnp.int32),
            pltpu.VMEM((TG,) + gates.shape, F32), pltpu.VMEM((TG, num_local * capacity, tokens), BF16),
            slot_buf, slot_buf, pltpu.VMEM(wall_size, BF16), pltpu.VMEM((2,) + wall_size[1:], F32),
            pltpu.VMEM((TG * capacity, 2 * hid), BF16),
            pltpu.SemaphoreType.DMA((5, 8)), pltpu.SemaphoreType.DMA((5, 8)),
            pltpu.SemaphoreType.DMA((4,)), pltpu.SemaphoreType.DMA((4,)),
            pltpu.SemaphoreType.DMA((2, 14)), pltpu.SemaphoreType.DMA((2, 14)),
            pltpu.SemaphoreType.DMA((4,)), pltpu.SemaphoreType.DMA((2,)), pltpu.SemaphoreType.DMA((num_local,)),
            pltpu.SemaphoreType.DMA((num_local - EARLY,)), pltpu.SemaphoreType.DMA((num_local,))],
        compiler_params=pltpu.CompilerParams(collective_id=1, has_side_effects=True,
                                             vmem_limit_bytes=63 << 20),
        cost_estimate=pl.CostEstimate(flops=40 * 10 ** 9, bytes_accessed=40 << 20, transcendentals=0),
        name='dispatch_rows',
    )(x_acts, ids, gates, dy, w_in, w_up, w_out)


class GradRing:
    def __init__(self, p, part, inbox, send_sems, recv_sems):
        self.part, self.inbox = part, inbox
        self.rows = part.shape[1] // 4
        self.copies, self.target = [], []
        self.home = p.z_slot(0)
        for way, device in ((0, p.z_up), (1, p.z_down)):
            way_copies, way_target = [], []
            for i in range(14):
                step, pos = divmod(i + 2, 4)
                piece = (pos + 2 - 2 * way) % 4
                slot = p.z_slot(4 - step if way == 0 else step - 4)
                src = part.at[slot, pl.ds(piece * self.rows, self.rows)]
                dst = inbox.at[way, pl.ds(i * self.rows, self.rows)]
                way_copies.append(send(src, dst, send_sems.at[way, i], recv_sems.at[way, i], device))
                way_target.append((slot, piece))
            self.copies.append(way_copies)
            self.target.append(way_target)

    def start(self, lo, hi):
        for i in range(lo, hi):
            for way in range(2):
                self.copies[way][i].start()

    def event(self, i):
        for way in range(2):
            self.copies[way][i].wait_recv()
            if i + 4 < 14:
                slot, piece = self.target[way][i + 4]
            else:
                slot, piece = self.home, (i - 10 + 2 - 2 * way) % 4
            rows = pl.ds(piece * self.rows, self.rows)
            self.part[slot, rows] = self.part[slot, rows] + self.inbox[way, pl.ds(i * self.rows, self.rows)]
            if i + 4 < 14:
                self.copies[way][i + 4].start()

    def finish(self):
        for way in range(2):
            for copy in self.copies[way]:
                copy.wait_send()


class Combine:
    def __init__(self, p, partial_sum, side_out, side_in, acc, half_in, up_in, down_in, send_sems, recv_sems):
        half = acc.shape[1] // 2
        self.low, self.high = pl.ds(0, half), pl.ds(half, half)
        low, high = self.low, self.high
        self.p, self.partial_sum = p, partial_sum
        self.side_out, self.side_in, self.acc, self.half_in = side_out, side_in, acc, half_in
        self.up_in, self.down_in = up_in, down_in

        def copy(i, src, dst, device):
            return send(src, dst, send_sems.at[i], recv_sems.at[i], device)

        self.sides = [copy(d, side_out.at[d], side_in.at[d], p.partner) for d in range(4)]
        self.far_up = copy(4, acc.at[2, low], half_in.at[0], p.up)
        self.far_down = copy(5, acc.at[2, high], half_in.at[1], p.down)
        self.up_a = copy(6, acc.at[1, high], up_in.at[high], p.up)
        self.up_b = copy(7, acc.at[1, low], up_in.at[low], p.up)
        self.down_a = copy(8, acc.at[3, low], down_in.at[low], p.down)
        self.down_b = copy(9, acc.at[3, high], down_in.at[high], p.down)

    def both(self, d):
        self.side_out[d] = self.partial_sum(self.p.slot(d, True))
        self.sides[d].start()
        self.acc[d] = self.partial_sum(self.p.slot(d))

    def add_side(self, d):
        self.sides[d].wait_recv()
        self.acc[d] = self.acc[d] + self.side_in[d]

    def start_far(self):
        self.far_up.start()
        self.far_down.start()

    def add_far(self):
        low, high, acc = self.low, self.high, self.acc
        self.far_up.wait_recv()
        acc[1, low] = acc[1, low] + self.half_in[0]
        self.up_b.start()
        self.far_down.wait_recv()
        acc[3, high] = acc[3, high] + self.half_in[1]
        self.down_b.start()

    def total(self):
        for copy in (self.up_a, self.up_b, self.down_a, self.down_b):
            copy.wait_recv()
        return (self.acc[0] + self.up_in[...] + self.down_in[...]).astype(BF16)

    def finish(self):
        for copy in self.sides + [self.far_up, self.far_down, self.up_a, self.up_b, self.down_a, self.down_b]:
            copy.wait_send()


def finish_kernel(num_stages, capacity, dw_ref, dxs_ref, xs_ref, xf_ref, wall_ref, rgb_ref, rgf_ref, out_ref,
                  x_buf, dab_ref, part, inbox, slots, hot_ref, xf_buf, w_buf, side_out, side_in, acc, half_in, up_in, down_in,
                  stage_dx, stage_y, stage_dw, z_send, z_recv, dx_send, dx_recv, y_send, y_recv, hop_send, hop_recv,
                  load_sems, slot_sems, x_sems, xf_sems, w_sems, out_sems, credit):
    p = Peers(num_stages)
    num_local = slots.shape[0]
    tokens, width = stage_y.shape
    late = num_local - EARLY

    def load_late(i):
        slot, e = lax.rem(i, 2), p.expert(7 - i)
        return (pltpu.make_async_copy(wall_ref.at[e], w_buf.at[slot], w_sems.at[slot]),
                pltpu.make_async_copy(xs_ref.at[i], x_buf.at[slot], x_sems.at[slot]))

    def load_slot(i):
        e = p.expert(7 - i)
        return pltpu.make_async_copy(dxs_ref.at[e], slots.at[e], slot_sems.at[i])

    def load_dw(i):
        e = p.expert(jnp.int32(i))
        return pltpu.make_async_copy(dw_ref.at[e], part.at[e], load_sems.at[i])

    for i in range(2):
        load_slot(jnp.int32(i)).start()
        for load in load_late(jnp.int32(i)):
            load.start()
    for i in range(2, num_local):
        load_slot(jnp.int32(i)).start()
    for i in range(EARLY):
        load_dw(EARLY - 1 - i).start()
    greet((p.up, p.down, p.partner, p.after, p.before, p.z_up, p.z_down))
    ring = GradRing(p, part, inbox, z_send, z_recv)

    def late_step(i, carry):
        for load in load_late(i):
            load.wait()
        load_slot(i).wait()
        slot, e = lax.rem(i, 2), p.expert(7 - i)
        expert_step(x_buf[slot], slots[e], w_buf[slot, :width], w_buf[slot, width:], part.at[e], slots.at[e], dab_ref)

        @pl.when(i == 0)
        def _():
            ring.start(0, 2)

        @pl.when(i + 2 < late)
        def _():
            for load in load_late(i + 2):
                load.start()

        return carry

    lax.fori_loop(0, late, late_step, 0)
    ring.start(2, 4)
    for i in range(late, num_local):
        load_slot(jnp.int32(i)).wait()

    def rows_of(s):
        return pl.ds(pl.multiple_of(s * capacity, 16), capacity)

    def partial_sum(rg_ref):
        def compute(s):
            fill_onehot(hot_ref, rg_ref[s, 0:8], capacity)
            rows = slots[:, rows_of(s)].reshape(hot_ref.shape[0], width)
            return lax.dot_general(hot_ref[...], rows, (((0,), (0,)), ((), ())), preferred_element_type=F32)
        return compute

    shared = (side_out, side_in, acc, half_in, up_in, down_in)
    dx_sum = Combine(p, partial_sum(rgb_ref), *shared, dx_send, dx_recv)
    y_sum = Combine(p, partial_sum(rgf_ref), *shared, y_send, y_recv)

    def load_xf(s):
        slot = lax.rem(s, 2)
        return pltpu.make_async_copy(xf_ref.at[s], xf_buf.at[slot], xf_sems.at[slot])

    def load_w(e):
        slot = lax.rem(e, 2)
        return pltpu.make_async_copy(wall_ref.at[e], w_buf.at[slot], w_sems.at[slot])

    def gather_step(s, carry):
        @pl.when(s < TG - 1)
        def _():
            load_xf(s + 1).start()

        load_xf(s).wait()
        fill_onehot(hot_ref, rgf_ref[s, 0:8], capacity)
        rows = jnp.dot(hot_ref[...], xf_buf[lax.rem(s, 2)], preferred_element_type=F32).astype(BF16)
        for k in range(num_local):
            slots[k, rows_of(s)] = rows[k * capacity:(k + 1) * capacity]
        return carry

    def forward_step(e, carry):
        @pl.when(e < num_local - 1)
        def _():
            load_w(e + 1).start()

        load_w(e).wait()
        slot = lax.rem(e, 2)
        wcat, wout = w_buf[slot, :width], w_buf[slot, width:]
        hid = wout.shape[0]
        pre = jnp.dot(slots[e], wcat, preferred_element_type=F32)
        a, b = pre[:, :hid], pre[:, hid:]
        h = (a * jax.nn.sigmoid(a) * b).astype(BF16)
        o = jnp.dot(h, wout, preferred_element_type=F32)
        for s in range(TG):
            col = gate_column(rgf_ref[s, pl.ds(e, 1)], rgf_ref[s, pl.ds(8 + e, 1)], capacity)
            slots[e, s * capacity:(s + 1) * capacity] = (col * o[s * capacity:(s + 1) * capacity]).astype(BF16)
        return carry

    load_xf(jnp.int32(0)).start()
    load_w(jnp.int32(0)).start()
    dx_sum.both(2)
    dx_sum.add_side(2)
    dx_sum.start_far()
    dx_sum.both(1)
    dx_sum.add_side(1)
    dx_sum.up_a.start()
    dx_sum.both(3)
    dx_sum.add_side(3)
    dx_sum.down_a.start()
    dx_sum.both(0)
    dx_sum.add_side(0)
    pl.semaphore_signal(credit.at[2], inc=1, device_id=p.partner, device_id_type=MESH)
    for i in range(EARLY):
        load_dw(i).wait()
    ring.event(0)
    lax.fori_loop(0, 3, gather_step, 0)
    dx_sum.add_far()
    ring.event(1)
    lax.fori_loop(3, TG, gather_step, 0)
    ring.event(2)
    lax.fori_loop(0, 5, forward_step, 0)
    ring.event(3)
    lax.fori_loop(5, num_local, forward_step, 0)
    stage_dx[...] = dx_sum.total()
    hop = send(stage_dx, out_ref.at[pl.ds(tokens, tokens)], hop_send, hop_recv, p.before)
    hop.start()
    pl.semaphore_signal(credit.at[1], inc=1, device_id=p.up, device_id_type=MESH)
    pl.semaphore_signal(credit.at[0], inc=1, device_id=p.down, device_id_type=MESH)
    dx_sum.finish()
    pl.semaphore_wait(credit.at[2], 1)
    y_sum.both(2)
    y_sum.add_side(2)
    pl.semaphore_wait(credit.at[0], 1)
    pl.semaphore_wait(credit.at[1], 1)
    y_sum.start_far()
    ring.event(4)
    y_sum.both(1)
    y_sum.add_side(1)
    y_sum.up_a.start()
    y_sum.both(3)
    y_sum.add_side(3)
    y_sum.down_a.start()
    y_sum.both(0)
    y_sum.add_side(0)
    ring.event(5)
    y_sum.add_far()
    ring.event(6)
    ring.event(7)
    ring.event(8)
    stage_y[...] = y_sum.total()
    put_y = pltpu.make_async_copy(stage_y, out_ref.at[pl.ds(0, tokens)], out_sems.at[0])
    put_y.start()
    for i in range(9, 14):
        ring.event(i)
    stage_dw[...] = part[ring.home].astype(BF16)
    put_dw = pltpu.make_async_copy(stage_dw, out_ref.at[pl.ds(2 * tokens, part.shape[1])], out_sems.at[1])
    put_dw.start()
    put_y.wait()
    hop.wait()
    y_sum.finish()
    ring.finish()
    put_dw.wait()


def finish_rows(dw, dxs, xs_late, xf_all, wall, rg_b, rg_f, capacity, num_stages):
    num_local, _, width = dxs.shape
    tokens = rg_b.shape[2]
    any_spec, vmem_spec = pl.BlockSpec(memory_space=pl.ANY), pl.BlockSpec(memory_space=pltpu.VMEM)
    dma, quad = pltpu.SemaphoreType.DMA, pltpu.VMEM((4, tokens, width), F32)
    one = pltpu.VMEM((tokens, width), F32)
    return pl.pallas_call(
        functools.partial(finish_kernel, num_stages, capacity),
        in_specs=[any_spec] * 5 + [vmem_spec] * 2,
        out_specs=any_spec,
        out_shape=jax.ShapeDtypeStruct((2 * tokens + dw.shape[1], width), BF16),
        scratch_shapes=[
            pltpu.VMEM((2,) + dxs.shape[1:], BF16), pltpu.VMEM((dxs.shape[1], width), BF16),
            pltpu.VMEM(dw.shape, F32), pltpu.VMEM((2, 14 * (dw.shape[1] // 4), width), F32),
            pltpu.VMEM(dxs.shape, BF16), pltpu.VMEM((num_local * capacity, tokens), BF16),
            pltpu.VMEM((2, tokens, width), BF16), pltpu.VMEM((2,) + wall.shape[1:], BF16),
            quad, quad, quad, pltpu.VMEM((2, tokens // 2, width), F32), one, one,
            pltpu.VMEM((tokens, width), BF16), pltpu.VMEM((tokens, width), BF16),
            pltpu.VMEM(dw.shape[1:], BF16),
            dma((2, 14)), dma((2, 14)), dma((10,)), dma((10,)), dma((10,)), dma((10,)), dma, dma,
            dma((EARLY,)), dma((num_local,)), dma((2,)), dma((2,)), dma((2,)), dma((2,)),
            pltpu.SemaphoreType.REGULAR((3,))],
        compiler_params=pltpu.CompilerParams(collective_id=2, has_side_effects=True,
                                             vmem_limit_bytes=63 << 20),
        cost_estimate=pl.CostEstimate(flops=60 * 10 ** 9, bytes_accessed=40 << 20, transcendentals=0),
        name='finish_rows',
    )(dw, dxs, xs_late, xf_all, wall, rg_b, rg_f)


def split_kernel(out_ref, y_ref, dx_ref, wi_ref, wu_ref, wo_ref, buf, in_sems, out_sems):
    tokens, (width, hid) = y_ref.shape[0], wi_ref.shape
    first = 2 * tokens
    spans = ((0, tokens), (tokens, tokens), (first, width), (first + width, hid))
    loads = [pltpu.make_async_copy(out_ref.at[pl.ds(lo, size)], buf.at[pl.ds(lo, size)], in_sems.at[i])
             for i, (lo, size) in enumerate(spans)]
    for load in loads:
        load.start()
    stores = []
    targets = (((0, tokens), (0, width), y_ref), ((tokens, tokens), (0, width), dx_ref),
               ((first, width), (0, hid), wi_ref), ((first, width), (hid, hid), wu_ref),
               ((first + width, hid), (0, width), wo_ref))
    for i, (rows, cols, ref) in enumerate(targets):
        if i != 3:
            loads[min(i, 2) if i < 3 else 3].wait()
        stores.append(pltpu.make_async_copy(buf.at[pl.ds(*rows), pl.ds(*cols)], ref, out_sems.at[i]))
        stores[-1].start()
    for store in stores:
        store.wait()


def split_rows(out, tokens, width, hid):
    any_spec = pl.BlockSpec(memory_space=pl.ANY)
    shapes = ((tokens, width), (tokens, width), (width, hid), (width, hid), (hid, width))
    return pl.pallas_call(
        split_kernel,
        in_specs=[any_spec],
        out_specs=[any_spec] * 5,
        out_shape=[jax.ShapeDtypeStruct(shape, BF16) for shape in shapes],
        scratch_shapes=[pltpu.VMEM(out.shape, BF16), pltpu.SemaphoreType.DMA((4,)), pltpu.SemaphoreType.DMA((5,))],
        name='split_rows',
    )(out)


def solution(mesh):
    num_stages = mesh.shape['stage']

    def device_fn(x_acts, expert_ids, gate_wts, w_in, w_up, w_out, d_out):
        tokens, width = x_acts.shape[2], x_acts.shape[3]
        hid = w_in.shape[3]
        capacity = 96

        ids = jnp.swapaxes(expert_ids[:, 0], 1, 2)
        gates = jnp.swapaxes(gate_wts[:, 0], 1, 2)
        dwall, dxs, xs_late, xf_all, wall, rg, rg_f = dispatch_rows(
            x_acts[:, 0], ids, gates, d_out[0], w_in[0, 0], w_up[0, 0], w_out[0, 0], capacity, num_stages)
        out = finish_rows(dwall, dxs, xs_late, xf_all, wall, rg, rg_f, capacity, num_stages)
        y, dx, dw_in, dw_up, dw_out = split_rows(out, tokens, width, hid)
        return y[None], dx[None], dw_in[None, None], dw_up[None, None], dw_out[None, None]

    tok_spec = P(None, 'stage', 'expert', None)
    w_spec = P('stage', 'expert', None, None)
    row_spec = P('stage', 'expert', None)
    return jax.shard_map(device_fn, mesh=mesh,
                         in_specs=(tok_spec, tok_spec, tok_spec, w_spec, w_spec, w_spec, row_spec),
                         out_specs=(row_spec, row_spec, w_spec, w_spec, w_spec), check_vma=False)
```

```python
import functools

import jax
import jax.numpy as jnp
from jax import lax
from jax.experimental import pallas as pl
from jax.experimental.pallas import tpu as pltpu
from jax.sharding import PartitionSpec as P

TG = 8
F32 = jnp.float32
BF16 = jnp.bfloat16
MESH = pl.DeviceIdType.MESH
EARLY = (2, 3, 4, 5, 6)
LATE = (7, 1, 0)


def routing_rows(gates, ids, group_rank, num_local):
    tokens = ids.shape[1]
    taken, gate = [], []
    for k in range(num_local):
        hit = ids == group_rank + k * TG
        taken.append(jnp.sum(jnp.where(hit, 1.0, 0.0), axis=0, keepdims=True))
        gate.append(jnp.sum(jnp.where(hit, gates, 0.0), axis=0, keepdims=True))
    taken, gate = jnp.concatenate(taken, axis=0), jnp.concatenate(gate, axis=0)
    lane = lax.broadcasted_iota(jnp.int32, taken.shape, 1)
    count, shift = taken, 1
    while shift < tokens:
        count = count + jnp.where(lane >= shift, pltpu.roll(count, shift, 1), 0.0)
        shift *= 2
    return jnp.where(taken > 0.0, count - 1.0, -1.0), gate


def slot_mask(rank_row, capacity):
    slot = lax.broadcasted_iota(jnp.int32, (capacity, rank_row.shape[1]), 0).astype(F32)
    return slot == rank_row


def fill_onehot(hot_ref, rank, capacity):
    for k in range(rank.shape[0]):
        hit = slot_mask(rank[k:k + 1], capacity)
        hot_ref[k * capacity:(k + 1) * capacity, :] = jnp.where(hit, 1.0, 0.0).astype(BF16)


def gate_column(rank_row, gate_row, capacity):
    hit = slot_mask(rank_row, capacity)
    return jnp.sum(jnp.where(hit, gate_row, 0.0), axis=1, keepdims=True)


class Peers:
    def __init__(self, num_stages, group_size=64):
        stage, me = lax.axis_index('stage'), lax.axis_index('expert')
        self.rank = lax.rem(me, TG)
        self.base = me - self.rank
        self.zpos = self.base // TG
        self.z_size = group_size // TG
        self.z_up = (stage, self.z_slot(1) * TG + self.rank)
        self.z_down = (stage, self.z_slot(-1) * TG + self.rank)
        self.core = lax.rem(self.rank, 2)
        self.ypos = (self.rank - self.core) // 2
        self.own, self.up_slot = self.rank, self.slot(1)
        self.far_slot, self.down_slot = self.slot(2), self.slot(3)
        self.up = (stage, self.base + self.slot(1))
        self.down = (stage, self.base + self.slot(3))
        self.partner = (stage, self.base + self.slot(0, True))
        self.after = (lax.rem(stage + 1, num_stages), me)
        self.before = (lax.rem(stage + num_stages - 1, num_stages), me)

    def z_slot(self, offset):
        return lax.rem(self.zpos + offset + self.z_size, self.z_size)

    def expert(self, i):
        return self.z_slot((1 - 2 * lax.rem(i, 2)) * ((i + 1) // 2))

    def arrival(self, j):
        h = j // 2
        offset = h + h // 2 - 2 * (h // 3)
        return lax.rem(self.ypos + offset, 4) * 2 + lax.rem(self.core + lax.rem(j, 2), 2)

    def slot(self, offset, other_core=False):
        core = 1 - self.core if other_core else self.core
        return lax.rem(self.ypos + offset, 4) * 2 + core


def greet(devices):
    barrier = pltpu.get_barrier_semaphore()
    for device in devices:
        pl.semaphore_signal(barrier, inc=1, device_id=device, device_id_type=MESH)
    pl.semaphore_wait(barrier, len(devices))


def send(src, dst, send_sem, recv_sem, device):
    return pltpu.make_async_remote_copy(src_ref=src, dst_ref=dst, send_sem=send_sem, recv_sem=recv_sem,
                                        device_id=device, device_id_type=MESH)


class Spread:
    def __init__(self, peers, src, buf, send_sems, recv_sems):
        half = buf.shape[1] // 2
        p = peers

        def copy(i, ref, device, dst=None):
            return send(ref, ref if dst is None else dst, send_sems.at[i], recv_sems.at[i], device)

        own = buf.at[p.own]
        self.own_up = copy(0, src, p.up, own)
        self.own_down = copy(1, src, p.down, own)
        self.fwd_up = copy(2, buf.at[p.down_slot, pl.ds(0, half)], p.up)
        self.fwd_down = copy(3, buf.at[p.up_slot, pl.ds(half, half)], p.down)
        self.own_side = copy(4, src, p.partner, own)
        self.down_side = copy(5, buf.at[p.down_slot], p.partner)
        self.up_side = copy(6, buf.at[p.up_slot], p.partner)
        self.far_side = copy(7, buf.at[p.far_slot], p.partner)

    def start(self):
        self.own_up.start()
        self.own_down.start()
        self.own_side.start()

    def forward(self):
        self.own_up.wait_recv()
        self.fwd_up.start()
        self.down_side.start()
        self.own_down.wait_recv()
        self.fwd_down.start()
        self.up_side.start()

    def near(self):
        for copy in (self.own_side, self.down_side, self.up_side):
            copy.wait_recv()

    def last(self):
        self.fwd_up.wait_recv()
        self.fwd_down.wait_recv()
        self.far_side.start()
        self.far_side.wait_recv()

    def finish(self):
        for copy in (self.own_up, self.own_down, self.fwd_up, self.fwd_down,
                     self.own_side, self.down_side, self.up_side, self.far_side):
            copy.wait_send()


class WeightRing:
    def __init__(self, p, buf, send_sems, recv_sems):
        self.rows = buf.shape[1] // 4
        self.copies = []
        for way, device in ((0, p.z_up), (1, p.z_down)):
            way_copies = []
            for i in range(14):
                step, pos = divmod(i, 4)
                piece = (pos + 2 * way) % 4
                slot = p.z_slot(-step if way == 0 else step)
                ref = buf.at[slot, pl.ds(piece * self.rows, self.rows)]
                way_copies.append(send(ref, ref, send_sems.at[way, i], recv_sems.at[way, i], device))
            self.copies.append(way_copies)

    def start(self):
        for pos in range(4):
            for way in range(2):
                self.copies[way][pos].start()

    def event(self, i):
        for way in range(2):
            self.copies[way][i].wait_recv()
            if i + 4 < 14:
                self.copies[way][i + 4].start()

    def finish(self):
        for way in range(2):
            for copy in self.copies[way]:
                copy.wait_send()


def expert_step(x, q, wcat, wout, dw_ref, dx_ref, dab_ref):
    width, hid = wcat.shape[0], wout.shape[0]
    pre = jnp.dot(x, wcat, preferred_element_type=F32)
    a, b = pre[:, :hid], pre[:, hid:]
    sig = jax.nn.sigmoid(a)
    act = a * sig
    h = (act * b).astype(BF16)
    dw_ref[width:] = lax.dot_general(h, q, (((0,), (0,)), ((), ())), preferred_element_type=F32)
    u = lax.dot_general(q, wout, (((1,), (1,)), ((), ())), preferred_element_type=F32)
    dab_ref[:, :hid] = (u * b * sig * (1.0 + a * (1.0 - sig))).astype(BF16)
    dab_ref[:, hid:] = (u * act).astype(BF16)
    dab = dab_ref[...]
    dw_ref[:width] = lax.dot_general(x, dab, (((0,), (0,)), ((), ())), preferred_element_type=F32)
    dx = lax.dot_general(dab, wcat, (((1,), (1,)), ((), ())), preferred_element_type=F32)
    dx_ref[...] = dx.astype(BF16)


def dispatch_kernel(num_stages, capacity, x_ref, ids_ref, gate_ref, dy_ref, wi_ref, wu_ref, wo_ref,
                    dw_ref, dxs_ref, xs_ref, xf_ref, wall_ref, rg_ref, ids_out, gate_out,
                    rgb_ref, dy_buf, xb_buf, xf_buf, ids_buf, gate_buf, hot_ref, xs_buf, q_buf, wall_buf, dw_buf, dab_ref,
                    send_sems, recv_sems, hop_send, hop_recv, z_send, z_recv, local_sems, dw_sems, dx_sems,
                    xs_sems, wall_sems, xf_sems, rg_sems):
    p = Peers(num_stages)
    num_local = xs_buf.shape[0]
    width, hid = wi_ref.shape
    block = wall_buf.at[p.z_slot(0)]
    keep = [pltpu.make_async_copy(wi_ref, block.at[pl.ds(0, width), pl.ds(0, hid)], local_sems.at[0]),
            pltpu.make_async_copy(wu_ref, block.at[pl.ds(0, width), pl.ds(hid, hid)], local_sems.at[1]),
            pltpu.make_async_copy(wo_ref, block.at[pl.ds(width, hid)], local_sems.at[2])]
    keep_dy = pltpu.make_async_copy(dy_ref, dy_buf.at[p.own], local_sems.at[3])
    for copy in keep:
        copy.start()
    keep_dy.start()
    greet((p.up, p.down, p.partner, p.after, p.before, p.z_up, p.z_down))
    hops = []
    for i, (src, buf) in enumerate(((ids_ref, ids_buf), (gate_ref, gate_buf),
                                    (x_ref.at[0], xb_buf), (x_ref.at[1], xf_buf))):
        hops.append(send(src, buf.at[p.own], hop_send.at[i], hop_recv.at[i], p.after))
    spread = [Spread(p, src, buf, send_sems.at[i], recv_sems.at[i]) for i, (src, buf) in enumerate((
        (ids_buf.at[p.own], ids_buf), (gate_buf.at[p.own], gate_buf), (xb_buf.at[p.own], xb_buf),
        (xf_buf.at[p.own], xf_buf), (dy_ref, dy_buf)))]
    s_ids, s_gate, s_xb, s_xf, s_dy = spread
    ring = WeightRing(p, wall_buf, z_send, z_recv)
    hops[0].start()
    hops[1].start()
    hops[2].start()
    s_dy.start()
    for copy in keep:
        copy.wait()
    ring.start()

    def put_wall(i):
        e = p.expert(jnp.int32(i))
        return pltpu.make_async_copy(wall_buf.at[e], wall_ref.at[e], wall_sems.at[i])

    put_wall(0).start()
    hops[3].start()
    hops[0].wait_recv()
    s_ids.start()
    hops[1].wait_recv()
    s_gate.start()
    ring.event(0)
    ring.event(1)
    s_ids.forward()
    s_gate.forward()
    s_dy.forward()
    hops[2].wait_recv()
    s_xb.start()
    ring.event(2)
    s_ids.near()
    s_gate.near()
    s_ids.last()
    s_gate.last()

    def route_step(s, carry):
        rank, gate = routing_rows(gate_buf[s, 0], ids_buf[s, 0], p.rank, num_local)
        rgb_ref[s, 0:8] = rank
        rgb_ref[s, 8:16] = gate
        fill_onehot(hot_ref.at[s], rgb_ref[s, 0:8], capacity)
        return carry

    def rows_of(s):
        return pl.ds(pl.multiple_of(s * capacity, 16), capacity)

    def dy_step(s, carry):
        rows = jnp.dot(hot_ref[s], dy_buf[s], preferred_element_type=F32)
        for k in range(num_local):
            col = gate_column(rgb_ref[s, k:k + 1], rgb_ref[s, 8 + k:9 + k], capacity)
            q_buf[k, rows_of(s)] = (col * rows[k * capacity:(k + 1) * capacity]).astype(BF16)
        return carry

    def x_step(j, carry):
        s = p.arrival(j)
        rows = jnp.dot(hot_ref[s], xb_buf[s], preferred_element_type=F32).astype(BF16)
        for k in range(num_local):
            xs_buf[k, rows_of(s)] = rows[k * capacity:(k + 1) * capacity]
        return carry

    half = TG // 2
    lax.fori_loop(0, half, route_step, 0)
    ring.event(3)
    put_wall(1).start()
    put_wall(2).start()
    lax.fori_loop(half, TG, route_step, 0)
    put_rg = [pltpu.make_async_copy(rgb_ref, rg_ref, rg_sems.at[0]),
              pltpu.make_async_copy(ids_buf.at[:, 1], ids_out, rg_sems.at[1]),
              pltpu.make_async_copy(gate_buf.at[:, 1], gate_out, rg_sems.at[2])]
    for copy in put_rg:
        copy.start()
    s_dy.near()
    s_dy.last()
    keep_dy.wait()
    ring.event(4)
    lax.fori_loop(0, half, dy_step, 0)
    ring.event(5)
    s_xb.forward()
    hops[3].wait_recv()
    s_xf.start()
    ring.event(6)
    lax.fori_loop(half, TG, dy_step, 0)
    ring.event(7)
    put_wall(3).start()
    put_wall(4).start()
    s_xb.near()
    lax.fori_loop(0, 6, x_step, 0)
    ring.event(8)
    s_xb.last()
    lax.fori_loop(6, TG, x_step, 0)
    ring.event(9)
    expert_of = p.expert

    def put_dw(i):
        slot = lax.rem(i, 2)
        return pltpu.make_async_copy(dw_buf.at[slot], dw_ref.at[expert_of(i)], dw_sems.at[slot])

    def put_dx(i):
        e = expert_of(i)
        return pltpu.make_async_copy(q_buf.at[e], dxs_ref.at[e], dx_sems.at[i])

    def put_xs(n):
        return pltpu.make_async_copy(xs_buf.at[expert_of(jnp.int32(LATE[n]))], xs_ref.at[n], xs_sems.at[n])

    def put_xf(j):
        s = p.arrival(jnp.int32(j))
        return pltpu.make_async_copy(xf_buf.at[s], xf_ref.at[s], xf_sems.at[j])

    for n in range(len(LATE)):
        put_xs(n).start()
        put_dx(jnp.int32(LATE[n])).start()

    def backward_step(i, carry):
        @pl.when(i == 3)
        def _():
            ring.event(10)

        @pl.when(i == 4)
        def _():
            s_xf.forward()

        @pl.when(i == 5)
        def _():
            ring.event(11)
            put_wall(5).start()
            put_wall(6).start()

        @pl.when(i == 6)
        def _():
            s_xf.near()
            for j in range(6):
                put_xf(j).start()
            ring.event(12)

        @pl.when(i >= EARLY[0] + 2)
        def _():
            put_dw(i - 2).wait()

        e = expert_of(i)
        expert_step(xs_buf[e], q_buf[e], wall_buf[e, :width], wall_buf[e, width:], dw_buf.at[lax.rem(i, 2)],
                    q_buf.at[e], dab_ref)
        put_dw(i).start()
        put_dx(i).start()
        return carry

    lax.fori_loop(EARLY[0], EARLY[-1] + 1, backward_step, 0)
    s_xf.last()
    for j in (6, 7):
        put_xf(j).start()
    ring.event(13)
    put_wall(7).start()
    for n in range(len(LATE)):
        put_xs(n).wait()
    for i in range(num_local):
        put_dx(jnp.int32(i)).wait()
    put_dw(jnp.int32(EARLY[-2])).wait()
    put_dw(jnp.int32(EARLY[-1])).wait()
    for s in spread:
        s.finish()
    for hop in hops:
        hop.wait_send()
    ring.finish()
    for i in range(num_local):
        put_xf(i).wait()
        put_wall(i).wait()
    for copy in put_rg:
        copy.wait()


def dispatch_rows(x_acts, ids, gates, dy, w_in, w_up, w_out, capacity, num_stages):
    tokens, width = dy.shape
    hid = w_in.shape[1]
    num_local = 8
    slot_shape = jax.ShapeDtypeStruct((num_local, TG * capacity, width), BF16)
    rg_shape = jax.ShapeDtypeStruct((TG, 16, tokens), F32)
    wall_size = (num_local, width + hid, width)
    any_spec = pl.BlockSpec(memory_space=pl.ANY)
    tok_buf = pltpu.VMEM((TG, tokens, width), BF16)
    slot_buf = pltpu.VMEM((num_local, TG * capacity, width), BF16)
    return pl.pallas_call(
        functools.partial(dispatch_kernel, num_stages, capacity),
        in_specs=[any_spec] * 7,
        out_specs=[any_spec] * 8,
        out_shape=[jax.ShapeDtypeStruct(wall_size, F32), slot_shape,
                   jax.ShapeDtypeStruct((len(LATE),) + slot_shape.shape[1:], BF16),
                   jax.ShapeDtypeStruct((TG, tokens, width), BF16), jax.ShapeDtypeStruct(wall_size, BF16),
                   rg_shape, jax.ShapeDtypeStruct((TG,) + ids.shape[1:], jnp.int32),
                   jax.ShapeDtypeStruct((TG,) + ids.shape[1:], F32)],
        scratch_shapes=[
            pltpu.VMEM(rg_shape.shape, F32), tok_buf, tok_buf, tok_buf, pltpu.VMEM((TG,) + ids.shape, jnp.int32),
            pltpu.VMEM((TG,) + gates.shape, F32), pltpu.VMEM((TG, num_local * capacity, tokens), BF16),
            slot_buf, slot_buf, pltpu.VMEM(wall_size, BF16), pltpu.VMEM((2,) + wall_size[1:], F32),
            pltpu.VMEM((TG * capacity, 2 * hid), BF16),
            pltpu.SemaphoreType.DMA((5, 8)), pltpu.SemaphoreType.DMA((5, 8)),
            pltpu.SemaphoreType.DMA((4,)), pltpu.SemaphoreType.DMA((4,)),
            pltpu.SemaphoreType.DMA((2, 14)), pltpu.SemaphoreType.DMA((2, 14)),
            pltpu.SemaphoreType.DMA((4,)), pltpu.SemaphoreType.DMA((2,)), pltpu.SemaphoreType.DMA((num_local,)),
            pltpu.SemaphoreType.DMA((len(LATE),)), pltpu.SemaphoreType.DMA((num_local,)),
            pltpu.SemaphoreType.DMA((TG,)), pltpu.SemaphoreType.DMA((3,))],
        compiler_params=pltpu.CompilerParams(collective_id=1, has_side_effects=True,
                                             vmem_limit_bytes=63 << 20),
        cost_estimate=pl.CostEstimate(flops=40 * 10 ** 9, bytes_accessed=40 << 20, transcendentals=0),
        name='dispatch_rows',
    )(x_acts, ids, gates, dy, w_in, w_up, w_out)


class GradRing:
    def __init__(self, p, part, inbox, send_sems, recv_sems):
        self.part, self.inbox = part, inbox
        self.rows = part.shape[1] // 4
        self.copies, self.target = [], []
        self.home = p.z_slot(0)
        for way, device in ((0, p.z_up), (1, p.z_down)):
            way_copies, way_target = [], []
            for i in range(14):
                step, pos = divmod(i + 2, 4)
                piece = (pos + 2 - 2 * way) % 4
                slot = p.z_slot(4 - step if way == 0 else step - 4)
                src = part.at[slot, pl.ds(piece * self.rows, self.rows)]
                dst = inbox.at[way, pl.ds(i * self.rows, self.rows)]
                way_copies.append(send(src, dst, send_sems.at[way, i], recv_sems.at[way, i], device))
                way_target.append((slot, piece))
            self.copies.append(way_copies)
            self.target.append(way_target)

    def start(self, lo, hi):
        for i in range(lo, hi):
            for way in range(2):
                self.copies[way][i].start()

    def event(self, k):
        i = (2, 3, 0, 1, 6, 7, 4, 5, 10, 11, 8, 9, 12, 13)[k]
        for way in range(2):
            self.copies[way][i].wait_recv()
            if i + 4 < 14:
                slot, piece = self.target[way][i + 4]
            else:
                slot, piece = self.home, (i - 10 + 2 - 2 * way) % 4
            rows = pl.ds(piece * self.rows, self.rows)
            self.part[slot, rows] = self.part[slot, rows] + self.inbox[way, pl.ds(i * self.rows, self.rows)]
            if i + 4 < 14:
                self.copies[way][i + 4].start()

    def finish(self):
        for way in range(2):
            for copy in self.copies[way]:
                copy.wait_send()


class Combine:
    def __init__(self, p, partial_sum, side_out, side_in, acc, half_in, up_in, down_in, send_sems, recv_sems):
        half = acc.shape[1] // 2
        self.low, self.high = pl.ds(0, half), pl.ds(half, half)
        low, high = self.low, self.high
        self.p, self.partial_sum = p, partial_sum
        self.side_out, self.side_in, self.acc, self.half_in = side_out, side_in, acc, half_in
        self.up_in, self.down_in = up_in, down_in

        def copy(i, src, dst, device):
            return send(src, dst, send_sems.at[i], recv_sems.at[i], device)

        self.sides = [copy(d, side_out.at[d], side_in.at[d], p.partner) for d in range(4)]
        self.far_up = copy(4, acc.at[2, low], half_in.at[0], p.up)
        self.far_down = copy(5, acc.at[2, high], half_in.at[1], p.down)
        self.up_a = copy(6, acc.at[1, high], up_in.at[high], p.up)
        self.up_b = copy(7, acc.at[1, low], up_in.at[low], p.up)
        self.down_a = copy(8, acc.at[3, low], down_in.at[low], p.down)
        self.down_b = copy(9, acc.at[3, high], down_in.at[high], p.down)

    def both(self, d):
        self.side_out[d] = self.partial_sum(self.p.slot(d, True))
        self.sides[d].start()
        self.acc[d] = self.partial_sum(self.p.slot(d))

    def add_side(self, d):
        self.sides[d].wait_recv()
        self.acc[d] = self.acc[d] + self.side_in[d]

    def start_far(self):
        self.far_up.start()
        self.far_down.start()

    def add_far(self):
        low, high, acc = self.low, self.high, self.acc
        self.far_up.wait_recv()
        acc[1, low] = acc[1, low] + self.half_in[0]
        self.up_b.start()
        self.far_down.wait_recv()
        acc[3, high] = acc[3, high] + self.half_in[1]
        self.down_b.start()

    def total(self):
        for copy in (self.up_a, self.up_b, self.down_a, self.down_b):
            copy.wait_recv()
        return (self.acc[0] + self.up_in[...] + self.down_in[...]).astype(BF16)

    def finish(self):
        for copy in self.sides + [self.far_up, self.far_down, self.up_a, self.up_b, self.down_a, self.down_b]:
            copy.wait_send()


def finish_kernel(num_stages, capacity, dw_ref, dxs_ref, xs_ref, xf_ref, wall_ref, rg_hbm, ids_hbm, gate_hbm, out_ref,
                  rgb_ref, rgf_ref, ids_buf, gate_buf, x_buf, dab_ref, part, inbox, slots, hot_ref, xf_buf, w_buf, side_out, side_in, acc, half_in, up_in, down_in,
                  stage_dx, stage_y, stage_dw, z_send, z_recv, dx_send, dx_recv, y_send, y_recv, hop_send, hop_recv,
                  load_sems, slot_sems, x_sems, xf_sems, w_sems, out_sems, rg_sems, credit):
    p = Peers(num_stages)
    num_local = slots.shape[0]
    tokens, width = stage_y.shape
    def late_number(i):
        return 2 - i + 5 * (1 - (i + 1) // 2)

    def load_late(i):
        slot, e = lax.rem(i, 2), p.expert(late_number(i))
        return (pltpu.make_async_copy(wall_ref.at[e], w_buf.at[slot], w_sems.at[slot]),
                pltpu.make_async_copy(xs_ref.at[i], x_buf.at[slot], x_sems.at[slot]),
                pltpu.make_async_copy(dxs_ref.at[e], slots.at[e], slot_sems.at[i]))

    def load_slot(i):
        e = p.expert(jnp.int32(i))
        return pltpu.make_async_copy(dxs_ref.at[e], slots.at[e], slot_sems.at[i + 1])

    def load_dw(i):
        e = p.expert(jnp.int32(i))
        return pltpu.make_async_copy(dw_ref.at[e], part.at[e], load_sems.at[i])

    load_rg = [pltpu.make_async_copy(rg_hbm, rgb_ref, rg_sems.at[0]),
               pltpu.make_async_copy(ids_hbm, ids_buf, rg_sems.at[1]),
               pltpu.make_async_copy(gate_hbm, gate_buf, rg_sems.at[2])]
    load_dw(5).start()
    load_dw(6).start()
    for i in range(2):
        for load in load_late(jnp.int32(i)):
            load.start()
    for load in load_rg:
        load.start()
    for i in EARLY:
        load_slot(i).start()
    for i in EARLY[:-2]:
        load_dw(i).start()
    greet((p.up, p.down, p.partner, p.after, p.before, p.z_up, p.z_down))
    ring = GradRing(p, part, inbox, z_send, z_recv)

    load_dw(5).wait()
    load_dw(6).wait()
    ring.start(2, 4)

    def late_step(i, carry):
        for load in load_late(i):
            load.wait()
        slot, e = lax.rem(i, 2), p.expert(late_number(i))
        expert_step(x_buf[slot], slots[e], w_buf[slot, :width], w_buf[slot, width:], part.at[e], slots.at[e], dab_ref)

        @pl.when(i == 0)
        def _():
            ring.start(0, 2)
            for load in load_late(i + 2):
                load.start()

        return carry

    lax.fori_loop(0, len(LATE), late_step, 0)
    for load in load_rg:
        load.wait()
    for i in EARLY:
        load_slot(i).wait()

    def rows_of(s):
        return pl.ds(pl.multiple_of(s * capacity, 16), capacity)

    def partial_sum(rg_ref):
        def compute(s):
            fill_onehot(hot_ref, rg_ref[s, 0:8], capacity)
            rows = slots[:, rows_of(s)].reshape(hot_ref.shape[0], width)
            return lax.dot_general(hot_ref[...], rows, (((0,), (0,)), ((), ())), preferred_element_type=F32)
        return compute

    shared = (side_out, side_in, acc, half_in, up_in, down_in)
    dx_sum = Combine(p, partial_sum(rgb_ref), *shared, dx_send, dx_recv)
    y_sum = Combine(p, partial_sum(rgf_ref), *shared, y_send, y_recv)

    def load_xf(s):
        slot = lax.rem(s, 2)
        return pltpu.make_async_copy(xf_ref.at[s], xf_buf.at[slot], xf_sems.at[slot])

    def load_w(e):
        slot = lax.rem(e, 2)
        return pltpu.make_async_copy(wall_ref.at[e], w_buf.at[slot], w_sems.at[slot])

    def route_step(s, carry):
        rank, gate = routing_rows(gate_buf[s], ids_buf[s], p.rank, num_local)
        rgf_ref[s, 0:8] = rank
        rgf_ref[s, 8:16] = gate
        return carry

    def gather_step(s, carry):
        @pl.when(s < TG - 1)
        def _():
            load_xf(s + 1).start()

        load_xf(s).wait()
        fill_onehot(hot_ref, rgf_ref[s, 0:8], capacity)
        rows = jnp.dot(hot_ref[...], xf_buf[lax.rem(s, 2)], preferred_element_type=F32).astype(BF16)
        for k in range(num_local):
            slots[k, rows_of(s)] = rows[k * capacity:(k + 1) * capacity]
        return carry

    def forward_step(e, carry):
        @pl.when(e < num_local - 1)
        def _():
            load_w(e + 1).start()

        load_w(e).wait()
        slot = lax.rem(e, 2)
        wcat, wout = w_buf[slot, :width], w_buf[slot, width:]
        hid = wout.shape[0]
        pre = jnp.dot(slots[e], wcat, preferred_element_type=F32)
        a, b = pre[:, :hid], pre[:, hid:]
        h = (a * jax.nn.sigmoid(a) * b).astype(BF16)
        o = jnp.dot(h, wout, preferred_element_type=F32)
        for s in range(TG):
            col = gate_column(rgf_ref[s, pl.ds(e, 1)], rgf_ref[s, pl.ds(8 + e, 1)], capacity)
            slots[e, s * capacity:(s + 1) * capacity] = (col * o[s * capacity:(s + 1) * capacity]).astype(BF16)
        return carry

    load_xf(jnp.int32(0)).start()
    load_w(jnp.int32(0)).start()
    dx_sum.both(2)
    dx_sum.add_side(2)
    dx_sum.start_far()
    dx_sum.both(1)
    dx_sum.add_side(1)
    dx_sum.up_a.start()
    dx_sum.both(3)
    dx_sum.add_side(3)
    dx_sum.down_a.start()
    dx_sum.both(0)
    dx_sum.add_side(0)
    pl.semaphore_signal(credit.at[2], inc=1, device_id=p.partner, device_id_type=MESH)
    for i in EARLY[:-2]:
        load_dw(i).wait()
    ring.event(0)
    lax.fori_loop(0, TG, route_step, 0)
    lax.fori_loop(0, 3, gather_step, 0)
    dx_sum.add_far()
    ring.event(1)
    lax.fori_loop(3, TG, gather_step, 0)
    ring.event(2)
    lax.fori_loop(0, 5, forward_step, 0)
    ring.event(3)
    lax.fori_loop(5, num_local, forward_step, 0)
    stage_dx[...] = dx_sum.total()
    hop = send(stage_dx, out_ref.at[pl.ds(tokens, tokens)], hop_send, hop_recv, p.before)
    hop.start()
    pl.semaphore_signal(credit.at[1], inc=1, device_id=p.up, device_id_type=MESH)
    pl.semaphore_signal(credit.at[0], inc=1, device_id=p.down, device_id_type=MESH)
    dx_sum.finish()
    pl.semaphore_wait(credit.at[2], 1)
    y_sum.both(2)
    y_sum.add_side(2)
    pl.semaphore_wait(credit.at[0], 1)
    pl.semaphore_wait(credit.at[1], 1)
    y_sum.start_far()
    ring.event(4)
    y_sum.both(1)
    y_sum.add_side(1)
    y_sum.up_a.start()
    y_sum.both(3)
    y_sum.add_side(3)
    y_sum.down_a.start()
    y_sum.both(0)
    y_sum.add_side(0)
    ring.event(5)
    y_sum.add_far()
    ring.event(6)
    ring.event(7)
    ring.event(8)
    stage_y[...] = y_sum.total()
    put_y = pltpu.make_async_copy(stage_y, out_ref.at[pl.ds(0, tokens)], out_sems.at[0])
    put_y.start()
    for i in range(9, 12):
        ring.event(i)
    puts = []
    for i in range(2):
        ring.event(12 + i)
        for piece in (i, i + 2):
            rows = pl.ds(piece * ring.rows, ring.rows)
            stage_dw[rows] = part[ring.home, rows].astype(BF16)
            puts.append(pltpu.make_async_copy(
                stage_dw.at[rows], out_ref.at[pl.ds(2 * tokens + piece * ring.rows, ring.rows)],
                out_sems.at[1 + piece]))
            puts[-1].start()
    put_y.wait()
    hop.wait()
    y_sum.finish()
    ring.finish()
    for put in puts:
        put.wait()


def finish_rows(dw, dxs, xs_late, xf_all, wall, rg, ids, gates, capacity, num_stages):
    num_local, _, width = dxs.shape
    tokens = rg.shape[2]
    any_spec = pl.BlockSpec(memory_space=pl.ANY)
    dma, quad = pltpu.SemaphoreType.DMA, pltpu.VMEM((4, tokens, width), F32)
    one = pltpu.VMEM((tokens, width), F32)
    return pl.pallas_call(
        functools.partial(finish_kernel, num_stages, capacity),
        in_specs=[any_spec] * 8,
        out_specs=any_spec,
        out_shape=jax.ShapeDtypeStruct((2 * tokens + dw.shape[1], width), BF16),
        scratch_shapes=[
            pltpu.VMEM(rg.shape, F32), pltpu.VMEM(rg.shape, F32), pltpu.VMEM(ids.shape, jnp.int32),
            pltpu.VMEM(gates.shape, F32), pltpu.VMEM((2,) + dxs.shape[1:], BF16), pltpu.VMEM((dxs.shape[1], width), BF16),
            pltpu.VMEM(dw.shape, F32), pltpu.VMEM((2, 14 * (dw.shape[1] // 4), width), F32),
            pltpu.VMEM(dxs.shape, BF16), pltpu.VMEM((num_local * capacity, tokens), BF16),
            pltpu.VMEM((2, tokens, width), BF16), pltpu.VMEM((2,) + wall.shape[1:], BF16),
            quad, quad, quad, pltpu.VMEM((2, tokens // 2, width), F32), one, one,
            pltpu.VMEM((tokens, width), BF16), pltpu.VMEM((tokens, width), BF16),
            pltpu.VMEM(dw.shape[1:], BF16),
            dma((2, 14)), dma((2, 14)), dma((10,)), dma((10,)), dma((10,)), dma((10,)), dma, dma,
            dma((num_local,)), dma((num_local,)), dma((2,)), dma((2,)), dma((2,)), dma((5,)),
            dma((3,)), pltpu.SemaphoreType.REGULAR((3,))],
        compiler_params=pltpu.CompilerParams(collective_id=2, has_side_effects=True,
                                             vmem_limit_bytes=63 << 20),
        cost_estimate=pl.CostEstimate(flops=60 * 10 ** 9, bytes_accessed=40 << 20, transcendentals=0),
        name='finish_rows',
    )(dw, dxs, xs_late, xf_all, wall, rg, ids, gates)


def split_kernel(out_ref, y_ref, dx_ref, wi_ref, wu_ref, wo_ref, buf, in_sems, out_sems):
    tokens, (width, hid) = y_ref.shape[0], wi_ref.shape
    first = 2 * tokens
    spans = ((0, tokens), (tokens, tokens), (first, width), (first + width, hid))
    loads = [pltpu.make_async_copy(out_ref.at[pl.ds(lo, size)], buf.at[pl.ds(lo, size)], in_sems.at[i])
             for i, (lo, size) in enumerate(spans)]
    for load in loads:
        load.start()
    stores = []
    targets = (((0, tokens), (0, width), y_ref), ((tokens, tokens), (0, width), dx_ref),
               ((first, width), (0, hid), wi_ref), ((first, width), (hid, hid), wu_ref),
               ((first + width, hid), (0, width), wo_ref))
    for i, (rows, cols, ref) in enumerate(targets):
        if i != 3:
            loads[min(i, 2) if i < 3 else 3].wait()
        stores.append(pltpu.make_async_copy(buf.at[pl.ds(*rows), pl.ds(*cols)], ref, out_sems.at[i]))
        stores[-1].start()
    for store in stores:
        store.wait()


def split_rows(out, tokens, width, hid):
    any_spec = pl.BlockSpec(memory_space=pl.ANY)
    shapes = ((tokens, width), (tokens, width), (width, hid), (width, hid), (hid, width))
    return pl.pallas_call(
        split_kernel,
        in_specs=[any_spec],
        out_specs=[any_spec] * 5,
        out_shape=[jax.ShapeDtypeStruct(shape, BF16) for shape in shapes],
        scratch_shapes=[pltpu.VMEM(out.shape, BF16), pltpu.SemaphoreType.DMA((4,)), pltpu.SemaphoreType.DMA((5,))],
        name='split_rows',
    )(out)


def solution(mesh):
    num_stages = mesh.shape['stage']

    def device_fn(x_acts, expert_ids, gate_wts, w_in, w_up, w_out, d_out):
        tokens, width = x_acts.shape[2], x_acts.shape[3]
        hid = w_in.shape[3]
        capacity = 96

        ids = jnp.swapaxes(expert_ids[:, 0], 1, 2)
        gates = jnp.swapaxes(gate_wts[:, 0], 1, 2)
        dwall, dxs, xs_late, xf_all, wall, rg, ids, gates = dispatch_rows(
            x_acts[:, 0], ids, gates, d_out[0], w_in[0, 0], w_up[0, 0], w_out[0, 0], capacity, num_stages)
        out = finish_rows(dwall, dxs, xs_late, xf_all, wall, rg, ids, gates, capacity, num_stages)
        y, dx, dw_in, dw_up, dw_out = split_rows(out, tokens, width, hid)
        return y[None], dx[None], dw_in[None, None], dw_up[None, None], dw_out[None, None]

    tok_spec = P(None, 'stage', 'expert', None)
    w_spec = P('stage', 'expert', None, None)
    row_spec = P('stage', 'expert', None)
    return jax.shard_map(device_fn, mesh=mesh,
                         in_specs=(tok_spec, tok_spec, tok_spec, w_spec, w_spec, w_spec, row_spec),
                         out_specs=(row_spec, row_spec, w_spec, w_spec, w_spec), check_vma=False)
```

```python
import functools

import jax
import jax.numpy as jnp
from jax import lax
from jax.experimental import pallas as pl
from jax.experimental.pallas import tpu as pltpu
from jax.sharding import PartitionSpec as P

TG = 8
F32 = jnp.float32
BF16 = jnp.bfloat16
MESH = pl.DeviceIdType.MESH
EARLY = (2, 3, 4, 5, 6)
LATE = (7, 1, 0)


def routing_rows(gates, ids, group_rank, num_local):
    tokens = ids.shape[1]
    taken, gate = [], []
    for k in range(num_local):
        hit = ids == group_rank + k * TG
        taken.append(jnp.sum(jnp.where(hit, 1.0, 0.0), axis=0, keepdims=True))
        gate.append(jnp.sum(jnp.where(hit, gates, 0.0), axis=0, keepdims=True))
    taken, gate = jnp.concatenate(taken, axis=0), jnp.concatenate(gate, axis=0)
    lane = lax.broadcasted_iota(jnp.int32, taken.shape, 1)
    count, shift = taken, 1
    while shift < tokens:
        count = count + jnp.where(lane >= shift, pltpu.roll(count, shift, 1), 0.0)
        shift *= 2
    return jnp.where(taken > 0.0, count - 1.0, -1.0), gate


def slot_mask(rank_row, capacity):
    slot = lax.broadcasted_iota(jnp.int32, (capacity, rank_row.shape[1]), 0).astype(F32)
    return slot == rank_row


def fill_onehot(hot_ref, rank, capacity):
    for k in range(rank.shape[0]):
        hit = slot_mask(rank[k:k + 1], capacity)
        hot_ref[k * capacity:(k + 1) * capacity, :] = jnp.where(hit, 1.0, 0.0).astype(BF16)


def gate_column(rank_row, gate_row, capacity):
    hit = slot_mask(rank_row, capacity)
    return jnp.sum(jnp.where(hit, gate_row, 0.0), axis=1, keepdims=True)


class Peers:
    def __init__(self, num_stages, group_size=64):
        stage, me = lax.axis_index('stage'), lax.axis_index('expert')
        self.rank = lax.rem(me, TG)
        self.base = me - self.rank
        self.zpos = self.base // TG
        self.z_size = group_size // TG
        self.z_up = (stage, self.z_slot(1) * TG + self.rank)
        self.z_down = (stage, self.z_slot(-1) * TG + self.rank)
        self.core = lax.rem(self.rank, 2)
        self.ypos = (self.rank - self.core) // 2
        self.own, self.up_slot = self.rank, self.slot(1)
        self.far_slot, self.down_slot = self.slot(2), self.slot(3)
        self.up = (stage, self.base + self.slot(1))
        self.down = (stage, self.base + self.slot(3))
        self.partner = (stage, self.base + self.slot(0, True))
        self.after = (lax.rem(stage + 1, num_stages), me)
        self.before = (lax.rem(stage + num_stages - 1, num_stages), me)

    def z_slot(self, offset):
        return lax.rem(self.zpos + offset + self.z_size, self.z_size)

    def expert(self, i):
        return self.z_slot((1 - 2 * lax.rem(i, 2)) * ((i + 1) // 2))

    def arrival(self, j):
        h = j // 2
        offset = h + h // 2 - 2 * (h // 3)
        return lax.rem(self.ypos + offset, 4) * 2 + lax.rem(self.core + lax.rem(j, 2), 2)

    def slot(self, offset, other_core=False):
        core = 1 - self.core if other_core else self.core
        return lax.rem(self.ypos + offset, 4) * 2 + core


def greet(devices):
    barrier = pltpu.get_barrier_semaphore()
    for device in devices:
        pl.semaphore_signal(barrier, inc=1, device_id=device, device_id_type=MESH)
    pl.semaphore_wait(barrier, len(devices))


def send(src, dst, send_sem, recv_sem, device):
    return pltpu.make_async_remote_copy(src_ref=src, dst_ref=dst, send_sem=send_sem, recv_sem=recv_sem,
                                        device_id=device, device_id_type=MESH)


class Spread:
    def __init__(self, peers, src, buf, send_sems, recv_sems):
        half = buf.shape[1] // 2
        p = peers

        def copy(i, ref, device, dst=None):
            return send(ref, ref if dst is None else dst, send_sems.at[i], recv_sems.at[i], device)

        own = buf.at[p.own]
        self.own_up = copy(0, src, p.up, own)
        self.own_down = copy(1, src, p.down, own)
        self.fwd_up = copy(2, buf.at[p.down_slot, pl.ds(0, half)], p.up)
        self.fwd_down = copy(3, buf.at[p.up_slot, pl.ds(half, half)], p.down)
        self.own_side = copy(4, src, p.partner, own)
        self.down_side = copy(5, buf.at[p.down_slot], p.partner)
        self.up_side = copy(6, buf.at[p.up_slot], p.partner)
        self.far_side = copy(7, buf.at[p.far_slot], p.partner)

    def start(self):
        self.own_up.start()
        self.own_down.start()
        self.own_side.start()

    def forward(self):
        self.own_up.wait_recv()
        self.fwd_up.start()
        self.down_side.start()
        self.own_down.wait_recv()
        self.fwd_down.start()
        self.up_side.start()

    def near(self):
        for copy in (self.own_side, self.down_side, self.up_side):
            copy.wait_recv()

    def last(self):
        self.fwd_up.wait_recv()
        self.fwd_down.wait_recv()
        self.far_side.start()
        self.far_side.wait_recv()

    def finish(self):
        for copy in (self.own_up, self.own_down, self.fwd_up, self.fwd_down,
                     self.own_side, self.down_side, self.up_side, self.far_side):
            copy.wait_send()


class WeightRing:
    def __init__(self, p, buf, send_sems, recv_sems):
        self.rows = buf.shape[1] // 4
        self.copies = []
        for way, device in ((0, p.z_up), (1, p.z_down)):
            way_copies = []
            for i in range(14):
                step, pos = divmod(i, 4)
                piece = (pos + 2 * way) % 4
                slot = p.z_slot(-step if way == 0 else step)
                ref = buf.at[slot, pl.ds(piece * self.rows, self.rows)]
                way_copies.append(send(ref, ref, send_sems.at[way, i], recv_sems.at[way, i], device))
            self.copies.append(way_copies)

    def start(self):
        for pos in range(4):
            for way in range(2):
                self.copies[way][pos].start()

    def event(self, i):
        for way in range(2):
            self.copies[way][i].wait_recv()
            if i + 4 < 14:
                self.copies[way][i + 4].start()

    def finish(self):
        for way in range(2):
            for copy in self.copies[way]:
                copy.wait_send()


def expert_step(x, q, wcat, wout, dw_ref, dx_ref, dab_ref):
    width, hid = wcat.shape[0], wout.shape[0]
    pre = jnp.dot(x, wcat, preferred_element_type=F32)
    a, b = pre[:, :hid], pre[:, hid:]
    sig = jax.nn.sigmoid(a)
    act = a * sig
    h = (act * b).astype(BF16)
    dw_ref[width:] = lax.dot_general(h, q, (((0,), (0,)), ((), ())), preferred_element_type=F32)
    u = lax.dot_general(q, wout, (((1,), (1,)), ((), ())), preferred_element_type=F32)
    dab_ref[:, :hid] = (u * b * sig * (1.0 + a * (1.0 - sig))).astype(BF16)
    dab_ref[:, hid:] = (u * act).astype(BF16)
    dab = dab_ref[...]
    dw_ref[:width] = lax.dot_general(x, dab, (((0,), (0,)), ((), ())), preferred_element_type=F32)
    dx = lax.dot_general(dab, wcat, (((1,), (1,)), ((), ())), preferred_element_type=F32)
    dx_ref[...] = dx.astype(BF16)


def dispatch_kernel(num_stages, capacity, x_ref, ids_ref, gate_ref, dy_ref, wi_ref, wu_ref, wo_ref,
                    dw_ref, dxs_ref, xs_ref, xf_ref, wall_ref, rg_ref, ids_out, gate_out,
                    rgb_ref, dy_buf, xb_buf, xf_buf, ids_buf, gate_buf, hot_ref, xs_buf, q_buf, wall_buf, dw_buf, dab_ref,
                    send_sems, recv_sems, hop_send, hop_recv, z_send, z_recv, local_sems, dw_sems, dx_sems,
                    xs_sems, wall_sems, xf_sems, rg_sems):
    p = Peers(num_stages)
    num_local = xs_buf.shape[0]
    width, hid = wi_ref.shape
    block = wall_buf.at[p.z_slot(0)]
    keep = [pltpu.make_async_copy(wi_ref, block.at[pl.ds(0, width), pl.ds(0, hid)], local_sems.at[0]),
            pltpu.make_async_copy(wu_ref, block.at[pl.ds(0, width), pl.ds(hid, hid)], local_sems.at[1]),
            pltpu.make_async_copy(wo_ref, block.at[pl.ds(width, hid)], local_sems.at[2])]
    keep_dy = pltpu.make_async_copy(dy_ref, dy_buf.at[p.own], local_sems.at[3])
    for copy in keep:
        copy.start()
    keep_dy.start()
    greet((p.up, p.down, p.partner, p.after, p.before, p.z_up, p.z_down))
    hops = []
    for i, (src, buf) in enumerate(((ids_ref, ids_buf), (gate_ref, gate_buf),
                                    (x_ref.at[0], xb_buf), (x_ref.at[1], xf_buf))):
        hops.append(send(src, buf.at[p.own], hop_send.at[i], hop_recv.at[i], p.after))
    spread = [Spread(p, src, buf, send_sems.at[i], recv_sems.at[i]) for i, (src, buf) in enumerate((
        (ids_buf.at[p.own], ids_buf), (gate_buf.at[p.own], gate_buf), (xb_buf.at[p.own], xb_buf),
        (xf_buf.at[p.own], xf_buf), (dy_ref, dy_buf)))]
    s_ids, s_gate, s_xb, s_xf, s_dy = spread
    ring = WeightRing(p, wall_buf, z_send, z_recv)
    hops[0].start()
    hops[1].start()
    hops[2].start()
    s_dy.start()
    for copy in keep:
        copy.wait()
    ring.start()

    def put_wall(i):
        e = p.expert(jnp.int32(i))
        return pltpu.make_async_copy(wall_buf.at[e], wall_ref.at[e], wall_sems.at[i])

    put_wall(0).start()
    hops[3].start()
    hops[0].wait_recv()
    s_ids.start()
    hops[1].wait_recv()
    s_gate.start()
    ring.event(0)
    ring.event(1)
    s_ids.forward()
    s_gate.forward()
    s_dy.forward()
    hops[2].wait_recv()
    s_xb.start()
    ring.event(2)
    s_ids.near()
    s_gate.near()
    s_ids.last()
    s_gate.last()

    def route_step(s, carry):
        rank, gate = routing_rows(gate_buf[s, 0], ids_buf[s, 0], p.rank, num_local)
        rgb_ref[s, 0:8] = rank
        rgb_ref[s, 8:16] = gate
        fill_onehot(hot_ref.at[s], rgb_ref[s, 0:8], capacity)
        return carry

    def rows_of(s):
        return pl.ds(pl.multiple_of(s * capacity, 16), capacity)

    def dy_step(s, carry):
        rows = jnp.dot(hot_ref[s], dy_buf[s], preferred_element_type=F32)
        for k in range(num_local):
            col = gate_column(rgb_ref[s, k:k + 1], rgb_ref[s, 8 + k:9 + k], capacity)
            q_buf[k, rows_of(s)] = (col * rows[k * capacity:(k + 1) * capacity]).astype(BF16)
        return carry

    def x_step(j, carry):
        s = p.arrival(j)
        rows = jnp.dot(hot_ref[s], xb_buf[s], preferred_element_type=F32).astype(BF16)
        for k in range(num_local):
            xs_buf[k, rows_of(s)] = rows[k * capacity:(k + 1) * capacity]
        return carry

    half = TG // 2
    lax.fori_loop(0, half, route_step, 0)
    ring.event(3)
    put_wall(1).start()
    put_wall(2).start()
    lax.fori_loop(half, TG, route_step, 0)
    put_rg = [pltpu.make_async_copy(rgb_ref, rg_ref, rg_sems.at[0]),
              pltpu.make_async_copy(ids_buf.at[:, 1], ids_out, rg_sems.at[1]),
              pltpu.make_async_copy(gate_buf.at[:, 1], gate_out, rg_sems.at[2])]
    for copy in put_rg:
        copy.start()
    s_dy.near()
    s_dy.last()
    keep_dy.wait()
    ring.event(4)
    lax.fori_loop(0, half, dy_step, 0)
    ring.event(5)
    s_xb.forward()
    hops[3].wait_recv()
    s_xf.start()
    ring.event(6)
    lax.fori_loop(half, TG, dy_step, 0)
    ring.event(7)
    put_wall(3).start()
    put_wall(4).start()
    s_xb.near()
    lax.fori_loop(0, 6, x_step, 0)
    ring.event(8)
    s_xb.last()
    lax.fori_loop(6, TG, x_step, 0)
    ring.event(9)
    expert_of = p.expert

    def put_dw(i):
        slot = lax.rem(i, 2)
        return pltpu.make_async_copy(dw_buf.at[slot], dw_ref.at[expert_of(i)], dw_sems.at[slot])

    def put_dx(i):
        e = expert_of(i)
        return pltpu.make_async_copy(q_buf.at[e], dxs_ref.at[e], dx_sems.at[i])

    def put_xs(n):
        return pltpu.make_async_copy(xs_buf.at[expert_of(jnp.int32(LATE[n]))], xs_ref.at[n], xs_sems.at[n])

    def put_xf(j):
        s = p.arrival(jnp.int32(j))
        return pltpu.make_async_copy(xf_buf.at[s], xf_ref.at[s], xf_sems.at[j])

    for n in range(len(LATE)):
        put_xs(n).start()
        put_dx(jnp.int32(LATE[n])).start()

    def backward_step(i, carry):
        @pl.when(i == 3)
        def _():
            ring.event(10)

        @pl.when(i == 4)
        def _():
            s_xf.forward()

        @pl.when(i == 5)
        def _():
            ring.event(11)
            put_wall(5).start()
            put_wall(6).start()

        @pl.when(i == 6)
        def _():
            s_xf.near()
            for j in range(6):
                put_xf(j).start()
            ring.event(12)

        @pl.when(i >= EARLY[0] + 2)
        def _():
            put_dw(i - 2).wait()

        e = expert_of(i)
        expert_step(xs_buf[e], q_buf[e], wall_buf[e, :width], wall_buf[e, width:], dw_buf.at[lax.rem(i, 2)],
                    q_buf.at[e], dab_ref)
        put_dw(i).start()
        put_dx(i).start()
        return carry

    lax.fori_loop(EARLY[0], EARLY[-1] + 1, backward_step, 0)
    s_xf.last()
    for j in (6, 7):
        put_xf(j).start()
    ring.event(13)
    put_wall(7).start()
    for n in range(len(LATE)):
        put_xs(n).wait()
    for i in range(num_local):
        put_dx(jnp.int32(i)).wait()
    put_dw(jnp.int32(EARLY[-2])).wait()
    put_dw(jnp.int32(EARLY[-1])).wait()
    for s in spread:
        s.finish()
    for hop in hops:
        hop.wait_send()
    ring.finish()
    for i in range(num_local):
        put_xf(i).wait()
        put_wall(i).wait()
    for copy in put_rg:
        copy.wait()


def dispatch_rows(x_acts, ids, gates, dy, w_in, w_up, w_out, capacity, num_stages):
    tokens, width = dy.shape
    hid = w_in.shape[1]
    num_local = 8
    slot_shape = jax.ShapeDtypeStruct((num_local, TG * capacity, width), BF16)
    rg_shape = jax.ShapeDtypeStruct((TG, 16, tokens), F32)
    wall_size = (num_local, width + hid, width)
    any_spec = pl.BlockSpec(memory_space=pl.ANY)
    tok_buf = pltpu.VMEM((TG, tokens, width), BF16)
    slot_buf = pltpu.VMEM((num_local, TG * capacity, width), BF16)
    return pl.pallas_call(
        functools.partial(dispatch_kernel, num_stages, capacity),
        in_specs=[any_spec] * 7,
        out_specs=[any_spec] * 8,
        out_shape=[jax.ShapeDtypeStruct(wall_size, F32), slot_shape,
                   jax.ShapeDtypeStruct((len(LATE),) + slot_shape.shape[1:], BF16),
                   jax.ShapeDtypeStruct((TG, tokens, width), BF16), jax.ShapeDtypeStruct(wall_size, BF16),
                   rg_shape, jax.ShapeDtypeStruct((TG,) + ids.shape[1:], jnp.int32),
                   jax.ShapeDtypeStruct((TG,) + ids.shape[1:], F32)],
        scratch_shapes=[
            pltpu.VMEM(rg_shape.shape, F32), tok_buf, tok_buf, tok_buf, pltpu.VMEM((TG,) + ids.shape, jnp.int32),
            pltpu.VMEM((TG,) + gates.shape, F32), pltpu.VMEM((TG, num_local * capacity, tokens), BF16),
            slot_buf, slot_buf, pltpu.VMEM(wall_size, BF16), pltpu.VMEM((2,) + wall_size[1:], F32),
            pltpu.VMEM((TG * capacity, 2 * hid), BF16),
            pltpu.SemaphoreType.DMA((5, 8)), pltpu.SemaphoreType.DMA((5, 8)),
            pltpu.SemaphoreType.DMA((4,)), pltpu.SemaphoreType.DMA((4,)),
            pltpu.SemaphoreType.DMA((2, 14)), pltpu.SemaphoreType.DMA((2, 14)),
            pltpu.SemaphoreType.DMA((4,)), pltpu.SemaphoreType.DMA((2,)), pltpu.SemaphoreType.DMA((num_local,)),
            pltpu.SemaphoreType.DMA((len(LATE),)), pltpu.SemaphoreType.DMA((num_local,)),
            pltpu.SemaphoreType.DMA((TG,)), pltpu.SemaphoreType.DMA((3,))],
        compiler_params=pltpu.CompilerParams(collective_id=1, has_side_effects=True,
                                             vmem_limit_bytes=63 << 20),
        cost_estimate=pl.CostEstimate(flops=40 * 10 ** 9, bytes_accessed=40 << 20, transcendentals=0),
        name='dispatch_rows',
    )(x_acts, ids, gates, dy, w_in, w_up, w_out)


class GradRing:
    def __init__(self, p, part, inbox, send_sems, recv_sems):
        self.part, self.inbox = part, inbox
        self.rows = part.shape[1] // 4
        self.copies, self.target = [], []
        self.home = p.z_slot(0)
        for way, device in ((0, p.z_up), (1, p.z_down)):
            way_copies, way_target = [], []
            for i in range(14):
                step, pos = divmod(i + 2, 4)
                piece = (pos + 2 - 2 * way) % 4
                slot = p.z_slot(4 - step if way == 0 else step - 4)
                src = part.at[slot, pl.ds(piece * self.rows, self.rows)]
                dst = inbox.at[way, pl.ds(i * self.rows, self.rows)]
                way_copies.append(send(src, dst, send_sems.at[way, i], recv_sems.at[way, i], device))
                way_target.append((slot, piece))
            self.copies.append(way_copies)
            self.target.append(way_target)

    def start(self, lo, hi):
        for i in range(lo, hi):
            for way in range(2):
                self.copies[way][i].start()

    def event(self, k):
        i = (2, 3, 0, 1, 6, 7, 4, 5, 10, 11, 8, 9, 12, 13)[k]
        for way in range(2):
            self.copies[way][i].wait_recv()
            if i + 4 < 14:
                slot, piece = self.target[way][i + 4]
            else:
                slot, piece = self.home, (i - 10 + 2 - 2 * way) % 4
            rows = pl.ds(piece * self.rows, self.rows)
            self.part[slot, rows] = self.part[slot, rows] + self.inbox[way, pl.ds(i * self.rows, self.rows)]
            if i + 4 < 14:
                self.copies[way][i + 4].start()

    def finish(self):
        for way in range(2):
            for copy in self.copies[way]:
                copy.wait_send()


class Combine:
    def __init__(self, p, partial_sum, side_out, side_in, acc, half_in, up_in, down_in, send_sems, recv_sems):
        half = acc.shape[1] // 2
        self.low, self.high = pl.ds(0, half), pl.ds(half, half)
        low, high = self.low, self.high
        self.p, self.partial_sum = p, partial_sum
        self.side_out, self.side_in, self.acc, self.half_in = side_out, side_in, acc, half_in
        self.up_in, self.down_in = up_in, down_in

        def copy(i, src, dst, device):
            return send(src, dst, send_sems.at[i], recv_sems.at[i], device)

        self.sides = [copy(d, side_out.at[d], side_in.at[d], p.partner) for d in range(4)]
        self.far_up = copy(4, acc.at[2, low], half_in.at[0], p.up)
        self.far_down = copy(5, acc.at[2, high], half_in.at[1], p.down)
        self.up_a = copy(6, acc.at[1, high], up_in.at[high], p.up)
        self.up_b = copy(7, acc.at[1, low], up_in.at[low], p.up)
        self.down_a = copy(8, acc.at[3, low], down_in.at[low], p.down)
        self.down_b = copy(9, acc.at[3, high], down_in.at[high], p.down)

    def both(self, d):
        self.side_out[d] = self.partial_sum(self.p.slot(d, True))
        self.sides[d].start()
        self.acc[d] = self.partial_sum(self.p.slot(d))

    def add_side(self, d):
        self.sides[d].wait_recv()
        self.acc[d] = self.acc[d] + self.side_in[d]

    def start_far(self):
        self.far_up.start()
        self.far_down.start()

    def add_far(self):
        low, high, acc = self.low, self.high, self.acc
        self.far_up.wait_recv()
        acc[1, low] = acc[1, low] + self.half_in[0]
        self.up_b.start()
        self.far_down.wait_recv()
        acc[3, high] = acc[3, high] + self.half_in[1]
        self.down_b.start()

    def total(self):
        for copy in (self.up_a, self.up_b, self.down_a, self.down_b):
            copy.wait_recv()
        return (self.acc[0] + self.up_in[...] + self.down_in[...]).astype(BF16)

    def finish(self):
        for copy in self.sides + [self.far_up, self.far_down, self.up_a, self.up_b, self.down_a, self.down_b]:
            copy.wait_send()


def finish_kernel(num_stages, capacity, dw_ref, dxs_ref, xs_ref, xf_ref, wall_ref, rg_hbm, ids_hbm, gate_hbm, out_ref,
                  rgb_ref, rgf_ref, ids_buf, gate_buf, x_buf, dab_ref, part, inbox, slots, hot_ref, xf_buf, w_buf, side_out, side_in, acc, half_in, up_in, down_in,
                  stage_dx, land_dx, z_send, z_recv, dx_send, dx_recv, y_send, y_recv, hop_send, hop_recv,
                  load_sems, slot_sems, x_sems, xf_sems, w_sems, rg_sems, credit):
    p = Peers(num_stages)
    num_local = slots.shape[0]
    tokens, width = stage_dx.shape
    def late_number(i):
        return 2 - i + 5 * (1 - (i + 1) // 2)

    def load_late(i):
        slot, e = lax.rem(i, 2), p.expert(late_number(i))
        return (pltpu.make_async_copy(wall_ref.at[e], w_buf.at[slot], w_sems.at[slot]),
                pltpu.make_async_copy(xs_ref.at[i], x_buf.at[slot], x_sems.at[slot]),
                pltpu.make_async_copy(dxs_ref.at[e], slots.at[e], slot_sems.at[i]))

    def load_slot(i):
        e = p.expert(jnp.int32(i))
        return pltpu.make_async_copy(dxs_ref.at[e], slots.at[e], slot_sems.at[i + 1])

    def load_dw(i):
        e = p.expert(jnp.int32(i))
        return pltpu.make_async_copy(dw_ref.at[e], part.at[e], load_sems.at[i])

    load_rg = [pltpu.make_async_copy(rg_hbm, rgb_ref, rg_sems.at[0]),
               pltpu.make_async_copy(ids_hbm, ids_buf, rg_sems.at[1]),
               pltpu.make_async_copy(gate_hbm, gate_buf, rg_sems.at[2])]
    load_dw(5).start()
    load_dw(6).start()
    for i in range(2):
        for load in load_late(jnp.int32(i)):
            load.start()
    for load in load_rg:
        load.start()
    for i in EARLY:
        load_slot(i).start()
    for i in EARLY[:-2]:
        load_dw(i).start()
    greet((p.up, p.down, p.partner, p.after, p.before, p.z_up, p.z_down))
    ring = GradRing(p, part, inbox, z_send, z_recv)

    load_dw(5).wait()
    load_dw(6).wait()
    ring.start(2, 4)

    def late_step(i, carry):
        for load in load_late(i):
            load.wait()
        slot, e = lax.rem(i, 2), p.expert(late_number(i))
        expert_step(x_buf[slot], slots[e], w_buf[slot, :width], w_buf[slot, width:], part.at[e], slots.at[e], dab_ref)

        @pl.when(i == 0)
        def _():
            ring.start(0, 2)
            for load in load_late(i + 2):
                load.start()

        return carry

    lax.fori_loop(0, len(LATE), late_step, 0)
    for load in load_rg:
        load.wait()
    for i in EARLY:
        load_slot(i).wait()

    def rows_of(s):
        return pl.ds(pl.multiple_of(s * capacity, 16), capacity)

    def partial_sum(rg_ref):
        def compute(s):
            fill_onehot(hot_ref, rg_ref[s, 0:8], capacity)
            rows = slots[:, rows_of(s)].reshape(hot_ref.shape[0], width)
            return lax.dot_general(hot_ref[...], rows, (((0,), (0,)), ((), ())), preferred_element_type=F32)
        return compute

    shared = (side_out, side_in, acc, half_in, up_in, down_in)
    dx_sum = Combine(p, partial_sum(rgb_ref), *shared, dx_send, dx_recv)
    y_sum = Combine(p, partial_sum(rgf_ref), *shared, y_send, y_recv)

    def load_xf(s):
        slot = lax.rem(s, 2)
        return pltpu.make_async_copy(xf_ref.at[s], xf_buf.at[slot], xf_sems.at[slot])

    def load_w(e):
        slot = lax.rem(e, 2)
        return pltpu.make_async_copy(wall_ref.at[e], w_buf.at[slot], w_sems.at[slot])

    def route_step(s, carry):
        rank, gate = routing_rows(gate_buf[s], ids_buf[s], p.rank, num_local)
        rgf_ref[s, 0:8] = rank
        rgf_ref[s, 8:16] = gate
        return carry

    def gather_step(s, carry):
        @pl.when(s < TG - 1)
        def _():
            load_xf(s + 1).start()

        load_xf(s).wait()
        fill_onehot(hot_ref, rgf_ref[s, 0:8], capacity)
        rows = jnp.dot(hot_ref[...], xf_buf[lax.rem(s, 2)], preferred_element_type=F32).astype(BF16)
        for k in range(num_local):
            slots[k, rows_of(s)] = rows[k * capacity:(k + 1) * capacity]
        return carry

    def forward_step(e, carry):
        @pl.when(e < num_local - 1)
        def _():
            load_w(e + 1).start()

        load_w(e).wait()
        slot = lax.rem(e, 2)
        wcat, wout = w_buf[slot, :width], w_buf[slot, width:]
        hid = wout.shape[0]
        pre = jnp.dot(slots[e], wcat, preferred_element_type=F32)
        a, b = pre[:, :hid], pre[:, hid:]
        h = (a * jax.nn.sigmoid(a) * b).astype(BF16)
        o = jnp.dot(h, wout, preferred_element_type=F32)
        for s in range(TG):
            col = gate_column(rgf_ref[s, pl.ds(e, 1)], rgf_ref[s, pl.ds(8 + e, 1)], capacity)
            slots[e, s * capacity:(s + 1) * capacity] = (col * o[s * capacity:(s + 1) * capacity]).astype(BF16)
        return carry

    load_xf(jnp.int32(0)).start()
    load_w(jnp.int32(0)).start()
    dx_sum.both(2)
    dx_sum.add_side(2)
    dx_sum.start_far()
    dx_sum.both(1)
    dx_sum.add_side(1)
    dx_sum.up_a.start()
    dx_sum.both(3)
    dx_sum.add_side(3)
    dx_sum.down_a.start()
    dx_sum.both(0)
    dx_sum.add_side(0)
    pl.semaphore_signal(credit.at[2], inc=1, device_id=p.partner, device_id_type=MESH)
    for i in EARLY[:-2]:
        load_dw(i).wait()
    ring.event(0)
    lax.fori_loop(0, TG, route_step, 0)
    lax.fori_loop(0, 3, gather_step, 0)
    dx_sum.add_far()
    ring.event(1)
    lax.fori_loop(3, TG, gather_step, 0)
    ring.event(2)
    lax.fori_loop(0, 5, forward_step, 0)
    ring.event(3)
    lax.fori_loop(5, num_local, forward_step, 0)
    stage_dx[...] = dx_sum.total()
    hop = send(stage_dx, land_dx, hop_send, hop_recv, p.before)
    hop.start()
    pl.semaphore_signal(credit.at[1], inc=1, device_id=p.up, device_id_type=MESH)
    pl.semaphore_signal(credit.at[0], inc=1, device_id=p.down, device_id_type=MESH)
    dx_sum.finish()
    pl.semaphore_wait(credit.at[2], 1)
    y_sum.both(2)
    y_sum.add_side(2)
    pl.semaphore_wait(credit.at[0], 1)
    pl.semaphore_wait(credit.at[1], 1)
    y_sum.start_far()
    ring.event(4)
    y_sum.both(1)
    y_sum.add_side(1)
    y_sum.up_a.start()
    y_sum.both(3)
    y_sum.add_side(3)
    y_sum.down_a.start()
    y_sum.both(0)
    y_sum.add_side(0)
    ring.event(5)
    y_sum.add_far()
    ring.event(6)
    ring.event(7)
    ring.event(8)
    out_ref[:tokens] = y_sum.total()
    for i in range(9, 12):
        ring.event(i)
    hop.wait()
    out_ref[tokens:2 * tokens] = land_dx[...]
    for i in range(2):
        ring.event(12 + i)
        for piece in (i, i + 2):
            rows = pl.ds(piece * ring.rows, ring.rows)
            out_ref[pl.ds(2 * tokens + piece * ring.rows, ring.rows)] = part[ring.home, rows].astype(BF16)
    y_sum.finish()
    ring.finish()


def finish_rows(dw, dxs, xs_late, xf_all, wall, rg, ids, gates, capacity, num_stages):
    num_local, _, width = dxs.shape
    tokens = rg.shape[2]
    any_spec = pl.BlockSpec(memory_space=pl.ANY)
    dma, quad = pltpu.SemaphoreType.DMA, pltpu.VMEM((4, tokens, width), F32)
    one = pltpu.VMEM((tokens, width), F32)
    return pl.pallas_call(
        functools.partial(finish_kernel, num_stages, capacity),
        in_specs=[any_spec] * 8,
        out_specs=pl.BlockSpec(memory_space=pltpu.VMEM),
        out_shape=pltpu.VMEM((2 * tokens + dw.shape[1], width), BF16),
        scratch_shapes=[
            pltpu.VMEM(rg.shape, F32), pltpu.VMEM(rg.shape, F32), pltpu.VMEM(ids.shape, jnp.int32),
            pltpu.VMEM(gates.shape, F32), pltpu.VMEM((2,) + dxs.shape[1:], BF16), pltpu.VMEM((dxs.shape[1], width), BF16),
            pltpu.VMEM(dw.shape, F32), pltpu.VMEM((2, 14 * (dw.shape[1] // 4), width), F32),
            pltpu.VMEM(dxs.shape, BF16), pltpu.VMEM((num_local * capacity, tokens), BF16),
            pltpu.VMEM((2, tokens, width), BF16), pltpu.VMEM((2,) + wall.shape[1:], BF16),
            quad, quad, quad, pltpu.VMEM((2, tokens // 2, width), F32), one, one,
            pltpu.VMEM((tokens, width), BF16), pltpu.VMEM((tokens, width), BF16),
            dma((2, 14)), dma((2, 14)), dma((10,)), dma((10,)), dma((10,)), dma((10,)), dma, dma,
            dma((num_local,)), dma((num_local,)), dma((2,)), dma((2,)), dma((2,)),
            dma((3,)), pltpu.SemaphoreType.REGULAR((3,))],
        compiler_params=pltpu.CompilerParams(collective_id=2, has_side_effects=True,
                                             vmem_limit_bytes=61 << 20),
        cost_estimate=pl.CostEstimate(flops=60 * 10 ** 9, bytes_accessed=40 << 20, transcendentals=0),
        name='finish_rows',
    )(dw, dxs, xs_late, xf_all, wall, rg, ids, gates)


def split_kernel(out_ref, y_ref, dx_ref, wi_ref, wu_ref, wo_ref, out_sems):
    tokens, (width, hid) = y_ref.shape[0], wi_ref.shape
    first = 2 * tokens
    targets = (((0, tokens), (0, width), y_ref), ((tokens, tokens), (0, width), dx_ref),
               ((first, width), (0, hid), wi_ref), ((first, width), (hid, hid), wu_ref),
               ((first + width, hid), (0, width), wo_ref))
    stores = []
    for i, (rows, cols, ref) in enumerate(targets):
        stores.append(pltpu.make_async_copy(out_ref.at[pl.ds(*rows), pl.ds(*cols)], ref, out_sems.at[i]))
        stores[-1].start()
    for store in stores:
        store.wait()


def split_rows(out, tokens, width, hid):
    shapes = ((tokens, width), (tokens, width), (width, hid), (width, hid), (hid, width))
    return pl.pallas_call(
        split_kernel,
        in_specs=[pl.BlockSpec(memory_space=pltpu.VMEM)],
        out_specs=[pl.BlockSpec(memory_space=pl.ANY)] * 5,
        out_shape=[jax.ShapeDtypeStruct(shape, BF16) for shape in shapes],
        scratch_shapes=[pltpu.SemaphoreType.DMA((5,))],
        compiler_params=pltpu.CompilerParams(vmem_limit_bytes=32 << 20),
        name='split_rows',
    )(out)


def solution(mesh):
    num_stages = mesh.shape['stage']

    def device_fn(x_acts, expert_ids, gate_wts, w_in, w_up, w_out, d_out):
        tokens, width = x_acts.shape[2], x_acts.shape[3]
        hid = w_in.shape[3]
        capacity = 96

        ids = jnp.swapaxes(expert_ids[:, 0], 1, 2)
        gates = jnp.swapaxes(gate_wts[:, 0], 1, 2)
        dwall, dxs, xs_late, xf_all, wall, rg, ids, gates = dispatch_rows(
            x_acts[:, 0], ids, gates, d_out[0], w_in[0, 0], w_up[0, 0], w_out[0, 0], capacity, num_stages)
        out = finish_rows(dwall, dxs, xs_late, xf_all, wall, rg, ids, gates, capacity, num_stages)
        y, dx, dw_in, dw_up, dw_out = split_rows(out, tokens, width, hid)
        return y[None], dx[None], dw_in[None, None], dw_up[None, None], dw_out[None, None]

    tok_spec = P(None, 'stage', 'expert', None)
    w_spec = P('stage', 'expert', None, None)
    row_spec = P('stage', 'expert', None)
    return jax.shard_map(device_fn, mesh=mesh,
                         in_specs=(tok_spec, tok_spec, tok_spec, w_spec, w_spec, w_spec, row_spec),
                         out_specs=(row_spec, row_spec, w_spec, w_spec, w_spec), check_vma=False)
```

```python
import functools

import jax
import jax.numpy as jnp
from jax import lax
from jax.experimental import pallas as pl
from jax.experimental.pallas import tpu as pltpu
from jax.sharding import PartitionSpec as P

TG = 8
F32 = jnp.float32
BF16 = jnp.bfloat16
MESH = pl.DeviceIdType.MESH
EARLY = (2, 3, 4, 5, 6)
LATE = (7, 1, 0)


def routing_rows(gates, ids, group_rank, num_local):
    tokens = ids.shape[1]
    taken, gate = [], []
    for k in range(num_local):
        hit = ids == group_rank + k * TG
        taken.append(jnp.sum(jnp.where(hit, 1.0, 0.0), axis=0, keepdims=True))
        gate.append(jnp.sum(jnp.where(hit, gates, 0.0), axis=0, keepdims=True))
    taken, gate = jnp.concatenate(taken, axis=0), jnp.concatenate(gate, axis=0)
    lane = lax.broadcasted_iota(jnp.int32, taken.shape, 1)
    count, shift = taken, 1
    while shift < tokens:
        count = count + jnp.where(lane >= shift, pltpu.roll(count, shift, 1), 0.0)
        shift *= 2
    return jnp.where(taken > 0.0, count - 1.0, -1.0), gate


def slot_mask(rank_row, capacity):
    slot = lax.broadcasted_iota(jnp.int32, (capacity, rank_row.shape[1]), 0).astype(F32)
    return slot == rank_row


def fill_onehot(hot_ref, rank, capacity):
    for k in range(rank.shape[0]):
        hit = slot_mask(rank[k:k + 1], capacity)
        hot_ref[k * capacity:(k + 1) * capacity, :] = jnp.where(hit, 1.0, 0.0).astype(BF16)


def gate_column(rank_row, gate_row, capacity):
    hit = slot_mask(rank_row, capacity)
    return jnp.sum(jnp.where(hit, gate_row, 0.0), axis=1, keepdims=True)


class Peers:
    def __init__(self, num_stages, group_size=64):
        stage, me = lax.axis_index('stage'), lax.axis_index('expert')
        self.rank = lax.rem(me, TG)
        self.base = me - self.rank
        self.zpos = self.base // TG
        self.z_size = group_size // TG
        self.z_up = (stage, self.z_slot(1) * TG + self.rank)
        self.z_down = (stage, self.z_slot(-1) * TG + self.rank)
        self.core = lax.rem(self.rank, 2)
        self.ypos = (self.rank - self.core) // 2
        self.own, self.up_slot = self.rank, self.slot(1)
        self.far_slot, self.down_slot = self.slot(2), self.slot(3)
        self.up = (stage, self.base + self.slot(1))
        self.down = (stage, self.base + self.slot(3))
        self.partner = (stage, self.base + self.slot(0, True))
        self.after = (lax.rem(stage + 1, num_stages), me)
        self.before = (lax.rem(stage + num_stages - 1, num_stages), me)

    def z_slot(self, offset):
        return lax.rem(self.zpos + offset + self.z_size, self.z_size)

    def expert(self, i):
        return self.z_slot((1 - 2 * lax.rem(i, 2)) * ((i + 1) // 2))

    def arrival(self, j):
        h = j // 2
        offset = h + h // 2 - 2 * (h // 3)
        return lax.rem(self.ypos + offset, 4) * 2 + lax.rem(self.core + lax.rem(j, 2), 2)

    def slot(self, offset, other_core=False):
        core = 1 - self.core if other_core else self.core
        return lax.rem(self.ypos + offset, 4) * 2 + core


def greet(devices):
    barrier = pltpu.get_barrier_semaphore()
    for device in devices:
        pl.semaphore_signal(barrier, inc=1, device_id=device, device_id_type=MESH)
    pl.semaphore_wait(barrier, len(devices))


def send(src, dst, send_sem, recv_sem, device):
    return pltpu.make_async_remote_copy(src_ref=src, dst_ref=dst, send_sem=send_sem, recv_sem=recv_sem,
                                        device_id=device, device_id_type=MESH)


class Spread:
    def __init__(self, peers, src, buf, send_sems, recv_sems):
        half = buf.shape[1] // 2
        p = peers

        def copy(i, ref, device, dst=None):
            return send(ref, ref if dst is None else dst, send_sems.at[i], recv_sems.at[i], device)

        own = buf.at[p.own]
        self.own_up = copy(0, src, p.up, own)
        self.own_down = copy(1, src, p.down, own)
        self.fwd_up = copy(2, buf.at[p.down_slot, pl.ds(0, half)], p.up)
        self.fwd_down = copy(3, buf.at[p.up_slot, pl.ds(half, half)], p.down)
        self.own_side = copy(4, src, p.partner, own)
        self.down_side = copy(5, buf.at[p.down_slot], p.partner)
        self.up_side = copy(6, buf.at[p.up_slot], p.partner)
        self.far_side = copy(7, buf.at[p.far_slot], p.partner)

    def start(self):
        self.own_up.start()
        self.own_down.start()
        self.own_side.start()

    def forward(self):
        self.own_up.wait_recv()
        self.fwd_up.start()
        self.down_side.start()
        self.own_down.wait_recv()
        self.fwd_down.start()
        self.up_side.start()

    def near(self):
        for copy in (self.own_side, self.down_side, self.up_side):
            copy.wait_recv()

    def last(self):
        self.fwd_up.wait_recv()
        self.fwd_down.wait_recv()
        self.far_side.start()
        self.far_side.wait_recv()

    def finish(self):
        for copy in (self.own_up, self.own_down, self.fwd_up, self.fwd_down,
                     self.own_side, self.down_side, self.up_side, self.far_side):
            copy.wait_send()


class WeightRing:
    def __init__(self, p, buf, send_sems, recv_sems):
        self.rows = buf.shape[1] // 4
        self.copies = []
        for way, device in ((0, p.z_up), (1, p.z_down)):
            way_copies = []
            for i in range(14):
                step, pos = divmod(i, 4)
                piece = (pos + 2 * way) % 4
                slot = p.z_slot(-step if way == 0 else step)
                ref = buf.at[slot, pl.ds(piece * self.rows, self.rows)]
                way_copies.append(send(ref, ref, send_sems.at[way, i], recv_sems.at[way, i], device))
            self.copies.append(way_copies)

    def start(self):
        for pos in range(4):
            for way in range(2):
                self.copies[way][pos].start()

    def event(self, i):
        for way in range(2):
            self.copies[way][i].wait_recv()
            if i + 4 < 14:
                self.copies[way][i + 4].start()

    def finish(self):
        for way in range(2):
            for copy in self.copies[way]:
                copy.wait_send()


def expert_step(x, q, wcat, wout, dw_ref, dx_ref, dab_ref):
    width, hid = wcat.shape[0], wout.shape[0]
    pre = jnp.dot(x, wcat, preferred_element_type=F32)
    a, b = pre[:, :hid], pre[:, hid:]
    sig = jax.nn.sigmoid(a)
    act = a * sig
    h = (act * b).astype(BF16)
    dw_ref[width:] = lax.dot_general(h, q, (((0,), (0,)), ((), ())), preferred_element_type=F32)
    u = lax.dot_general(q, wout, (((1,), (1,)), ((), ())), preferred_element_type=F32)
    dab_ref[:, :hid] = (u * b * sig * (1.0 + a * (1.0 - sig))).astype(BF16)
    dab_ref[:, hid:] = (u * act).astype(BF16)
    dab = dab_ref[...]
    dw_ref[:width] = lax.dot_general(x, dab, (((0,), (0,)), ((), ())), preferred_element_type=F32)
    dx = lax.dot_general(dab, wcat, (((1,), (1,)), ((), ())), preferred_element_type=F32)
    dx_ref[...] = dx.astype(BF16)


def dispatch_kernel(num_stages, capacity, x_ref, ids_ref, gate_ref, dy_ref, wi_ref, wu_ref, wo_ref,
                    dw_ref, dxs_ref, xs_ref, xf_ref, wall_ref, rg_ref, ids_out, gate_out,
                    rgb_ref, dy_buf, xb_buf, xf_buf, ids_buf, gate_buf, hot_ref, xs_buf, q_buf, wall_buf, dw_buf, dab_ref,
                    send_sems, recv_sems, hop_send, hop_recv, z_send, z_recv, local_sems, dw_sems, dx_sems,
                    xs_sems, wall_sems, xf_sems, rg_sems):
    p = Peers(num_stages)
    num_local = xs_buf.shape[0]
    width, hid = wi_ref.shape
    block = wall_buf.at[p.z_slot(0)]
    keep = [pltpu.make_async_copy(wi_ref, block.at[pl.ds(0, width), pl.ds(0, hid)], local_sems.at[0]),
            pltpu.make_async_copy(wu_ref, block.at[pl.ds(0, width), pl.ds(hid, hid)], local_sems.at[1]),
            pltpu.make_async_copy(wo_ref, block.at[pl.ds(width, hid)], local_sems.at[2])]
    keep_dy = pltpu.make_async_copy(dy_ref, dy_buf.at[p.own], local_sems.at[3])
    for copy in keep:
        copy.start()
    keep_dy.start()
    greet((p.up, p.down, p.partner, p.after, p.before, p.z_up, p.z_down))
    hops = []
    for i, (src, buf) in enumerate(((ids_ref, ids_buf), (gate_ref, gate_buf),
                                    (x_ref.at[0], xb_buf), (x_ref.at[1], xf_buf))):
        hops.append(send(src, buf.at[p.own], hop_send.at[i], hop_recv.at[i], p.after))
    spread = [Spread(p, src, buf, send_sems.at[i], recv_sems.at[i]) for i, (src, buf) in enumerate((
        (ids_buf.at[p.own], ids_buf), (gate_buf.at[p.own], gate_buf), (xb_buf.at[p.own], xb_buf),
        (xf_buf.at[p.own], xf_buf), (dy_ref, dy_buf)))]
    s_ids, s_gate, s_xb, s_xf, s_dy = spread
    ring = WeightRing(p, wall_buf, z_send, z_recv)
    hops[0].start()
    hops[1].start()
    hops[2].start()
    s_dy.start()
    for copy in keep:
        copy.wait()
    ring.start()

    def put_wall(i):
        e = p.expert(jnp.int32(i))
        return pltpu.make_async_copy(wall_buf.at[e], wall_ref.at[e], wall_sems.at[i])

    put_wall(0).start()
    hops[3].start()
    hops[0].wait_recv()
    s_ids.start()
    hops[1].wait_recv()
    s_gate.start()
    ring.event(0)
    ring.event(1)
    s_ids.forward()
    s_gate.forward()
    s_dy.forward()
    hops[2].wait_recv()
    s_xb.start()
    ring.event(2)
    s_ids.near()
    s_gate.near()
    s_ids.last()
    s_gate.last()

    def route_step(s, carry):
        rank, gate = routing_rows(gate_buf[s, 0], ids_buf[s, 0], p.rank, num_local)
        rgb_ref[s, 0:8] = rank
        rgb_ref[s, 8:16] = gate
        fill_onehot(hot_ref.at[s], rgb_ref[s, 0:8], capacity)
        return carry

    def rows_of(s):
        return pl.ds(pl.multiple_of(s * capacity, 16), capacity)

    def dy_step(s, carry):
        rows = jnp.dot(hot_ref[s], dy_buf[s], preferred_element_type=F32)
        for k in range(num_local):
            col = gate_column(rgb_ref[s, k:k + 1], rgb_ref[s, 8 + k:9 + k], capacity)
            q_buf[k, rows_of(s)] = (col * rows[k * capacity:(k + 1) * capacity]).astype(BF16)
        return carry

    def x_step(j, carry):
        s = p.arrival(j)
        rows = jnp.dot(hot_ref[s], xb_buf[s], preferred_element_type=F32).astype(BF16)
        for k in range(num_local):
            xs_buf[k, rows_of(s)] = rows[k * capacity:(k + 1) * capacity]
        return carry

    half = TG // 2
    lax.fori_loop(0, half, route_step, 0)
    ring.event(3)
    put_wall(1).start()
    put_wall(2).start()
    lax.fori_loop(half, TG, route_step, 0)
    put_rg = [pltpu.make_async_copy(rgb_ref, rg_ref, rg_sems.at[0]),
              pltpu.make_async_copy(ids_buf.at[:, 1], ids_out, rg_sems.at[1]),
              pltpu.make_async_copy(gate_buf.at[:, 1], gate_out, rg_sems.at[2])]
    for copy in put_rg:
        copy.start()
    s_dy.near()
    s_dy.last()
    keep_dy.wait()
    ring.event(4)
    lax.fori_loop(0, half, dy_step, 0)
    ring.event(5)
    s_xb.forward()
    hops[3].wait_recv()
    s_xf.start()
    ring.event(6)
    lax.fori_loop(half, TG, dy_step, 0)
    ring.event(7)
    put_wall(3).start()
    put_wall(4).start()
    s_xb.near()
    lax.fori_loop(0, 6, x_step, 0)
    ring.event(8)
    s_xb.last()
    lax.fori_loop(6, TG, x_step, 0)
    ring.event(9)
    expert_of = p.expert

    def put_dw(i):
        slot = lax.rem(i, 2)
        return pltpu.make_async_copy(dw_buf.at[slot], dw_ref.at[expert_of(i)], dw_sems.at[slot])

    def put_dx(i):
        e = expert_of(i)
        return pltpu.make_async_copy(q_buf.at[e], dxs_ref.at[e], dx_sems.at[i])

    def put_xs(n):
        return pltpu.make_async_copy(xs_buf.at[expert_of(jnp.int32(LATE[n]))], xs_ref.at[n], xs_sems.at[n])

    def put_xf(j):
        s = p.arrival(jnp.int32(j))
        return pltpu.make_async_copy(xf_buf.at[s], xf_ref.at[s], xf_sems.at[j])

    for n in range(len(LATE)):
        put_xs(n).start()
        put_dx(jnp.int32(LATE[n])).start()

    def backward_step(i, carry):
        @pl.when(i == 3)
        def _():
            ring.event(10)

        @pl.when(i == 4)
        def _():
            s_xf.forward()

        @pl.when(i == 5)
        def _():
            ring.event(11)
            put_wall(5).start()
            put_wall(6).start()

        @pl.when(i == 6)
        def _():
            s_xf.near()
            for j in range(6):
                put_xf(j).start()
            ring.event(12)

        @pl.when(i >= EARLY[0] + 2)
        def _():
            put_dw(i - 2).wait()

        e = expert_of(i)
        expert_step(xs_buf[e], q_buf[e], wall_buf[e, :width], wall_buf[e, width:], dw_buf.at[lax.rem(i, 2)],
                    q_buf.at[e], dab_ref)
        put_dw(i).start()
        put_dx(i).start()
        return carry

    lax.fori_loop(EARLY[0], EARLY[-1] + 1, backward_step, 0)
    s_xf.last()
    for j in (6, 7):
        put_xf(j).start()
    ring.event(13)
    put_wall(7).start()
    for n in range(len(LATE)):
        put_xs(n).wait()
    for i in range(num_local):
        put_dx(jnp.int32(i)).wait()
    put_dw(jnp.int32(EARLY[-2])).wait()
    put_dw(jnp.int32(EARLY[-1])).wait()
    for s in spread:
        s.finish()
    for hop in hops:
        hop.wait_send()
    ring.finish()
    for i in range(num_local):
        put_xf(i).wait()
        put_wall(i).wait()
    for copy in put_rg:
        copy.wait()


def dispatch_rows(x_acts, ids, gates, dy, w_in, w_up, w_out, capacity, num_stages):
    tokens, width = dy.shape
    hid = w_in.shape[1]
    num_local = 8
    slot_shape = jax.ShapeDtypeStruct((num_local, TG * capacity, width), BF16)
    rg_shape = jax.ShapeDtypeStruct((TG, 16, tokens), F32)
    wall_size = (num_local, width + hid, width)
    any_spec = pl.BlockSpec(memory_space=pl.ANY)
    tok_buf = pltpu.VMEM((TG, tokens, width), BF16)
    slot_buf = pltpu.VMEM((num_local, TG * capacity, width), BF16)
    return pl.pallas_call(
        functools.partial(dispatch_kernel, num_stages, capacity),
        in_specs=[any_spec] * 7,
        out_specs=[any_spec] * 8,
        out_shape=[jax.ShapeDtypeStruct(wall_size, F32), slot_shape,
                   jax.ShapeDtypeStruct((len(LATE),) + slot_shape.shape[1:], BF16),
                   jax.ShapeDtypeStruct((TG, tokens, width), BF16), jax.ShapeDtypeStruct(wall_size, BF16),
                   rg_shape, jax.ShapeDtypeStruct((TG,) + ids.shape[1:], jnp.int32),
                   jax.ShapeDtypeStruct((TG,) + ids.shape[1:], F32)],
        scratch_shapes=[
            pltpu.VMEM(rg_shape.shape, F32), tok_buf, tok_buf, tok_buf, pltpu.VMEM((TG,) + ids.shape, jnp.int32),
            pltpu.VMEM((TG,) + gates.shape, F32), pltpu.VMEM((TG, num_local * capacity, tokens), BF16),
            slot_buf, slot_buf, pltpu.VMEM(wall_size, BF16), pltpu.VMEM((2,) + wall_size[1:], F32),
            pltpu.VMEM((TG * capacity, 2 * hid), BF16),
            pltpu.SemaphoreType.DMA((5, 8)), pltpu.SemaphoreType.DMA((5, 8)),
            pltpu.SemaphoreType.DMA((4,)), pltpu.SemaphoreType.DMA((4,)),
            pltpu.SemaphoreType.DMA((2, 14)), pltpu.SemaphoreType.DMA((2, 14)),
            pltpu.SemaphoreType.DMA((4,)), pltpu.SemaphoreType.DMA((2,)), pltpu.SemaphoreType.DMA((num_local,)),
            pltpu.SemaphoreType.DMA((len(LATE),)), pltpu.SemaphoreType.DMA((num_local,)),
            pltpu.SemaphoreType.DMA((TG,)), pltpu.SemaphoreType.DMA((3,))],
        compiler_params=pltpu.CompilerParams(collective_id=1, has_side_effects=True,
                                             vmem_limit_bytes=63 << 20),
        cost_estimate=pl.CostEstimate(flops=40 * 10 ** 9, bytes_accessed=40 << 20, transcendentals=0),
        name='dispatch_rows',
    )(x_acts, ids, gates, dy, w_in, w_up, w_out)


class GradRing:
    def __init__(self, p, part, inbox, send_sems, recv_sems):
        self.part, self.inbox = part, inbox
        self.rows = part.shape[1] // 4
        self.copies, self.target = [], []
        self.home = p.z_slot(0)
        for way, device in ((0, p.z_up), (1, p.z_down)):
            way_copies, way_target = [], []
            for i in range(14):
                step, pos = divmod(i + 2, 4)
                piece = (pos + 2 - 2 * way) % 4
                slot = p.z_slot(4 - step if way == 0 else step - 4)
                src = part.at[slot, pl.ds(piece * self.rows, self.rows)]
                dst = inbox.at[way, pl.ds(i * self.rows, self.rows)]
                way_copies.append(send(src, dst, send_sems.at[way, i], recv_sems.at[way, i], device))
                way_target.append((slot, piece))
            self.copies.append(way_copies)
            self.target.append(way_target)

    def start(self, lo, hi):
        for i in range(lo, hi):
            for way in range(2):
                self.copies[way][i].start()

    def event(self, k):
        i = (2, 3, 0, 1, 6, 7, 4, 5, 10, 11, 8, 9, 12, 13)[k]
        for way in range(2):
            self.copies[way][i].wait_recv()
            if i + 4 < 14:
                slot, piece = self.target[way][i + 4]
            else:
                slot, piece = self.home, (i - 10 + 2 - 2 * way) % 4
            rows = pl.ds(piece * self.rows, self.rows)
            self.part[slot, rows] = self.part[slot, rows] + self.inbox[way, pl.ds(i * self.rows, self.rows)]
            if i + 4 < 14:
                self.copies[way][i + 4].start()

    def finish(self):
        for way in range(2):
            for copy in self.copies[way]:
                copy.wait_send()


class Combine:
    def __init__(self, p, partial_sum, side_out, side_in, acc, half_in, up_in, down_in, send_sems, recv_sems):
        half = acc.shape[1] // 2
        self.low, self.high = pl.ds(0, half), pl.ds(half, half)
        low, high = self.low, self.high
        self.p, self.partial_sum = p, partial_sum
        self.side_out, self.side_in, self.acc, self.half_in = side_out, side_in, acc, half_in
        self.up_in, self.down_in = up_in, down_in

        def copy(i, src, dst, device):
            return send(src, dst, send_sems.at[i], recv_sems.at[i], device)

        self.sides = [copy(d, side_out.at[d], side_in.at[d], p.partner) for d in range(4)]
        self.far_up = copy(4, acc.at[2, low], half_in.at[0], p.up)
        self.far_down = copy(5, acc.at[2, high], half_in.at[1], p.down)
        self.up_a = copy(6, acc.at[1, high], up_in.at[high], p.up)
        self.up_b = copy(7, acc.at[1, low], up_in.at[low], p.up)
        self.down_a = copy(8, acc.at[3, low], down_in.at[low], p.down)
        self.down_b = copy(9, acc.at[3, high], down_in.at[high], p.down)

    def both(self, d):
        self.side_out[d] = self.partial_sum(self.p.slot(d, True))
        self.sides[d].start()
        self.acc[d] = self.partial_sum(self.p.slot(d))

    def add_side(self, d):
        self.sides[d].wait_recv()
        self.acc[d] = self.acc[d] + self.side_in[d]

    def start_far(self):
        self.far_up.start()
        self.far_down.start()

    def add_far(self):
        low, high, acc = self.low, self.high, self.acc
        self.far_up.wait_recv()
        acc[1, low] = acc[1, low] + self.half_in[0]
        self.up_b.start()
        self.far_down.wait_recv()
        acc[3, high] = acc[3, high] + self.half_in[1]
        self.down_b.start()

    def total(self):
        for copy in (self.up_a, self.up_b, self.down_a, self.down_b):
            copy.wait_recv()
        return (self.acc[0] + self.up_in[...] + self.down_in[...]).astype(BF16)

    def finish(self):
        for copy in self.sides + [self.far_up, self.far_down, self.up_a, self.up_b, self.down_a, self.down_b]:
            copy.wait_send()


def finish_kernel(num_stages, capacity, dw_ref, dxs_ref, xs_ref, xf_ref, wall_ref, rg_hbm, ids_hbm, gate_hbm, out_ref,
                  rgb_ref, rgf_ref, ids_buf, gate_buf, x_buf, dab_ref, part, inbox, slots, hot_ref, xf_buf, w_buf, side_out, side_in, acc, half_in, up_in, down_in,
                  stage_dx, land_dx, z_send, z_recv, dx_send, dx_recv, y_send, y_recv, hop_send, hop_recv,
                  load_sems, slot_sems, x_sems, xf_sems, w_sems, rg_sems, credit):
    p = Peers(num_stages)
    num_local = slots.shape[0]
    tokens, width = stage_dx.shape
    def late_number(i):
        return 2 - i + 5 * (1 - (i + 1) // 2)

    def load_late(i):
        slot, e = lax.rem(i, 2), p.expert(late_number(i))
        return (pltpu.make_async_copy(wall_ref.at[e], w_buf.at[slot], w_sems.at[slot]),
                pltpu.make_async_copy(xs_ref.at[i], x_buf.at[slot], x_sems.at[slot]),
                pltpu.make_async_copy(dxs_ref.at[e], slots.at[e], slot_sems.at[i]))

    def load_slot(i):
        e = p.expert(jnp.int32(i))
        return pltpu.make_async_copy(dxs_ref.at[e], slots.at[e], slot_sems.at[i + 1])

    def load_dw(i):
        e = p.expert(jnp.int32(i))
        return pltpu.make_async_copy(dw_ref.at[e], part.at[e], load_sems.at[i])

    load_rg = [pltpu.make_async_copy(rg_hbm, rgb_ref, rg_sems.at[0]),
               pltpu.make_async_copy(ids_hbm, ids_buf, rg_sems.at[1]),
               pltpu.make_async_copy(gate_hbm, gate_buf, rg_sems.at[2])]
    half = part.shape[1] // 2

    def load_half(i, lo, sem):
        e, rows = p.expert(jnp.int32(i)), pl.ds(lo, half)
        return pltpu.make_async_copy(dw_ref.at[e, rows], part.at[e, rows], load_sems.at[sem])

    first_halves = (load_half(6, half, 6), load_half(5, 0, 5))
    second_halves = (load_half(6, 0, 1), load_half(5, half, 0))
    for load in first_halves:
        load.start()
    for i in range(2):
        for load in load_late(jnp.int32(i)):
            load.start()
    for load in load_rg:
        load.start()
    for i in EARLY:
        load_slot(i).start()
    for load in second_halves:
        load.start()
    for i in EARLY[:-2]:
        load_dw(i).start()
    greet((p.up, p.down, p.partner, p.after, p.before, p.z_up, p.z_down))
    ring = GradRing(p, part, inbox, z_send, z_recv)

    for load in first_halves:
        load.wait()
    ring.start(2, 4)

    def late_step(i, carry):
        for load in load_late(i):
            load.wait()
        slot, e = lax.rem(i, 2), p.expert(late_number(i))
        expert_step(x_buf[slot], slots[e], w_buf[slot, :width], w_buf[slot, width:], part.at[e], slots.at[e], dab_ref)

        @pl.when(i == 0)
        def _():
            ring.start(0, 2)
            for load in load_late(i + 2):
                load.start()

        return carry

    lax.fori_loop(0, len(LATE), late_step, 0)
    for load in load_rg:
        load.wait()
    for i in EARLY:
        load_slot(i).wait()

    def rows_of(s):
        return pl.ds(pl.multiple_of(s * capacity, 16), capacity)

    def partial_sum(rg_ref):
        def compute(s):
            fill_onehot(hot_ref, rg_ref[s, 0:8], capacity)
            rows = slots[:, rows_of(s)].reshape(hot_ref.shape[0], width)
            return lax.dot_general(hot_ref[...], rows, (((0,), (0,)), ((), ())), preferred_element_type=F32)
        return compute

    shared = (side_out, side_in, acc, half_in, up_in, down_in)
    dx_sum = Combine(p, partial_sum(rgb_ref), *shared, dx_send, dx_recv)
    y_sum = Combine(p, partial_sum(rgf_ref), *shared, y_send, y_recv)

    def load_xf(s):
        slot = lax.rem(s, 2)
        return pltpu.make_async_copy(xf_ref.at[s], xf_buf.at[slot], xf_sems.at[slot])

    def load_w(e):
        slot = lax.rem(e, 2)
        return pltpu.make_async_copy(wall_ref.at[e], w_buf.at[slot], w_sems.at[slot])

    def route_step(s, carry):
        rank, gate = routing_rows(gate_buf[s], ids_buf[s], p.rank, num_local)
        rgf_ref[s, 0:8] = rank
        rgf_ref[s, 8:16] = gate
        return carry

    def gather_step(s, carry):
        @pl.when(s < TG - 1)
        def _():
            load_xf(s + 1).start()

        load_xf(s).wait()
        fill_onehot(hot_ref, rgf_ref[s, 0:8], capacity)
        rows = jnp.dot(hot_ref[...], xf_buf[lax.rem(s, 2)], preferred_element_type=F32).astype(BF16)
        for k in range(num_local):
            slots[k, rows_of(s)] = rows[k * capacity:(k + 1) * capacity]
        return carry

    def forward_step(e, carry):
        @pl.when(e < num_local - 1)
        def _():
            load_w(e + 1).start()

        load_w(e).wait()
        slot = lax.rem(e, 2)
        wcat, wout = w_buf[slot, :width], w_buf[slot, width:]
        hid = wout.shape[0]
        pre = jnp.dot(slots[e], wcat, preferred_element_type=F32)
        a, b = pre[:, :hid], pre[:, hid:]
        h = (a * jax.nn.sigmoid(a) * b).astype(BF16)
        o = jnp.dot(h, wout, preferred_element_type=F32)
        for s in range(TG):
            col = gate_column(rgf_ref[s, pl.ds(e, 1)], rgf_ref[s, pl.ds(8 + e, 1)], capacity)
            slots[e, s * capacity:(s + 1) * capacity] = (col * o[s * capacity:(s + 1) * capacity]).astype(BF16)
        return carry

    load_xf(jnp.int32(0)).start()
    load_w(jnp.int32(0)).start()
    dx_sum.both(2)
    dx_sum.add_side(2)
    dx_sum.start_far()
    dx_sum.both(1)
    dx_sum.add_side(1)
    dx_sum.up_a.start()
    dx_sum.both(3)
    dx_sum.add_side(3)
    dx_sum.down_a.start()
    dx_sum.both(0)
    dx_sum.add_side(0)
    pl.semaphore_signal(credit.at[2], inc=1, device_id=p.partner, device_id_type=MESH)
    for load in second_halves:
        load.wait()
    for i in EARLY[:-2]:
        load_dw(i).wait()
    ring.event(0)
    lax.fori_loop(0, TG, route_step, 0)
    lax.fori_loop(0, 3, gather_step, 0)
    dx_sum.add_far()
    ring.event(1)
    lax.fori_loop(3, TG, gather_step, 0)
    ring.event(2)
    lax.fori_loop(0, 5, forward_step, 0)
    ring.event(3)
    lax.fori_loop(5, num_local, forward_step, 0)
    stage_dx[...] = dx_sum.total()
    hop = send(stage_dx, land_dx, hop_send, hop_recv, p.before)
    hop.start()
    pl.semaphore_signal(credit.at[1], inc=1, device_id=p.up, device_id_type=MESH)
    pl.semaphore_signal(credit.at[0], inc=1, device_id=p.down, device_id_type=MESH)
    dx_sum.finish()
    pl.semaphore_wait(credit.at[2], 1)
    y_sum.both(2)
    y_sum.add_side(2)
    pl.semaphore_wait(credit.at[0], 1)
    pl.semaphore_wait(credit.at[1], 1)
    y_sum.start_far()
    ring.event(4)
    y_sum.both(1)
    y_sum.add_side(1)
    y_sum.up_a.start()
    y_sum.both(3)
    y_sum.add_side(3)
    y_sum.down_a.start()
    y_sum.both(0)
    y_sum.add_side(0)
    ring.event(5)
    y_sum.add_far()
    ring.event(6)
    ring.event(7)
    ring.event(8)
    out_ref[:tokens] = y_sum.total()
    for i in range(9, 12):
        ring.event(i)
    hop.wait()
    out_ref[tokens:2 * tokens] = land_dx[...]
    for i in range(2):
        ring.event(12 + i)
        for piece in (i, i + 2):
            rows = pl.ds(piece * ring.rows, ring.rows)
            out_ref[pl.ds(2 * tokens + piece * ring.rows, ring.rows)] = part[ring.home, rows].astype(BF16)
    y_sum.finish()
    ring.finish()


def finish_rows(dw, dxs, xs_late, xf_all, wall, rg, ids, gates, capacity, num_stages):
    num_local, _, width = dxs.shape
    tokens = rg.shape[2]
    any_spec = pl.BlockSpec(memory_space=pl.ANY)
    dma, quad = pltpu.SemaphoreType.DMA, pltpu.VMEM((4, tokens, width), F32)
    one = pltpu.VMEM((tokens, width), F32)
    return pl.pallas_call(
        functools.partial(finish_kernel, num_stages, capacity),
        in_specs=[any_spec] * 8,
        out_specs=pl.BlockSpec(memory_space=pltpu.VMEM),
        out_shape=pltpu.VMEM((2 * tokens + dw.shape[1], width), BF16),
        scratch_shapes=[
            pltpu.VMEM(rg.shape, F32), pltpu.VMEM(rg.shape, F32), pltpu.VMEM(ids.shape, jnp.int32),
            pltpu.VMEM(gates.shape, F32), pltpu.VMEM((2,) + dxs.shape[1:], BF16), pltpu.VMEM((dxs.shape[1], width), BF16),
            pltpu.VMEM(dw.shape, F32), pltpu.VMEM((2, 14 * (dw.shape[1] // 4), width), F32),
            pltpu.VMEM(dxs.shape, BF16), pltpu.VMEM((num_local * capacity, tokens), BF16),
            pltpu.VMEM((2, tokens, width), BF16), pltpu.VMEM((2,) + wall.shape[1:], BF16),
            quad, quad, quad, pltpu.VMEM((2, tokens // 2, width), F32), one, one,
            pltpu.VMEM((tokens, width), BF16), pltpu.VMEM((tokens, width), BF16),
            dma((2, 14)), dma((2, 14)), dma((10,)), dma((10,)), dma((10,)), dma((10,)), dma, dma,
            dma((num_local,)), dma((num_local,)), dma((2,)), dma((2,)), dma((2,)),
            dma((3,)), pltpu.SemaphoreType.REGULAR((3,))],
        compiler_params=pltpu.CompilerParams(collective_id=2, has_side_effects=True,
                                             vmem_limit_bytes=61 << 20),
        cost_estimate=pl.CostEstimate(flops=60 * 10 ** 9, bytes_accessed=40 << 20, transcendentals=0),
        name='finish_rows',
    )(dw, dxs, xs_late, xf_all, wall, rg, ids, gates)


def split_kernel(out_ref, y_ref, dx_ref, wi_ref, wu_ref, wo_ref, out_sems):
    tokens, (width, hid) = y_ref.shape[0], wi_ref.shape
    first = 2 * tokens
    targets = (((0, tokens), (0, width), y_ref), ((tokens, tokens), (0, width), dx_ref),
               ((first, width), (0, hid), wi_ref), ((first, width), (hid, hid), wu_ref),
               ((first + width, hid), (0, width), wo_ref))
    stores = []
    for i, (rows, cols, ref) in enumerate(targets):
        stores.append(pltpu.make_async_copy(out_ref.at[pl.ds(*rows), pl.ds(*cols)], ref, out_sems.at[i]))
        stores[-1].start()
    for store in stores:
        store.wait()


def split_rows(out, tokens, width, hid):
    shapes = ((tokens, width), (tokens, width), (width, hid), (width, hid), (hid, width))
    return pl.pallas_call(
        split_kernel,
        in_specs=[pl.BlockSpec(memory_space=pltpu.VMEM)],
        out_specs=[pl.BlockSpec(memory_space=pl.ANY)] * 5,
        out_shape=[jax.ShapeDtypeStruct(shape, BF16) for shape in shapes],
        scratch_shapes=[pltpu.SemaphoreType.DMA((5,))],
        compiler_params=pltpu.CompilerParams(vmem_limit_bytes=32 << 20),
        name='split_rows',
    )(out)


def solution(mesh):
    num_stages = mesh.shape['stage']

    def device_fn(x_acts, expert_ids, gate_wts, w_in, w_up, w_out, d_out):
        tokens, width = x_acts.shape[2], x_acts.shape[3]
        hid = w_in.shape[3]
        capacity = 96

        ids = jnp.swapaxes(expert_ids[:, 0], 1, 2)
        gates = jnp.swapaxes(gate_wts[:, 0], 1, 2)
        dwall, dxs, xs_late, xf_all, wall, rg, ids, gates = dispatch_rows(
            x_acts[:, 0], ids, gates, d_out[0], w_in[0, 0], w_up[0, 0], w_out[0, 0], capacity, num_stages)
        out = finish_rows(dwall, dxs, xs_late, xf_all, wall, rg, ids, gates, capacity, num_stages)
        y, dx, dw_in, dw_up, dw_out = split_rows(out, tokens, width, hid)
        return y[None], dx[None], dw_in[None, None], dw_up[None, None], dw_out[None, None]

    tok_spec = P(None, 'stage', 'expert', None)
    w_spec = P('stage', 'expert', None, None)
    row_spec = P('stage', 'expert', None)
    return jax.shard_map(device_fn, mesh=mesh,
                         in_specs=(tok_spec, tok_spec, tok_spec, w_spec, w_spec, w_spec, row_spec),
                         out_specs=(row_spec, row_spec, w_spec, w_spec, w_spec), check_vma=False)
```
